32 devices in a mesh: batch: 1 (over z), rows: 4 (over y), ksplit: 8 (over x, core).
Axes of the slice: x: 4, y: 4, z: 1, core: 2. Of those that a mesh axis runs over, the one named last changes fastest.
The devices are a block of a 4x4x8 slice.
Arguments:
- a_vals: bfloat16 [4, 8, 12, 128, 128], P(('batch', 'rows'), 'ksplit')
- b_vals: bfloat16 [8, 72, 128, 128], P(('batch', 'ksplit'))
- pairs: int32 [4, 8, 432, 1, 2], P(('batch', 'rows'), 'ksplit')
- plist_idx: int32 [4, 8, 432, 2], P(('batch', 'rows'), 'ksplit')
- c_idx: int32 [4, 8, 72, 2], P(('batch', 'rows'), 'ksplit')
Outputs:
- output: float32 [4, 8, 72, 128, 128], P(('batch', 'rows'), 'ksplit')
All inputs are finite; a program needn't handle non-finite values.
Results may differ from the reference program's by a relative error of at most 0.001.
Values are sent between devices in bfloat16 or wider.
A program may use at most 768 MiB of HBM per device.

```python
import jax
import jax.numpy as jnp
from jax import lax

BLOCK_SIZE = 128
ROW_GROUPS = 4
K_DEVICES = 8
BLOCK_ROWS = 512
BLOCK_COLS = 512
ROWS_TOUCH = 12
COLS_PER_DEV = 6
SENDERS = 6
K_PER_ROW = 1

ROW_LOCAL = BLOCK_ROWS // ROW_GROUPS
K_ACTIVE = 2 * K_PER_ROW
COL_TOUCH = SENDERS * COLS_PER_DEV
OWNER_SHARE = ROWS_TOUCH * COLS_PER_DEV // K_DEVICES
CAP_A = ROWS_TOUCH * K_PER_ROW
CAP_B = K_ACTIVE * COL_TOUCH
CAP_C = K_DEVICES * OWNER_SHARE
CAP_DEST = SENDERS * OWNER_SHARE
CAP_PART = K_DEVICES * CAP_DEST


def permute_rows(key, count, length):
    return jax.vmap(lambda sub_key: jax.random.permutation(sub_key, length))(jax.random.split(key, count))


def draw_indices(key):
    key_list = jax.random.split(key, 8)
    row_pick = permute_rows(key_list[0], ROW_GROUPS, ROW_LOCAL)[:, :ROWS_TOUCH]
    row_glob = row_pick + ROW_LOCAL * jnp.arange(ROW_GROUPS)[:, None]
    col_union = jax.random.permutation(key_list[1], BLOCK_COLS)[:K_DEVICES * COLS_PER_DEV]
    owner_shift = jax.random.randint(key_list[2], (ROW_GROUPS,), 0, K_DEVICES)
    band_start = jax.random.randint(key_list[3], (ROW_GROUPS, K_DEVICES, ROWS_TOUCH), 0, K_ACTIVE)
    a_order = permute_rows(key_list[4], ROW_GROUPS * K_DEVICES, CAP_A).reshape(ROW_GROUPS, K_DEVICES, CAP_A)
    b_order = permute_rows(key_list[5], K_DEVICES, CAP_B)
    c_order = permute_rows(key_list[6], ROW_GROUPS * K_DEVICES, CAP_C).reshape(ROW_GROUPS, K_DEVICES, CAP_C)
    p_order = permute_rows(key_list[7], ROW_GROUPS * K_DEVICES * K_DEVICES, CAP_DEST).reshape(ROW_GROUPS, K_DEVICES, K_DEVICES, CAP_DEST)
    dev_ids = jnp.arange(K_DEVICES)
    group_ids = jnp.arange(ROW_GROUPS)
    group4 = group_ids[:, None, None, None]
    owner4 = dev_ids[None, :, None, None]
    class4 = dev_ids[None, None, :, None]
    share4 = jnp.arange(OWNER_SHARE)[None, None, None, :]
    owned_pos = (owner4 - owner_shift[:, None, None, None]) % K_DEVICES + K_DEVICES * share4
    c_row = jnp.broadcast_to(row_glob[group4, owned_pos // COLS_PER_DEV], (ROW_GROUPS, K_DEVICES, K_DEVICES, OWNER_SHARE))
    c_col = col_union[K_DEVICES * (owned_pos % COLS_PER_DEV) + class4]
    c_all = jnp.stack([c_row, c_col], axis=-1).reshape(ROW_GROUPS, K_DEVICES, CAP_C, 2)
    c_idx = c_all[group_ids[:, None, None], dev_ids[None, :, None], c_order]
    full_shape = (ROW_GROUPS, K_DEVICES, K_DEVICES, SENDERS, OWNER_SHARE)
    group5 = group_ids[:, None, None, None, None]
    source5 = dev_ids[None, :, None, None, None]
    dest5 = dev_ids[None, None, :, None, None]
    sender5 = jnp.arange(SENDERS)[None, None, None, :, None]
    share5 = jnp.arange(OWNER_SHARE)[None, None, None, None, :]
    sent_pos = (dest5 - owner_shift[:, None, None, None, None]) % K_DEVICES + K_DEVICES * share5
    row_slot = jnp.broadcast_to(sent_pos // COLS_PER_DEV, full_shape)
    col_set = sent_pos % COLS_PER_DEV
    col_pos = K_DEVICES * col_set + (source5 - sender5) % K_DEVICES
    local_col = jnp.broadcast_to(sender5 * COLS_PER_DEV + col_set, full_shape)
    p_row = row_glob[group5, row_slot]
    p_col = col_union[col_pos]
    plist_all = jnp.stack([p_row, p_col], axis=-1).reshape(ROW_GROUPS, K_DEVICES, K_DEVICES, CAP_DEST, 2)
    step_ids = jnp.arange(K_PER_ROW)
    group6 = group5[..., None]
    source6 = source5[..., None]
    row6 = row_slot[..., None]
    a_slot = a_order[group6, source6, row6 * K_PER_ROW + step_ids]
    k_slot = (band_start[group6, source6, row6] + step_ids) % K_ACTIVE
    b_slot = b_order[source6, k_slot * COL_TOUCH + local_col[..., None]]
    pair_all = jnp.stack([a_slot, b_slot], axis=-1).reshape(ROW_GROUPS, K_DEVICES, K_DEVICES, CAP_DEST, K_PER_ROW, 2)
    reorder = (group_ids[:, None, None, None], dev_ids[None, :, None, None], dev_ids[None, None, :, None], p_order)
    plist_idx = plist_all[reorder].reshape(ROW_GROUPS, K_DEVICES, CAP_PART, 2)
    pairs = pair_all[reorder].reshape(ROW_GROUPS, K_DEVICES, CAP_PART, K_PER_ROW, 2)
    return pairs.astype(jnp.int32), plist_idx.astype(jnp.int32), c_idx.astype(jnp.int32)


def setup_inputs(seed: int = 0, part: int = 0) -> dict:
    base_key = jax.random.fold_in(jax.random.key(seed), part)
    index_key, a_key, b_key = jax.random.split(base_key, 3)
    pairs, plist_idx, c_idx = draw_indices(index_key)
    a_scale = (BLOCK_SIZE * K_PER_ROW * SENDERS) ** -0.5
    a_vals = (jax.random.normal(a_key, (ROW_GROUPS, K_DEVICES, CAP_A, BLOCK_SIZE, BLOCK_SIZE), jnp.float32) * a_scale).astype(jnp.bfloat16)
    b_vals = jax.random.normal(b_key, (K_DEVICES, CAP_B, BLOCK_SIZE, BLOCK_SIZE), jnp.float32).astype(jnp.bfloat16)
    return {'a_vals': a_vals, 'b_vals': b_vals, 'pairs': pairs, 'plist_idx': plist_idx, 'c_idx': c_idx}


def device_partials(a_dev, b_dev, pair_dev):
    a_sel = jnp.take(a_dev, pair_dev[:, :, 0], axis=0).astype(jnp.float32)
    b_sel = jnp.take(b_dev, pair_dev[:, :, 1], axis=0).astype(jnp.float32)
    return jnp.einsum('stab,stbc->sac', a_sel, b_sel).astype(jnp.bfloat16)


def reference(a_vals, b_vals, pairs, plist_idx, c_idx):
    flat_size = BLOCK_SIZE * BLOCK_SIZE

    def produce(device):
        group = device // K_DEVICES
        source = device % K_DEVICES
        return device_partials(a_vals[group, source], b_vals[source], pairs[group, source])

    partials = lax.map(produce, jnp.arange(ROW_GROUPS * K_DEVICES))
    partials = partials.reshape(ROW_GROUPS, K_DEVICES, K_DEVICES, CAP_DEST, flat_size)
    sent_idx = plist_idx.reshape(ROW_GROUPS, K_DEVICES, K_DEVICES, CAP_DEST, 2)

    def collect(device):
        group = device // K_DEVICES
        owner = device % K_DEVICES
        recv_vals = partials[group, :, owner].reshape(CAP_PART, flat_size).astype(jnp.float32)
        recv_idx = sent_idx[group, :, owner].reshape(CAP_PART, 2)
        hit_mask = jnp.all(c_idx[group, owner][:, None, :] == recv_idx[None, :, :], axis=-1).astype(jnp.float32)
        return jnp.dot(hit_mask, recv_vals, preferred_element_type=jnp.float32)

    c_vals = lax.map(collect, jnp.arange(ROW_GROUPS * K_DEVICES))
    return c_vals.reshape(ROW_GROUPS, K_DEVICES, CAP_C, BLOCK_SIZE, BLOCK_SIZE)
```

```python
import functools

import jax
import jax.numpy as jnp
from jax import lax
from jax.experimental import pallas as pl
from jax.experimental.pallas import tpu as pltpu
from jax.sharding import PartitionSpec as P

MESH = pl.DeviceIdType.MESH
RING = 4
HALF_CHUNKS = (4, 5, 5)


def plan(nb):
    half = sum(HALF_CHUNKS)
    quad = (nb - 4 * half) // RING
    assert 4 * half + RING * quad == nb and quad % 2 == 0
    return half, quad


def kernel(na, nb, nc, a_hbm, b_hbm, pairs_hbm, plist_hbm, cidx_hbm, out_hbm, *scratch):
    bm, bs, am, sa = scratch[0:4], scratch[4:8], scratch[8:12], scratch[12:16]
    (meta_pairs, meta_plist, cidx, tab_v, tab_s, cacc,
     loc_sem, send_sem, recv_sem, dsend, drecv, msend, mrecv, out_sem) = scratch[16:]
    half, quad = plan(nb)
    ks = lax.axis_index("ksplit")
    y = lax.axis_index("rows")
    core = ks % 2
    x = ks // 2

    def col(dx):
        return ((x + dx) % RING) * 2 + core

    sib = {"ksplit": x * 2 + (1 - core)}
    xp, xm = {"ksplit": col(1)}, {"ksplit": col(3)}
    yp, ym = {"rows": (y + 1) % RING}, {"rows": (y + 3) % RING}

    loads = [
        pltpu.make_async_copy(pairs_hbm, meta_pairs.at[0], loc_sem.at[0]),
        pltpu.make_async_copy(plist_hbm, meta_plist.at[0], loc_sem.at[1]),
        pltpu.make_async_copy(b_hbm, bm[0], loc_sem.at[2]),
        pltpu.make_async_copy(a_hbm, am[0].at[pl.ds(0, na)], loc_sem.at[3]),
        pltpu.make_async_copy(cidx_hbm, cidx, loc_sem.at[4]),
    ]
    for load in loads:
        load.start()

    barrier = pltpu.get_barrier_semaphore()
    peers = []
    for dx in range(RING):
        for flip in range(2):
            if dx or flip:
                other = core if not flip else 1 - core
                peers.append((dx, flip, {"ksplit": ((x + dx) % RING) * 2 + other}))
    for _, _, dev in peers:
        pl.semaphore_signal(barrier, inc=1, device_id=dev, device_id_type=MESH)
    for dev in (yp, ym):
        pl.semaphore_signal(barrier, inc=1, device_id=dev, device_id_type=MESH)
    zero = jnp.zeros(am[0].shape[1:], am[0].dtype)
    for ref in (*am, *sa):
        ref[na] = zero
    pl.semaphore_wait(barrier, len(peers) + 2)

    loads[0].wait()
    loads[1].wait()
    meta = []
    for dx, flip, dev in peers:
        slot = ((RING - dx) % RING) * 2 + flip
        for n, buf in enumerate((meta_pairs, meta_plist)):
            copy = pltpu.make_async_remote_copy(
                src_ref=buf.at[0], dst_ref=buf.at[slot],
                send_sem=msend.at[2 * slot + n], recv_sem=mrecv.at[2 * slot + n],
                device_id=dev, device_id_type=MESH)
            copy.start()
            meta.append(copy)

    sems = {}
    sent = []

    def remote(key, src, dst, start, size, dev):
        if key not in sems:
            sems[key] = len(sems)
        n = sems[key]
        return pltpu.make_async_remote_copy(
            src_ref=src.at[pl.ds(start, size)], dst_ref=dst.at[pl.ds(start, size)],
            send_sem=send_sem.at[n], recv_sem=recv_sem.at[n],
            device_id=dev, device_id_type=MESH)

    def send(key, src, dst, start, size, dev):
        copy = remote(key, src, dst, start, size, dev)
        copy.start()
        sent.append(copy)

    def arrive(key, dst, start, size):
        remote(key, dst, dst, start, size, sib).wait_recv()

    def share_b(d, start, size):
        pltpu.make_async_remote_copy(
            src_ref=bm[d].at[pl.ds(start, size)], dst_ref=bs[d].at[pl.ds(start, size)],
            send_sem=dsend.at[d], recv_sem=drecv.at[d], device_id=sib, device_id_type=MESH).start()

    def share_a(d, start, size):
        pltpu.make_async_remote_copy(
            src_ref=am[d].at[pl.ds(start, size)], dst_ref=sa[d].at[pl.ds(start, size)],
            send_sem=dsend.at[4 + d], recv_sem=drecv.at[4 + d], device_id=sib, device_id_type=MESH).start()

    offs, spot = [], 0
    for size in HALF_CHUNKS:
        offs.append((spot, size))
        spot += size
    mine = (y % 2) * (2 * half)
    theirs = (1 - y % 2) * (2 * half)

    def quad_at(dy):
        return 4 * half + ((y + dy) % RING) * quad

    qh = quad // 2
    nk = len(offs)
    ah = na // 2

    loads[2].wait()
    for k, (off, size) in enumerate(offs):
        u, v = mine + off, mine + half + off
        send(("x+", "u", k), bm[0], bm[3], u, size, xp)
        send(("x-", "v", k), bm[0], bm[1], v, size, xm)
        send(("x+", "v", k), bm[0], bm[3], v, size, xp)
        send(("x-", "u", k), bm[0], bm[1], u, size, xm)
    send(("x+", "w"), bm[0], bm[3], quad_at(0), quad, xp)
    send(("x-", "w"), bm[0], bm[1], quad_at(0), quad, xm)
    share_b(0, 0, nb)
    loads[3].wait()
    share_a(0, 0, na)

    loads[4].wait()
    for copy in meta:
        copy.wait_recv()
    npart = meta_plist.shape[2]
    ckey = cidx[0:1, :] * 4096 + cidx[1:2, :]
    eye = lax.broadcasted_iota(jnp.int32, (nc, nc), 0) == lax.broadcasted_iota(jnp.int32, (nc, nc), 1)
    ccol = jnp.sum(jnp.where(eye, jnp.broadcast_to(ckey, (nc, nc)), 0), axis=1, keepdims=True)
    lane = lax.broadcasted_iota(jnp.int32, (nc, 128), 1)
    table = jnp.zeros((nc, 128), jnp.int32)
    for slot in range(2 * RING):
        pkey = meta_plist[slot, 0:1, :] * 4096 + meta_plist[slot, 1:2, :]
        pval = meta_pairs[slot, 0:1, :] * 4096 + meta_pairs[slot, 1:2, :] - na * 4096
        hit = jnp.broadcast_to(ccol, (nc, npart)) == jnp.broadcast_to(pkey, (nc, npart))
        found = jnp.sum(jnp.where(hit, jnp.broadcast_to(pval, (nc, npart)), 0), axis=1, keepdims=True) + na * 4096
        table = jnp.where(lane == 2 * slot, jnp.clip(found // 4096, 0, na), table)
        table = jnp.where(lane == 2 * slot + 1, jnp.clip(found % 4096, 0, nb - 1), table)
    tab_v[...] = table
    tab_copy = pltpu.make_async_copy(tab_v, tab_s, loc_sem.at[5])
    tab_copy.start()

    def y_send(tag, d, start, size, plus=True, minus=True):
        if plus:
            send(("y+", d) + tag, bm[d], bm[d], start, size, yp)
        if minus:
            send(("y-", d) + tag, bm[d], bm[d], start, size, ym)

    def y_arrivals(d, k):
        off, size = offs[k]
        arrive(("y+", d, "u", k), bm[d], theirs + off, size)
        share_b(d, theirs + off, size)
        arrive(("y-", d, "v", k), bm[d], theirs + half + off, size)
        share_b(d, theirs + half + off, size)

    for k, (off, size) in enumerate(offs):
        u, v = mine + off, mine + half + off
        arrive(("x+", "u", k), bm[3], u, size)
        y_send(("u", k), 3, u, size, minus=False)
        send(("f+", "u", k), bm[3], bm[2], u, size, xp)
        share_b(3, u, size)
        arrive(("x-", "v", k), bm[1], v, size)
        y_send(("v", k), 1, v, size, plus=False)
        send(("f-", "v", k), bm[1], bm[2], v, size, xm)
        share_b(1, v, size)
        arrive(("x+", "v", k), bm[3], v, size)
        y_send(("v", k), 3, v, size, plus=False)
        share_b(3, v, size)
        arrive(("x-", "u", k), bm[1], u, size)
        y_send(("u", k), 1, u, size, minus=False)
        share_b(1, u, size)
        if k:
            y_arrivals(3, k - 1)
            y_arrivals(1, k - 1)
    q0 = quad_at(0)
    arrive(("x+", "w"), bm[3], q0, quad)
    y_send(("w",), 3, q0, quad)
    send(("f+", "w"), bm[3], bm[2], q0, qh, xp)
    arrive(("x-", "w"), bm[1], q0, quad)
    y_send(("w",), 1, q0, quad)
    send(("f-", "w"), bm[1], bm[2], q0 + qh, qh, xm)
    for part in range(2):
        send(("x+", "a", part), am[0], am[3], part * ah, ah, xp)
        send(("x-", "a", 1 - part), am[0], am[1], (1 - part) * ah, ah, xm)
    share_b(3, q0, quad)
    share_b(1, q0, quad)
    y_arrivals(3, nk - 1)
    y_arrivals(1, nk - 1)

    for k, (off, size) in enumerate(offs):
        u, v = mine + off, mine + half + off
        arrive(("f+", "u", k), bm[2], u, size)
        y_send(("u", k), 2, u, size, minus=False)
        share_b(2, u, size)
        arrive(("f-", "v", k), bm[2], v, size)
        y_send(("v", k), 2, v, size, plus=False)
        share_b(2, v, size)
        if k == 0:
            for d in (3, 1):
                qm, qp = quad_at(3), quad_at(1)
                arrive(("y+", d, "w"), bm[d], qm, quad)
                send(("g+", d), bm[d], bm[d], qm, qh, yp)
                share_b(d, qm, quad)
                arrive(("y-", d, "w"), bm[d], qp, quad)
                send(("g-", d), bm[d], bm[d], qp + qh, qh, ym)
                share_b(d, qp, quad)
        else:
            y_arrivals(2, k - 1)
    arrive(("f+", "w"), bm[2], q0, qh)
    y_send(("w", 0), 2, q0, qh)
    arrive(("f-", "w"), bm[2], q0 + qh, qh)
    y_send(("w", 1), 2, q0 + qh, qh)
    share_b(2, q0, quad)

    def wait_b(d):
        pltpu.make_async_copy(bs[d], bs[d], drecv.at[d]).wait()

    def wait_a(d):
        view = sa[d].at[pl.ds(0, na)]
        pltpu.make_async_copy(view, view, drecv.at[4 + d]).wait()

    size = cacc.shape[1]

    def stage(d, first=False, last=False):
        blank = jnp.zeros((size, size), bm[0].dtype)
        group = 4

        def body(step, carry):
            for sub in range(group):
                c = step * group + sub
                lhs = jnp.concatenate([am[d][tab_s[c, 4 * d]], sa[d][tab_s[c, 4 * d + 2]]], axis=1)
                rhs = jnp.concatenate([
                    jnp.concatenate([bm[d][tab_s[c, 4 * d + 1]], blank], axis=1),
                    jnp.concatenate([blank, bs[d][tab_s[c, 4 * d + 3]]], axis=1)], axis=0)
                prod = jnp.dot(lhs, rhs, preferred_element_type=jnp.float32)
                prod = prod.astype(jnp.bfloat16).astype(jnp.float32)
                total = prod[:, :size] + prod[:, size:]
                cacc[c] = total if first else cacc[c] + total
            return carry

        if not last:
            lax.fori_loop(0, nc // group, body, 0)
            return []
        outs = []
        per = nc // 6
        for n in range(6):
            lax.fori_loop(n * per // group, (n + 1) * per // group, body, 0)
            view = pl.ds(n * per, per)
            copy = pltpu.make_async_copy(cacc.at[view], out_hbm.at[view], out_sem.at[n])
            copy.start()
            outs.append(copy)
        return outs

    tab_copy.wait()
    wait_b(0)
    wait_a(0)
    stage(0, first=True)

    for d in (3, 1):
        far = quad_at(2)
        arrive(("g+", d), bm[d], far, qh)
        arrive(("g-", d), bm[d], far + qh, qh)
        share_b(d, far, quad)
    arrive(("x+", "a", 0), am[3], 0, ah)
    send(("f+", "a"), am[3], am[2], 0, ah, xp)
    share_a(3, 0, ah)
    arrive(("x-", "a", 1), am[1], ah, ah)
    send(("f-", "a"), am[1], am[2], ah, ah, xm)
    share_a(1, ah, ah)
    y_arrivals(2, nk - 1)
    arrive(("x+", "a", 1), am[3], ah, ah)
    share_a(3, ah, ah)
    arrive(("x-", "a", 0), am[1], 0, ah)
    share_a(1, 0, ah)

    qm, qp, far = quad_at(3), quad_at(1), quad_at(2)
    arrive(("y+", 2, "w", 0), bm[2], qm, qh)
    send(("g+", 2), bm[2], bm[2], qm, qh, yp)
    arrive(("y-", 2, "w", 1), bm[2], qp + qh, qh)
    send(("g-", 2), bm[2], bm[2], qp + qh, qh, ym)
    arrive(("y+", 2, "w", 1), bm[2], qm + qh, qh)
    share_b(2, qm, quad)
    arrive(("y-", 2, "w", 0), bm[2], qp, qh)
    share_b(2, qp, quad)

    for d in (3, 1):
        wait_b(d)
        wait_a(d)
        stage(d)

    arrive(("g+", 2), bm[2], far, qh)
    arrive(("g-", 2), bm[2], far + qh, qh)
    share_b(2, far, quad)
    arrive(("f+", "a"), am[2], 0, ah)
    share_a(2, 0, ah)
    arrive(("f-", "a"), am[2], ah, ah)
    share_a(2, ah, ah)
    wait_b(2)
    wait_a(2)
    outs = stage(2, last=True)

    for copy in sent:
        copy.wait_send()
    for copy in meta:
        copy.wait_send()
    for d in range(RING):
        pltpu.make_async_copy(bm[d], bm[d], dsend.at[d]).wait()
        view = am[d].at[pl.ds(0, na)]
        pltpu.make_async_copy(view, view, dsend.at[4 + d]).wait()
    for copy in outs:
        copy.wait()


def solution(mesh):
    row_spec = P(('batch', 'rows'), 'ksplit')
    col_spec = P(('batch', 'ksplit'))
    assert mesh.shape['rows'] == RING and mesh.shape['ksplit'] == 2 * RING

    def device_step(a_loc, b_loc, pair_loc, plist_loc, cidx_loc):
        a, b = a_loc[0, 0], b_loc[0]
        pairs = pair_loc[0, 0, :, 0, :].T
        plist = plist_loc[0, 0].T
        cidx = cidx_loc[0, 0].T
        na, nb, nc, size = a.shape[0], b.shape[0], cidx.shape[1], a.shape[-1]
        npart = plist.shape[1]
        nsem = 80
        block = (size, size)
        any_spec = pl.BlockSpec(memory_space=pl.ANY)
        out = pl.pallas_call(
            functools.partial(kernel, na, nb, nc),
            out_shape=jax.ShapeDtypeStruct((nc, *block), jnp.float32),
            in_specs=[pl.BlockSpec(memory_space=pltpu.HBM)] * 5,
            out_specs=any_spec,
            scratch_shapes=[
                *[pltpu.VMEM((nb, *block), b.dtype) for _ in range(2 * RING)],
                *[pltpu.VMEM((na + 1, *block), a.dtype) for _ in range(2 * RING)],
                pltpu.VMEM((2 * RING, 2, npart), jnp.int32),
                pltpu.VMEM((2 * RING, 2, npart), jnp.int32),
                pltpu.VMEM((2, nc), jnp.int32),
                pltpu.VMEM((nc, 128), jnp.int32),
                pltpu.SMEM((nc, 128), jnp.int32),
                pltpu.VMEM((nc, *block), jnp.float32),
                pltpu.SemaphoreType.DMA((6,)),
                pltpu.SemaphoreType.DMA((nsem,)),
                pltpu.SemaphoreType.DMA((nsem,)),
                pltpu.SemaphoreType.DMA((2 * RING,)),
                pltpu.SemaphoreType.DMA((2 * RING,)),
                pltpu.SemaphoreType.DMA((4 * RING,)),
                pltpu.SemaphoreType.DMA((4 * RING,)),
                pltpu.SemaphoreType.DMA((6,)),
            ],
            compiler_params=pltpu.CompilerParams(
                collective_id=0, has_side_effects=True, vmem_limit_bytes=40 * 2**20),
        )(a, b, pairs, plist, cidx)
        return out[None, None]

    return jax.shard_map(device_step, mesh=mesh, in_specs=(row_spec, col_spec, row_spec, row_spec, row_spec), out_specs=row_spec, check_vma=False)
```

```python
import functools

import jax
import jax.numpy as jnp
from jax import lax
from jax.experimental import pallas as pl
from jax.experimental.pallas import tpu as pltpu
from jax.sharding import PartitionSpec as P

MESH = pl.DeviceIdType.MESH
RING = 4
HALF_CHUNKS = (4, 5, 5)
GROUP = 12


def plan(nb):
    half = sum(HALF_CHUNKS)
    quad = (nb - 4 * half) // RING
    assert 4 * half + RING * quad == nb and quad % 2 == 0
    return half, quad


def kernel(na, nb, nc, a_hbm, b_hbm, pairs_hbm, plist_hbm, cidx_hbm, out_hbm, *scratch):
    bm, bs, am, sa = scratch[0:4], scratch[4:8], scratch[8:12], scratch[12:16]
    (meta_pairs, meta_plist, cidx, tab_v, tab_s, cacc,
     loc_sem, send_sem, recv_sem, dsend, drecv, msend, mrecv, out_sem) = scratch[16:]
    half, quad = plan(nb)
    ks = lax.axis_index("ksplit")
    y = lax.axis_index("rows")
    core = ks % 2
    x = ks // 2

    def col(dx):
        return ((x + dx) % RING) * 2 + core

    sib = {"ksplit": x * 2 + (1 - core)}
    xp, xm = {"ksplit": col(1)}, {"ksplit": col(3)}
    yp, ym = {"rows": (y + 1) % RING}, {"rows": (y + 3) % RING}

    loads = [
        pltpu.make_async_copy(pairs_hbm, meta_pairs.at[0], loc_sem.at[0]),
        pltpu.make_async_copy(plist_hbm, meta_plist.at[0], loc_sem.at[1]),
        pltpu.make_async_copy(b_hbm, bm[0], loc_sem.at[2]),
        pltpu.make_async_copy(a_hbm, am[0].at[pl.ds(0, na)], loc_sem.at[3]),
        pltpu.make_async_copy(cidx_hbm, cidx, loc_sem.at[4]),
    ]
    for load in loads:
        load.start()

    barrier = pltpu.get_barrier_semaphore()
    peers = []
    for dx in range(RING):
        for flip in range(2):
            if dx or flip:
                other = core if not flip else 1 - core
                peers.append((dx, flip, {"ksplit": ((x + dx) % RING) * 2 + other}))
    for _, _, dev in peers:
        pl.semaphore_signal(barrier, inc=1, device_id=dev, device_id_type=MESH)
    for dev in (yp, ym):
        pl.semaphore_signal(barrier, inc=1, device_id=dev, device_id_type=MESH)
    zero = jnp.zeros(am[0].shape[1:], am[0].dtype)
    for ref in (*am, *sa):
        ref[na] = zero
    pl.semaphore_wait(barrier, len(peers) + 2)

    loads[0].wait()
    loads[1].wait()
    meta = []
    for dx, flip, dev in peers:
        slot = ((RING - dx) % RING) * 2 + flip
        for n, buf in enumerate((meta_pairs, meta_plist)):
            copy = pltpu.make_async_remote_copy(
                src_ref=buf.at[0], dst_ref=buf.at[slot],
                send_sem=msend.at[2 * slot + n], recv_sem=mrecv.at[2 * slot + n],
                device_id=dev, device_id_type=MESH)
            copy.start()
            meta.append(copy)

    sems = {}
    sent = []

    def remote(key, src, dst, start, size, dev):
        if key not in sems:
            sems[key] = len(sems)
        n = sems[key]
        return pltpu.make_async_remote_copy(
            src_ref=src.at[pl.ds(start, size)], dst_ref=dst.at[pl.ds(start, size)],
            send_sem=send_sem.at[n], recv_sem=recv_sem.at[n],
            device_id=dev, device_id_type=MESH)

    def send(key, src, dst, start, size, dev):
        copy = remote(key, src, dst, start, size, dev)
        copy.start()
        sent.append(copy)

    def arrive(key, dst, start, size):
        remote(key, dst, dst, start, size, sib).wait_recv()

    def share_b(d, start, size):
        pltpu.make_async_remote_copy(
            src_ref=bm[d].at[pl.ds(start, size)], dst_ref=bs[d].at[pl.ds(start, size)],
            send_sem=dsend.at[d], recv_sem=drecv.at[d], device_id=sib, device_id_type=MESH).start()

    def share_a(d, start, size):
        pltpu.make_async_remote_copy(
            src_ref=am[d].at[pl.ds(start, size)], dst_ref=sa[d].at[pl.ds(start, size)],
            send_sem=dsend.at[4 + d], recv_sem=drecv.at[4 + d], device_id=sib, device_id_type=MESH).start()

    offs, spot = [], 0
    for size in HALF_CHUNKS:
        offs.append((spot, size))
        spot += size
    mine = (y % 2) * (2 * half)
    theirs = (1 - y % 2) * (2 * half)

    def quad_at(dy):
        return 4 * half + ((y + dy) % RING) * quad

    qh = quad // 2
    nk = len(offs)
    ah = na // 2

    loads[2].wait()
    for k, (off, size) in enumerate(offs):
        u, v = mine + off, mine + half + off
        send(("x+", "u", k), bm[0], bm[3], u, size, xp)
        send(("x-", "v", k), bm[0], bm[1], v, size, xm)
        send(("x+", "v", k), bm[0], bm[3], v, size, xp)
        send(("x-", "u", k), bm[0], bm[1], u, size, xm)
    send(("x+", "w"), bm[0], bm[3], quad_at(0), quad, xp)
    send(("x-", "w"), bm[0], bm[1], quad_at(0), quad, xm)
    share_b(0, 0, nb)
    loads[3].wait()
    share_a(0, 0, na)

    loads[4].wait()
    for copy in meta:
        copy.wait_recv()
    npart = meta_plist.shape[2]
    ckey = cidx[0:1, :] * 4096 + cidx[1:2, :]
    eye = lax.broadcasted_iota(jnp.int32, (nc, nc), 0) == lax.broadcasted_iota(jnp.int32, (nc, nc), 1)
    ccol = jnp.sum(jnp.where(eye, jnp.broadcast_to(ckey, (nc, nc)), 0), axis=1, keepdims=True)
    lane = lax.broadcasted_iota(jnp.int32, (nc, 128), 1)
    table = jnp.zeros((nc, 128), jnp.int32)
    for slot in range(2 * RING):
        pkey = meta_plist[slot, 0:1, :] * 4096 + meta_plist[slot, 1:2, :]
        pval = meta_pairs[slot, 0:1, :] * 4096 + meta_pairs[slot, 1:2, :] - na * 4096
        hit = jnp.broadcast_to(ccol, (nc, npart)) == jnp.broadcast_to(pkey, (nc, npart))
        found = jnp.sum(jnp.where(hit, jnp.broadcast_to(pval, (nc, npart)), 0), axis=1, keepdims=True) + na * 4096
        table = jnp.where(lane == 2 * slot, jnp.clip(lax.shift_right_arithmetic(found, 12), 0, na), table)
        table = jnp.where(lane == 2 * slot + 1, jnp.clip(found & 4095, 0, nb - 1), table)
    tab_v[...] = table
    tab_copy = pltpu.make_async_copy(tab_v, tab_s, loc_sem.at[5])
    tab_copy.start()

    def y_send(tag, d, start, size, plus=True, minus=True):
        if plus:
            send(("y+", d) + tag, bm[d], bm[d], start, size, yp)
        if minus:
            send(("y-", d) + tag, bm[d], bm[d], start, size, ym)

    def y_arrivals(d, k):
        off, size = offs[k]
        arrive(("y+", d, "u", k), bm[d], theirs + off, size)
        share_b(d, theirs + off, size)
        arrive(("y-", d, "v", k), bm[d], theirs + half + off, size)
        share_b(d, theirs + half + off, size)

    for k, (off, size) in enumerate(offs):
        u, v = mine + off, mine + half + off
        arrive(("x+", "u", k), bm[3], u, size)
        y_send(("u", k), 3, u, size, minus=False)
        send(("f+", "u", k), bm[3], bm[2], u, size, xp)
        share_b(3, u, size)
        arrive(("x-", "v", k), bm[1], v, size)
        y_send(("v", k), 1, v, size, plus=False)
        send(("f-", "v", k), bm[1], bm[2], v, size, xm)
        share_b(1, v, size)
        arrive(("x+", "v", k), bm[3], v, size)
        y_send(("v", k), 3, v, size, plus=False)
        share_b(3, v, size)
        arrive(("x-", "u", k), bm[1], u, size)
        y_send(("u", k), 1, u, size, minus=False)
        share_b(1, u, size)
        if k:
            y_arrivals(3, k - 1)
            y_arrivals(1, k - 1)
    q0 = quad_at(0)
    arrive(("x+", "w"), bm[3], q0, quad)
    y_send(("w",), 3, q0, quad)
    send(("f+", "w"), bm[3], bm[2], q0, qh, xp)
    arrive(("x-", "w"), bm[1], q0, quad)
    y_send(("w",), 1, q0, quad)
    send(("f-", "w"), bm[1], bm[2], q0 + qh, qh, xm)
    for part in range(2):
        send(("x+", "a", part), am[0], am[3], part * ah, ah, xp)
        send(("x-", "a", 1 - part), am[0], am[1], (1 - part) * ah, ah, xm)
    share_b(3, q0, quad)
    share_b(1, q0, quad)
    y_arrivals(3, nk - 1)
    y_arrivals(1, nk - 1)

    for k, (off, size) in enumerate(offs):
        u, v = mine + off, mine + half + off
        arrive(("f+", "u", k), bm[2], u, size)
        y_send(("u", k), 2, u, size, minus=False)
        share_b(2, u, size)
        arrive(("f-", "v", k), bm[2], v, size)
        y_send(("v", k), 2, v, size, plus=False)
        share_b(2, v, size)
        if k == 0:
            for d in (3, 1):
                qm, qp = quad_at(3), quad_at(1)
                arrive(("y+", d, "w"), bm[d], qm, quad)
                send(("g+", d), bm[d], bm[d], qm, qh, yp)
                share_b(d, qm, quad)
                arrive(("y-", d, "w"), bm[d], qp, quad)
                send(("g-", d), bm[d], bm[d], qp + qh, qh, ym)
                share_b(d, qp, quad)
        else:
            y_arrivals(2, k - 1)
    arrive(("f+", "w"), bm[2], q0, qh)
    y_send(("w", 0), 2, q0, qh)
    arrive(("f-", "w"), bm[2], q0 + qh, qh)
    y_send(("w", 1), 2, q0 + qh, qh)
    share_b(2, q0, quad)

    def wait_b(d):
        pltpu.make_async_copy(bs[d], bs[d], drecv.at[d]).wait()

    def wait_a(d):
        view = sa[d].at[pl.ds(0, na)]
        pltpu.make_async_copy(view, view, drecv.at[4 + d]).wait()

    size = cacc.shape[1]

    def stage(d, first=False, last=False):
        blank = jnp.zeros((size, size), bm[0].dtype)
        group = GROUP

        def body(step, carry):
            for sub in range(group):
                c = step * group + sub
                lhs = jnp.concatenate([am[d][tab_s[c, 4 * d]], sa[d][tab_s[c, 4 * d + 2]]], axis=1)
                rhs = jnp.concatenate([
                    jnp.concatenate([bm[d][tab_s[c, 4 * d + 1]], blank], axis=1),
                    jnp.concatenate([blank, bs[d][tab_s[c, 4 * d + 3]]], axis=1)], axis=0)
                prod = jnp.dot(lhs, rhs, preferred_element_type=jnp.float32)
                prod = prod.astype(jnp.bfloat16).astype(jnp.float32)
                total = prod[:, :size] + prod[:, size:]
                cacc[c] = total if first else cacc[c] + total
            return carry

        if not last:
            lax.fori_loop(0, nc // group, body, 0)
            return []
        outs = []
        per = nc // 6
        for n in range(6):
            lax.fori_loop(n * per // group, (n + 1) * per // group, body, 0)
            view = pl.ds(n * per, per)
            copy = pltpu.make_async_copy(cacc.at[view], out_hbm.at[view], out_sem.at[n])
            copy.start()
            outs.append(copy)
        return outs

    tab_copy.wait()
    wait_b(0)
    wait_a(0)
    stage(0, first=True)

    for d in (3, 1):
        far = quad_at(2)
        arrive(("g+", d), bm[d], far, qh)
        arrive(("g-", d), bm[d], far + qh, qh)
        share_b(d, far, quad)
    arrive(("x+", "a", 0), am[3], 0, ah)
    send(("f+", "a"), am[3], am[2], 0, ah, xp)
    share_a(3, 0, ah)
    arrive(("x-", "a", 1), am[1], ah, ah)
    send(("f-", "a"), am[1], am[2], ah, ah, xm)
    share_a(1, ah, ah)
    y_arrivals(2, nk - 1)
    arrive(("x+", "a", 1), am[3], ah, ah)
    share_a(3, ah, ah)
    arrive(("x-", "a", 0), am[1], 0, ah)
    share_a(1, 0, ah)

    qm, qp, far = quad_at(3), quad_at(1), quad_at(2)
    arrive(("y+", 2, "w", 0), bm[2], qm, qh)
    send(("g+", 2), bm[2], bm[2], qm, qh, yp)
    arrive(("y-", 2, "w", 1), bm[2], qp + qh, qh)
    send(("g-", 2), bm[2], bm[2], qp + qh, qh, ym)
    arrive(("y+", 2, "w", 1), bm[2], qm + qh, qh)
    share_b(2, qm, quad)
    arrive(("y-", 2, "w", 0), bm[2], qp, qh)
    share_b(2, qp, quad)

    for d in (3, 1):
        wait_b(d)
        wait_a(d)
        stage(d)

    arrive(("g+", 2), bm[2], far, qh)
    arrive(("g-", 2), bm[2], far + qh, qh)
    share_b(2, far, quad)
    arrive(("f+", "a"), am[2], 0, ah)
    share_a(2, 0, ah)
    arrive(("f-", "a"), am[2], ah, ah)
    share_a(2, ah, ah)
    wait_b(2)
    wait_a(2)
    outs = stage(2, last=True)

    for copy in sent:
        copy.wait_send()
    for copy in meta:
        copy.wait_send()
    for d in range(RING):
        pltpu.make_async_copy(bm[d], bm[d], dsend.at[d]).wait()
        view = am[d].at[pl.ds(0, na)]
        pltpu.make_async_copy(view, view, dsend.at[4 + d]).wait()
    for copy in outs:
        copy.wait()


def solution(mesh):
    row_spec = P(('batch', 'rows'), 'ksplit')
    col_spec = P(('batch', 'ksplit'))
    assert mesh.shape['rows'] == RING and mesh.shape['ksplit'] == 2 * RING

    def device_step(a_loc, b_loc, pair_loc, plist_loc, cidx_loc):
        a, b = a_loc[0, 0], b_loc[0]
        pairs = pair_loc[0, 0, :, 0, :].T
        plist = plist_loc[0, 0].T
        cidx = cidx_loc[0, 0].T
        na, nb, nc, size = a.shape[0], b.shape[0], cidx.shape[1], a.shape[-1]
        npart = plist.shape[1]
        nsem = 80
        block = (size, size)
        any_spec = pl.BlockSpec(memory_space=pl.ANY)
        out = pl.pallas_call(
            functools.partial(kernel, na, nb, nc),
            out_shape=jax.ShapeDtypeStruct((nc, *block), jnp.float32),
            in_specs=[pl.BlockSpec(memory_space=pltpu.HBM)] * 5,
            out_specs=any_spec,
            scratch_shapes=[
                *[pltpu.VMEM((nb, *block), b.dtype) for _ in range(2 * RING)],
                *[pltpu.VMEM((na + 1, *block), a.dtype) for _ in range(2 * RING)],
                pltpu.VMEM((2 * RING, 2, npart), jnp.int32),
                pltpu.VMEM((2 * RING, 2, npart), jnp.int32),
                pltpu.VMEM((2, nc), jnp.int32),
                pltpu.VMEM((nc, 128), jnp.int32),
                pltpu.SMEM((nc, 128), jnp.int32),
                pltpu.VMEM((nc, *block), jnp.float32),
                pltpu.SemaphoreType.DMA((6,)),
                pltpu.SemaphoreType.DMA((nsem,)),
                pltpu.SemaphoreType.DMA((nsem,)),
                pltpu.SemaphoreType.DMA((2 * RING,)),
                pltpu.SemaphoreType.DMA((2 * RING,)),
                pltpu.SemaphoreType.DMA((4 * RING,)),
                pltpu.SemaphoreType.DMA((4 * RING,)),
                pltpu.SemaphoreType.DMA((6,)),
            ],
            compiler_params=pltpu.CompilerParams(
                collective_id=0, has_side_effects=True, vmem_limit_bytes=67043328),
        )(a, b, pairs, plist, cidx)
        return out[None, None]

    return jax.shard_map(device_step, mesh=mesh, in_specs=(row_spec, col_spec, row_spec, row_spec, row_spec), out_specs=row_spec, check_vma=False)
```

```python
import functools

import jax
import jax.numpy as jnp
from jax import lax
from jax.experimental import pallas as pl
from jax.experimental.pallas import tpu as pltpu
from jax.sharding import PartitionSpec as P


MESH = pl.DeviceIdType.MESH
RING = 4
HALF_CHUNKS = (2, 4, 4, 4)
GROUP = 12
LEFT, RIGHT, FAR = 3, 1, 2


def plan(nb):
    half = sum(HALF_CHUNKS)
    quad = (nb - 4 * half) // RING
    assert 4 * half + RING * quad == nb and quad % 2 == 0
    return half, quad


def kernel(na, nb, nc, a_hbm, b_hbm, pairs_hbm, plist_hbm, cidx_hbm, acc, *scratch):
    mine, twin = scratch[0:RING], scratch[RING:2 * RING]
    (meta, cidx, tab_v, tab_s, loc_sem, link_sem, recv_sem, dsend, drecv, msem) = scratch[2 * RING:]
    half, quad = plan(nb)
    nk, qh, ah = len(HALF_CHUNKS), quad // 2, na // 2
    offs = [(sum(HALF_CHUNKS[:k]), HALF_CHUNKS[k]) for k in range(nk)]
    ks = lax.axis_index("ksplit")
    y = lax.axis_index("rows")
    core = ks % 2
    x = ks // 2

    def chip(dx, flip=0):
        return {"ksplit": ((x + dx) % RING) * 2 + (1 - core if flip else core)}

    sib = chip(0, 1)
    links = {
        "x+": (0, chip(1)), "x-": (1, chip(3)),
        "y+": (2, {"rows": (y + 1) % RING}), "y-": (3, {"rows": (y + 3) % RING}),
    }
    peers = [(dx, flip) for dx in range(RING) for flip in range(2) if dx or flip]

    loads = [
        pltpu.make_async_copy(b_hbm, mine[0].at[pl.ds(0, nb)], loc_sem.at[0]),
        pltpu.make_async_copy(a_hbm, mine[0].at[pl.ds(nb, na)], loc_sem.at[1]),
        pltpu.make_async_copy(pairs_hbm, meta.at[0, 0], loc_sem.at[2]),
        pltpu.make_async_copy(plist_hbm, meta.at[0, 1], loc_sem.at[3]),
        pltpu.make_async_copy(cidx_hbm, cidx, loc_sem.at[4]),
    ]
    for load in loads:
        load.start()

    barrier = pltpu.get_barrier_semaphore()
    devices = [chip(*p) for p in peers] + [links["y+"][1], links["y-"][1]]
    for dev in devices:
        pl.semaphore_signal(barrier, inc=1, device_id=dev, device_id_type=MESH)
    zero = jnp.zeros(mine[0].shape[1:], mine[0].dtype)
    for ref in (*mine, *twin):
        ref[nb + na] = zero
    with jax.named_scope('barrier'):
        pl.semaphore_wait(barrier, len(devices))

    sems = {}
    load_of = {}
    link_of = [0] * len(links)

    def index(key):
        return sems.setdefault(key, len(sems))

    def send(link, key, src, dst, start, size):
        slot, dev = links[link]
        n = index(key)
        load_of[n] = load_of.get(n, 0) + size
        link_of[slot] += size
        pltpu.make_async_remote_copy(
            src_ref=mine[src].at[pl.ds(start, size)], dst_ref=mine[dst].at[pl.ds(start, size)],
            send_sem=link_sem.at[slot], recv_sem=recv_sem.at[n],
            device_id=dev, device_id_type=MESH).start()

    def take(size, sem):
        view = mine[0].at[pl.ds(0, size)]
        pltpu.make_async_copy(view, view, sem).wait()

    waited = {}

    def arrive(key, size):
        n = index(key)
        waited[n] = waited.get(n, 0) + size
        with jax.named_scope('_'.join(str(t) for t in key).replace('+', 'p').replace('-', 'm').replace(' ', '')):
            take(size, recv_sem.at[n])

    def share(d, start, size):
        pltpu.make_async_remote_copy(
            src_ref=mine[d].at[pl.ds(start, size)], dst_ref=twin[d].at[pl.ds(start, size)],
            send_sem=dsend.at[d], recv_sem=drecv.at[d], device_id=sib, device_id_type=MESH).start()

    own = (y % 2) * (2 * half)
    theirs = (1 - y % 2) * (2 * half)

    def quad_at(dy):
        return 4 * half + ((y + dy) % RING) * quad

    def lay(k, base):
        off, size = offs[k]
        return base + off, base + half + off, size

    loads[0].wait()
    for k in range(nk):
        u, v, size = lay(k, own)
        send("x+", ("x+", "u", k), 0, LEFT, u, size)
        send("x-", ("x-", "v", k), 0, RIGHT, v, size)
        send("x+", ("x+", "v", k), 0, LEFT, v, size)
        send("x-", ("x-", "u", k), 0, RIGHT, u, size)
        if k == 0:
            loads[2].wait()
            loads[3].wait()
            for dx, flip in peers:
                slot = ((RING - dx) % RING) * 2 + flip
                pltpu.make_async_remote_copy(
                    src_ref=meta.at[0], dst_ref=meta.at[slot],
                    send_sem=msem.at[0], recv_sem=msem.at[1],
                    device_id=chip(dx, flip), device_id_type=MESH).start()
    send("x+", ("x+", "w"), 0, LEFT, quad_at(0), quad)
    send("x-", ("x-", "w"), 0, RIGHT, quad_at(0), quad)
    loads[1].wait()

    def build_table():
      with jax.named_scope('table'):
            loads[4].wait()
            others = meta.at[pl.ds(1, 2 * RING - 1)]
            pltpu.make_async_copy(others, others, msem.at[1]).wait()
            npart = meta.shape[3]
            ckey = cidx[0:1, :] * 4096 + cidx[1:2, :]
            eye = lax.broadcasted_iota(jnp.int32, (nc, nc), 0) == lax.broadcasted_iota(jnp.int32, (nc, nc), 1)
            ccol = jnp.sum(jnp.where(eye, jnp.broadcast_to(ckey, (nc, nc)), 0), axis=1, keepdims=True)
            lane = lax.broadcasted_iota(jnp.int32, (nc, 128), 1)
            table = jnp.zeros((nc, 128), jnp.int32)
            for slot in range(2 * RING):
                pkey = meta[slot, 1, 0:1, :] * 4096 + meta[slot, 1, 1:2, :]
                pval = meta[slot, 0, 0:1, :] * 4096 + meta[slot, 0, 1:2, :] - na * 4096
                hit = jnp.broadcast_to(ccol, (nc, npart)) == jnp.broadcast_to(pkey, (nc, npart))
                found = jnp.sum(jnp.where(hit, jnp.broadcast_to(pval, (nc, npart)), 0), axis=1, keepdims=True) + na * 4096
                a_at = nb + jnp.clip(lax.shift_right_arithmetic(found, 12), 0, na)
                b_at = jnp.clip(found & 4095, 0, nb - 1)
                table = jnp.where(lane == 2 * slot, a_at, table)
                table = jnp.where(lane == 2 * slot + 1, b_at, table)
            tab_v[...] = table
            pltpu.make_async_copy(tab_v, tab_s, loc_sem.at[5]).start()

    size_c = acc.shape[1]
    blank = jnp.zeros((size_c, size_c), mine[0].dtype)

    def stage(d, lo=0, hi=nc, first=False):
        def body(step, carry):
            for sub in range(GROUP):
                c = step * GROUP + sub
                lhs = jnp.concatenate([mine[d][tab_s[c, 4 * d]], twin[d][tab_s[c, 4 * d + 2]]], axis=1)
                rhs = jnp.concatenate([
                    jnp.concatenate([mine[d][tab_s[c, 4 * d + 1]], blank], axis=1),
                    jnp.concatenate([blank, twin[d][tab_s[c, 4 * d + 3]]], axis=1)], axis=0)
                prod = jnp.dot(lhs, rhs, preferred_element_type=jnp.float32)
                prod = prod.astype(jnp.bfloat16).astype(jnp.float32)
                total = prod[:, :size_c] + prod[:, size_c:]
                acc[c] = total if first else acc[c] + total
            return carry

        with jax.named_scope(f'stage{d}_{lo}'):
            lax.fori_loop(lo // GROUP, hi // GROUP, body, 0)

    def ready(d):
        take_twin = twin[d].at[pl.ds(0, nb + na)]
        with jax.named_scope(f'ready{d}'):
            pltpu.make_async_copy(take_twin, take_twin, drecv.at[d]).wait()

    def y_taken(cols, k):
        u, v, size = lay(k, theirs)
        arrive(("y+", cols, k), size * len(cols))
        arrive(("y-", cols, k), size * len(cols))
        for d in cols:
            share(d, u, size)
            share(d, v, size)

    near = (LEFT, RIGHT)
    third = nc // 3

    for k in range(nk):
        u, v, size = lay(k, own)
        arrive(("x+", "u", k), size)
        send("y+", ("y+", near, k), LEFT, LEFT, u, size)
        send("x+", ("f", k), LEFT, FAR, u, size)
        arrive(("x-", "v", k), size)
        send("y-", ("y-", near, k), RIGHT, RIGHT, v, size)
        send("x-", ("f", k), RIGHT, FAR, v, size)
        share(LEFT, u, size)
        share(RIGHT, v, size)
        if k == 1:
            build_table()
        elif k == 2:
            pltpu.make_async_copy(tab_v, tab_s, loc_sem.at[5]).wait()
            ready(0)
            stage(0, 0, third, first=True)
        elif k == 3:
            stage(0, 2 * third, nc, first=True)
        arrive(("x+", "v", k), size)
        send("y-", ("y-", near, k), LEFT, LEFT, v, size)
        arrive(("x-", "u", k), size)
        send("y+", ("y+", near, k), RIGHT, RIGHT, u, size)
        share(LEFT, v, size)
        share(RIGHT, u, size)
        if k == 0:
            share(0, 0, nb + na)
        elif k == 2:
            stage(0, third, 2 * third, first=True)
        if k:
            y_taken(near, k - 1)
    q0, qm, qp, qf = quad_at(0), quad_at(3), quad_at(1), quad_at(2)
    arrive(("x+", "w"), quad)
    arrive(("x-", "w"), quad)
    for d in near:
        send("y+", ("y+", near, "w"), d, d, q0, quad)
        send("y-", ("y-", near, "w"), d, d, q0, quad)
    send("x+", ("f", "w"), LEFT, FAR, q0, qh)
    send("x-", ("f", "w"), RIGHT, FAR, q0 + qh, qh)
    for part in range(2):
        send("x+", ("a", part), 0, LEFT, nb + part * ah, ah)
        send("x-", ("a", part), 0, RIGHT, nb + (1 - part) * ah, ah)
    for d in near:
        share(d, q0, quad)
    y_taken(near, nk - 1)

    def far_block(k):
        u, v, size = lay(k, own)
        arrive(("f", k), 2 * size)
        send("y+", ("y+", (FAR,), k), FAR, FAR, u, size)
        send("y-", ("y-", (FAR,), k), FAR, FAR, v, size)
        share(FAR, u, size)
        share(FAR, v, size)

    far_block(0)
    far_block(1)
    arrive(("y+", near, "w"), 2 * quad)
    for d in near:
        send("y+", ("g", near), d, d, qm, qh)
    arrive(("y-", near, "w"), 2 * quad)
    for d in near:
        send("y-", ("g", near), d, d, qp + qh, qh)
    for d in near:
        share(d, qm, quad)
        share(d, qp, quad)
    for k in range(2, nk):
        far_block(k)
    arrive(("f", "w"), 2 * qh)
    send("y+", ("y+", "w", 0), FAR, FAR, q0, qh)
    send("y-", ("y-", "w", 1), FAR, FAR, q0 + qh, qh)
    send("y+", ("yw",), FAR, FAR, q0 + qh, qh)
    send("y-", ("yw",), FAR, FAR, q0, qh)
    share(FAR, q0, quad)
    y_taken((FAR,), 0)
    y_taken((FAR,), 1)
    arrive(("g", near), 4 * qh)
    for d in near:
        share(d, qf, quad)

    arrive(("a", 0), 2 * ah)
    send("x+", ("f", "a"), LEFT, FAR, nb, ah)
    send("x-", ("f", "a"), RIGHT, FAR, nb + ah, ah)
    share(LEFT, nb, ah)
    share(RIGHT, nb + ah, ah)
    for k in range(2, nk):
        y_taken((FAR,), k)
    arrive(("a", 1), 2 * ah)
    share(LEFT, nb + ah, ah)
    share(RIGHT, nb, ah)
    arrive(("y+", "w", 0), qh)
    send("y+", ("g", FAR), FAR, FAR, qm, qh)
    arrive(("y-", "w", 1), qh)
    send("y-", ("g", FAR), FAR, FAR, qp + qh, qh)
    ready(LEFT)
    stage(LEFT)
    arrive(("yw",), 2 * qh)
    share(FAR, qm, quad)
    share(FAR, qp, quad)
    ready(RIGHT)
    stage(RIGHT, 0, nc // 2)
    arrive(("g", FAR), 2 * qh)
    share(FAR, qf, quad)
    arrive(("f", "a"), 2 * ah)
    share(FAR, nb, na)
    stage(RIGHT, nc // 2, nc)
    ready(FAR)
    stage(FAR)

    assert load_of == waited
    with jax.named_scope('sendwaits'):
        for slot, size in enumerate(link_of):
            take(size, link_sem.at[slot])
        own_meta = meta.at[pl.ds(0, 2 * RING - 1)]
        pltpu.make_async_copy(own_meta, own_meta, msem.at[0]).wait()
        for d in range(RING):
            take(nb + na, dsend.at[d])


def solution(mesh):
    row_spec = P(('batch', 'rows'), 'ksplit')
    col_spec = P(('batch', 'ksplit'))
    assert mesh.shape['rows'] == RING and mesh.shape['ksplit'] == 2 * RING

    def device_step(a_loc, b_loc, pair_loc, plist_loc, cidx_loc):
        a, b = a_loc[0, 0], b_loc[0]
        pairs = pair_loc[0, 0, :, 0, :].T
        plist = plist_loc[0, 0].T
        cidx = cidx_loc[0, 0].T
        na, nb, nc, size = a.shape[0], b.shape[0], cidx.shape[1], a.shape[-1]
        npart = plist.shape[1]
        nsem = 49
        block = (size, size)
        args = [pltpu.with_memory_space_constraint(t, pltpu.HBM) for t in (a, b, pairs, plist, cidx)]
        out = pl.pallas_call(
            functools.partial(kernel, na, nb, nc),
            out_shape=jax.ShapeDtypeStruct((nc, *block), jnp.float32),
            in_specs=[pl.BlockSpec(memory_space=pltpu.HBM)] * 5,
            out_specs=pl.BlockSpec(memory_space=pltpu.VMEM),
            scratch_shapes=[
                *[pltpu.VMEM((nb + na + 1, *block), b.dtype) for _ in range(2 * RING)],
                pltpu.VMEM((2 * RING, 2, 2, npart), jnp.int32),
                pltpu.VMEM((2, nc), jnp.int32),
                pltpu.VMEM((nc, 128), jnp.int32),
                pltpu.SMEM((nc, 128), jnp.int32),
                pltpu.SemaphoreType.DMA((6,)),
                pltpu.SemaphoreType.DMA((4,)),
                pltpu.SemaphoreType.DMA((nsem,)),
                pltpu.SemaphoreType.DMA((RING,)),
                pltpu.SemaphoreType.DMA((RING,)),
                pltpu.SemaphoreType.DMA((2,)),
            ],
            compiler_params=pltpu.CompilerParams(
                collective_id=0, has_side_effects=True, vmem_limit_bytes=30 * 2**20),
        )(*args)
        return out[None, None]

    return jax.shard_map(device_step, mesh=mesh, in_specs=(row_spec, col_spec, row_spec, row_spec, row_spec), out_specs=row_spec, check_vma=False)
```

```python
import functools

import jax
import jax.numpy as jnp
from jax import lax
from jax.experimental import pallas as pl
from jax.experimental.pallas import tpu as pltpu
from jax.sharding import PartitionSpec as P


MESH = pl.DeviceIdType.MESH
RING = 4
HALF_CHUNKS = (3, 3, 4, 4)
LEFT, RIGHT, FAR = 3, 1, 2


def plan(nb):
    half = sum(HALF_CHUNKS)
    quad = (nb - 4 * half) // RING
    assert 4 * half + RING * quad == nb and quad % 2 == 0
    return half, quad


def kernel(na, nb, nc, a_hbm, b_hbm, pairs_hbm, plist_hbm, cidx_hbm, acc, *scratch):
    mine, twin = scratch[0:RING], scratch[RING:2 * RING]
    (meta, cidx, tab_v, tab_s, loc_sem, link_sem, recv_sem, dsend, drecv, msem) = scratch[2 * RING:]
    half, quad = plan(nb)
    nk, qh, ah = len(HALF_CHUNKS), quad // 2, na // 2
    offs = [(sum(HALF_CHUNKS[:k]), HALF_CHUNKS[k]) for k in range(nk)]
    ks = lax.axis_index("ksplit")
    y = lax.axis_index("rows")
    core = ks % 2
    x = ks // 2

    def chip(dx, flip=0):
        return {"ksplit": ((x + dx) % RING) * 2 + (1 - core if flip else core)}

    sib = chip(0, 1)
    links = {
        "x+": (0, chip(1)), "x-": (1, chip(3)),
        "y+": (2, {"rows": (y + 1) % RING}), "y-": (3, {"rows": (y + 3) % RING}),
    }

    loads = [
        pltpu.make_async_copy(b_hbm, mine[0].at[pl.ds(0, nb)], loc_sem.at[0]),
        pltpu.make_async_copy(a_hbm, mine[0].at[pl.ds(nb, na)], loc_sem.at[1]),
        pltpu.make_async_copy(pairs_hbm, meta.at[0, 0], loc_sem.at[2]),
        pltpu.make_async_copy(plist_hbm, meta.at[0, 1], loc_sem.at[3]),
        pltpu.make_async_copy(cidx_hbm, cidx, loc_sem.at[4]),
    ]
    for load in loads:
        load.start()

    barrier = pltpu.get_barrier_semaphore()
    devices = [dev for _, dev in links.values()] + [chip(2), sib]
    for dev in devices:
        pl.semaphore_signal(barrier, inc=1, device_id=dev, device_id_type=MESH)
    zero = jnp.zeros(mine[0].shape[1:], mine[0].dtype)
    for ref in (*mine, *twin):
        ref[nb + na] = zero
    with jax.named_scope('barrier'):
        pl.semaphore_wait(barrier, len(devices))

    sems = {}
    load_of = {}
    link_of = [0] * len(links)

    def index(key):
        return sems.setdefault(key, len(sems))

    def send(link, key, src, dst, start, size):
        slot, dev = links[link]
        n = index(key)
        load_of[n] = load_of.get(n, 0) + size
        link_of[slot] += size
        pltpu.make_async_remote_copy(
            src_ref=mine[src].at[pl.ds(start, size)], dst_ref=mine[dst].at[pl.ds(start, size)],
            send_sem=link_sem.at[slot], recv_sem=recv_sem.at[n],
            device_id=dev, device_id_type=MESH).start()

    def take(size, sem):
        view = mine[0].at[pl.ds(0, size)]
        pltpu.make_async_copy(view, view, sem).wait()

    waited = {}

    def arrive(key, size):
        n = index(key)
        waited[n] = waited.get(n, 0) + size
        with jax.named_scope('_'.join(str(t) for t in key).replace('+', 'p').replace('-', 'm').replace(' ', '')):
            take(size, recv_sem.at[n])

    def share(d, start, size):
        pltpu.make_async_remote_copy(
            src_ref=mine[d].at[pl.ds(start, size)], dst_ref=twin[d].at[pl.ds(start, size)],
            send_sem=dsend.at[d], recv_sem=drecv.at[d], device_id=sib, device_id_type=MESH).start()

    own = (y % 2) * (2 * half)
    theirs = (1 - y % 2) * (2 * half)

    def quad_at(dy):
        return 4 * half + ((y + dy) % RING) * quad

    def lay(k, base):
        off, size = offs[k]
        return base + off, base + half + off, size

    q0, qm, qp, qf = quad_at(0), quad_at(3), quad_at(1), quad_at(2)

    loads[0].wait()
    for part in range(2):
        send("x+", ("x+", "w", part), 0, LEFT, q0 + part * qh, qh)
        send("x-", ("x-", "w", part), 0, RIGHT, q0 + (1 - part) * qh, qh)
    loads[2].wait()
    loads[3].wait()

    def list_to(slot, src, dev, sem):
        pltpu.make_async_remote_copy(
            src_ref=meta.at[src], dst_ref=meta.at[slot], send_sem=msem.at[0], recv_sem=msem.at[sem],
            device_id=dev, device_id_type=MESH).start()

    def lists_taken(count, sem):
        view = meta.at[pl.ds(0, count)]
        pltpu.make_async_copy(view, view, msem.at[sem]).wait()

    for dx in range(1, RING):
        list_to(2 * (RING - dx), 0, chip(dx), 1)
    list_to(1, 0, sib, 2)
    for k in range(nk):
        u, v, size = lay(k, own)
        send("x+", ("x+", "u", k), 0, LEFT, u, size)
        send("x-", ("x-", "v", k), 0, RIGHT, v, size)
        send("x+", ("x+", "v", k), 0, LEFT, v, size)
        send("x-", ("x-", "u", k), 0, RIGHT, u, size)
    loads[1].wait()

    def build_table():
      with jax.named_scope('table'):
            loads[4].wait()
            lists_taken(RING, 2)
            npart = meta.shape[3]
            ckey = cidx[0:1, :] * 4096 + cidx[1:2, :]
            eye = lax.broadcasted_iota(jnp.int32, (nc, nc), 0) == lax.broadcasted_iota(jnp.int32, (nc, nc), 1)
            ccol = jnp.sum(jnp.where(eye, jnp.broadcast_to(ckey, (nc, nc)), 0), axis=1, keepdims=True)
            lane = lax.broadcasted_iota(jnp.int32, (nc, 128), 1)
            table = jnp.zeros((nc, 128), jnp.int32)
            for slot in range(2 * RING):
                pkey = meta[slot, 1, 0:1, :] * 4096 + meta[slot, 1, 1:2, :]
                pval = meta[slot, 0, 0:1, :] * 4096 + meta[slot, 0, 1:2, :] - na * 4096
                hit = jnp.broadcast_to(ccol, (nc, npart)) == jnp.broadcast_to(pkey, (nc, npart))
                found = jnp.sum(jnp.where(hit, jnp.broadcast_to(pval, (nc, npart)), 0), axis=1, keepdims=True) + na * 4096
                a_at = nb + jnp.clip(lax.shift_right_arithmetic(found, 12), 0, na)
                b_at = jnp.clip(found & 4095, 0, nb - 1)
                table = jnp.where(lane == 2 * slot, a_at, table)
                table = jnp.where(lane == 2 * slot + 1, b_at, table)
            tab_v[...] = table
            pltpu.make_async_copy(tab_v, tab_s, loc_sem.at[5]).start()

    def stage(d, lo=0, hi=nc, group=24, first=False):
        def product(ref, n, c):
            p = jnp.dot(ref[tab_s[c, n]], ref[tab_s[c, n + 1]], preferred_element_type=jnp.float32)
            return p.astype(jnp.bfloat16).astype(jnp.float32)

        def body(step, carry):
            for sub in range(group):
                c = step * group + sub
                total = product(mine[d], 4 * d, c) + product(twin[d], 4 * d + 2, c)
                acc[c] = total if first else acc[c] + total
            return carry

        with jax.named_scope(f'stage{d}_{lo}'):
            lax.fori_loop(lo // group, hi // group, body, 0)

    def ready(d):
        take_twin = twin[d].at[pl.ds(0, nb + na)]
        with jax.named_scope(f'ready{d}'):
            pltpu.make_async_copy(take_twin, take_twin, drecv.at[d]).wait()

    def y_taken(cols, k):
        u, v, size = lay(k, theirs)
        arrive(("y+", cols, k), size * len(cols))
        arrive(("y-", cols, k), size * len(cols))
        for d in cols:
            share(d, u, size)
            share(d, v, size)

    near = (LEFT, RIGHT)
    third = nc // 3

    for part in range(2):
        for link, d, at in (("x+", LEFT, q0 + part * qh), ("x-", RIGHT, q0 + (1 - part) * qh)):
            arrive((link, "w", part), qh)
            send("y+", ("y+w", near), d, d, at, qh)
            send("y-", ("y-w", near), d, d, at, qh)
            if part == 0:
                send(link, ("f", "w"), d, FAR, at, qh)
        for d in near:
            share(d, q0 + (part if d == LEFT else 1 - part) * qh, qh)
    share(0, 0, nb + na)

    def spread(k):
        for d in (near if k == 0 else (FAR,)):
            send("y+", ("g", k), d, d, qm, qh)
            send("y-", ("g", k), d, d, qp + qh, qh)
            share(d, qm, quad)
            share(d, qp, quad)

    for k in range(nk):
        u, v, size = lay(k, own)
        arrive(("x+", "u", k), size)
        send("y+", ("y+", near, k), LEFT, LEFT, u, size)
        send("x+", ("f", k), LEFT, FAR, u, size)
        arrive(("x-", "v", k), size)
        send("y-", ("y-", near, k), RIGHT, RIGHT, v, size)
        send("x-", ("f", k), RIGHT, FAR, v, size)
        share(LEFT, u, size)
        share(RIGHT, v, size)
        if k == 0:
            lists_taken(RING - 1, 1)
            for d in range(1, RING):
                list_to(2 * d + 1, 2 * d, sib, 2)
        elif k == 1:
            arrive(("y+w", near), 4 * qh)
            arrive(("y-w", near), 4 * qh)
            spread(0)
        elif k == 2:
            stage(0, third, 2 * third, first=True)
            y_taken(near, 0)
        elif k == 3:
            y_taken(near, 1)
        arrive(("x+", "v", k), size)
        send("y-", ("y-", near, k), LEFT, LEFT, v, size)
        arrive(("x-", "u", k), size)
        send("y+", ("y+", near, k), RIGHT, RIGHT, u, size)
        share(LEFT, v, size)
        share(RIGHT, u, size)
        if k == 0:
            build_table()
        elif k == 1:
            pltpu.make_async_copy(tab_v, tab_s, loc_sem.at[5]).wait()
            ready(0)
            stage(0, 0, third, first=True)
        elif k == 2:
            stage(0, 2 * third, nc, first=True)
    for part in range(2):
        send("x+", ("a", part), 0, LEFT, nb + part * ah, ah)
        send("x-", ("a", part), 0, RIGHT, nb + (1 - part) * ah, ah)
    arrive(("g", 0), 4 * qh)
    for d in near:
        share(d, qf, quad)

    def far_block(k):
        u, v, size = lay(k, own)
        arrive(("f", k), 2 * size)
        send("y+", ("y+", (FAR,), k), FAR, FAR, u, size)
        send("y-", ("y-", (FAR,), k), FAR, FAR, v, size)
        share(FAR, u, size)
        share(FAR, v, size)

    arrive(("f", "w"), 2 * qh)
    send("y+", ("y+w", FAR), FAR, FAR, q0, quad)
    send("y-", ("y-w", FAR), FAR, FAR, q0, quad)
    share(FAR, q0, quad)
    y_taken(near, 2)
    far_block(0)
    far_block(1)
    y_taken(near, 3)
    far_block(2)
    arrive(("y+w", FAR), quad)
    arrive(("y-w", FAR), quad)
    spread(1)
    far_block(3)
    y_taken((FAR,), 0)

    arrive(("a", 0), 2 * ah)
    send("x+", ("f", "a"), LEFT, FAR, nb, ah)
    send("x-", ("f", "a"), RIGHT, FAR, nb + ah, ah)
    share(LEFT, nb, ah)
    share(RIGHT, nb + ah, ah)
    y_taken((FAR,), 1)
    y_taken((FAR,), 2)
    arrive(("a", 1), 2 * ah)
    share(LEFT, nb + ah, ah)
    share(RIGHT, nb, ah)
    y_taken((FAR,), 3)
    ready(LEFT)
    stage(LEFT)
    arrive(("g", 1), 2 * qh)
    share(FAR, qf, quad)
    ready(RIGHT)
    stage(RIGHT, 0, 2 * third)
    arrive(("f", "a"), 2 * ah)
    share(FAR, nb, na)
    stage(RIGHT, 2 * third, nc)
    ready(FAR)
    stage(FAR, group=nc // 2)

    assert load_of == waited and len(sems) == recv_sem.shape[0], len(sems)
    with jax.named_scope('sendwaits'):
        for slot, size in enumerate(link_of):
            take(size, link_sem.at[slot])
        own_meta = meta.at[pl.ds(0, 2 * RING - 1)]
        pltpu.make_async_copy(own_meta, own_meta, msem.at[0]).wait()
        for d in range(RING):
            take(nb + na, dsend.at[d])


def solution(mesh):
    row_spec = P(('batch', 'rows'), 'ksplit')
    col_spec = P(('batch', 'ksplit'))
    assert mesh.shape['rows'] == RING and mesh.shape['ksplit'] == 2 * RING

    def device_step(a_loc, b_loc, pair_loc, plist_loc, cidx_loc):
        a, b = a_loc[0, 0], b_loc[0]
        pairs = pair_loc[0, 0, :, 0, :].T
        plist = plist_loc[0, 0].T
        cidx = cidx_loc[0, 0].T
        na, nb, nc, size = a.shape[0], b.shape[0], cidx.shape[1], a.shape[-1]
        npart = plist.shape[1]
        nsem = 14 + 9 * len(HALF_CHUNKS)
        block = (size, size)
        args = [pltpu.with_memory_space_constraint(t, pltpu.HBM) for t in (a, b, pairs, plist, cidx)]
        out = pl.pallas_call(
            functools.partial(kernel, na, nb, nc),
            out_shape=jax.ShapeDtypeStruct((nc, *block), jnp.float32),
            in_specs=[pl.BlockSpec(memory_space=pltpu.HBM)] * 5,
            out_specs=pl.BlockSpec(memory_space=pltpu.VMEM),
            scratch_shapes=[
                *[pltpu.VMEM((nb + na + 1, *block), b.dtype) for _ in range(2 * RING)],
                pltpu.VMEM((2 * RING, 2, 2, npart), jnp.int32),
                pltpu.VMEM((2, nc), jnp.int32),
                pltpu.VMEM((nc, 128), jnp.int32),
                pltpu.SMEM((nc, 128), jnp.int32),
                pltpu.SemaphoreType.DMA((6,)),
                pltpu.SemaphoreType.DMA((4,)),
                pltpu.SemaphoreType.DMA((nsem,)),
                pltpu.SemaphoreType.DMA((RING,)),
                pltpu.SemaphoreType.DMA((RING,)),
                pltpu.SemaphoreType.DMA((3,)),
            ],
            compiler_params=pltpu.CompilerParams(
                collective_id=0, has_side_effects=True, vmem_limit_bytes=30 * 2**20),
        )(*args)
        return out[None, None]

    return jax.shard_map(device_step, mesh=mesh, in_specs=(row_spec, col_spec, row_spec, row_spec, row_spec), out_specs=row_spec, check_vma=False)
```

```python
import functools

import jax
import jax.numpy as jnp
from jax import lax
from jax.experimental import pallas as pl
from jax.experimental.pallas import tpu as pltpu
from jax.sharding import PartitionSpec as P


MESH = pl.DeviceIdType.MESH
RING = 4
HALF_CHUNKS = (3, 3, 3, 4)
LEFT, RIGHT, FAR = 3, 1, 2


def plan(nb):
    half = sum(HALF_CHUNKS)
    quad = (nb - 4 * half) // RING
    assert 4 * half + RING * quad == nb
    return half, quad


def kernel(na, nb, nc, a_hbm, b_hbm, pairs_hbm, plist_hbm, cidx_hbm, acc, *scratch):
    mine, twin = scratch[0:RING], scratch[RING:2 * RING]
    (meta, cidx, tab_v, tab_s, loc_sem, link_sem, recv_sem, dsend, drecv, msem) = scratch[2 * RING:]
    half, quad = plan(nb)
    nk, ah = len(HALF_CHUNKS), na // 2
    parts = ((0, quad // 2), (quad // 2, quad - quad // 2))
    offs = [(sum(HALF_CHUNKS[:k]), HALF_CHUNKS[k]) for k in range(nk)]
    ks = lax.axis_index("ksplit")
    y = lax.axis_index("rows")
    core = ks % 2
    x = ks // 2

    def chip(dx, flip=0):
        return {"ksplit": ((x + dx) % RING) * 2 + (1 - core if flip else core)}

    sib = chip(0, 1)
    links = {
        "x+": (0, chip(1)), "x-": (1, chip(3)),
        "y+": (2, {"rows": (y + 1) % RING}), "y-": (3, {"rows": (y + 3) % RING}),
    }

    loads = [
        pltpu.make_async_copy(b_hbm, mine[0].at[pl.ds(0, nb)], loc_sem.at[0]),
        pltpu.make_async_copy(a_hbm, mine[0].at[pl.ds(nb, na)], loc_sem.at[1]),
        pltpu.make_async_copy(pairs_hbm, meta.at[0, 0], loc_sem.at[2]),
        pltpu.make_async_copy(plist_hbm, meta.at[0, 1], loc_sem.at[3]),
        pltpu.make_async_copy(cidx_hbm, cidx, loc_sem.at[4]),
    ]
    for load in loads:
        load.start()

    barrier = pltpu.get_barrier_semaphore()
    devices = [dev for _, dev in links.values()] + [chip(2), sib]
    for dev in devices:
        pl.semaphore_signal(barrier, inc=1, device_id=dev, device_id_type=MESH)
    zero = jnp.zeros(mine[0].shape[1:], mine[0].dtype)
    for ref in (*mine, *twin):
        ref[nb + na] = zero
    with jax.named_scope('barrier'):
        pl.semaphore_wait(barrier, len(devices))

    sems = {}
    load_of = {}
    link_of = [0] * len(links)

    def index(key):
        return sems.setdefault(key, len(sems))

    def send(link, key, src, dst, start, size):
        slot, dev = links[link]
        n = index(key)
        load_of[n] = load_of.get(n, 0) + size
        link_of[slot] += size
        pltpu.make_async_remote_copy(
            src_ref=mine[src].at[pl.ds(start, size)], dst_ref=mine[dst].at[pl.ds(start, size)],
            send_sem=link_sem.at[slot], recv_sem=recv_sem.at[n],
            device_id=dev, device_id_type=MESH).start()

    def take(size, sem):
        view = mine[0].at[pl.ds(0, size)]
        pltpu.make_async_copy(view, view, sem).wait()

    waited = {}

    def arrive(key, size):
        n = index(key)
        waited[n] = waited.get(n, 0) + size
        with jax.named_scope('_'.join(str(t) for t in key).replace('+', 'p').replace('-', 'm').replace(' ', '')):
            take(size, recv_sem.at[n])

    def share(d, start, size):
        pltpu.make_async_remote_copy(
            src_ref=mine[d].at[pl.ds(start, size)], dst_ref=twin[d].at[pl.ds(start, size)],
            send_sem=dsend.at[d], recv_sem=drecv.at[d], device_id=sib, device_id_type=MESH).start()

    own = (y % 2) * (2 * half)
    theirs = (1 - y % 2) * (2 * half)

    def quad_at(dy):
        return 4 * half + ((y + dy) % RING) * quad

    def lay(k, base):
        off, size = offs[k]
        return base + off, base + half + off, size

    q0, qm, qp, qf = quad_at(0), quad_at(3), quad_at(1), quad_at(2)

    loads[0].wait()
    for part in range(2):
        for link, d, (off, size) in (("x+", LEFT, parts[part]), ("x-", RIGHT, parts[1 - part])):
            send(link, (link, "w", part), 0, d, q0 + off, size)
    loads[2].wait()
    loads[3].wait()

    def list_to(slot, src, dev, sem):
        pltpu.make_async_remote_copy(
            src_ref=meta.at[src], dst_ref=meta.at[slot], send_sem=msem.at[0], recv_sem=msem.at[sem],
            device_id=dev, device_id_type=MESH).start()

    def lists_taken(count, sem):
        view = meta.at[pl.ds(0, count)]
        pltpu.make_async_copy(view, view, msem.at[sem]).wait()

    for dx in range(1, RING):
        list_to(2 * (RING - dx), 0, chip(dx), 1)
    list_to(1, 0, sib, 2)
    for k in range(nk):
        u, v, size = lay(k, own)
        send("x+", ("x+", "u", k), 0, LEFT, u, size)
        send("x-", ("x-", "v", k), 0, RIGHT, v, size)
        send("x+", ("x+", "v", k), 0, LEFT, v, size)
        send("x-", ("x-", "u", k), 0, RIGHT, u, size)
    loads[1].wait()

    def build_table():
      with jax.named_scope('table'):
            loads[4].wait()
            lists_taken(RING, 2)
            npart = meta.shape[3]
            ckey = cidx[0:1, :] * 4096 + cidx[1:2, :]
            eye = lax.broadcasted_iota(jnp.int32, (nc, nc), 0) == lax.broadcasted_iota(jnp.int32, (nc, nc), 1)
            ccol = jnp.sum(jnp.where(eye, jnp.broadcast_to(ckey, (nc, nc)), 0), axis=1, keepdims=True)
            lane = lax.broadcasted_iota(jnp.int32, (nc, 128), 1)
            table = jnp.zeros((nc, 128), jnp.int32)
            for slot in range(2 * RING):
                pkey = meta[slot, 1, 0:1, :] * 4096 + meta[slot, 1, 1:2, :]
                pval = meta[slot, 0, 0:1, :] * 4096 + meta[slot, 0, 1:2, :] - na * 4096
                hit = jnp.broadcast_to(ccol, (nc, npart)) == jnp.broadcast_to(pkey, (nc, npart))
                found = jnp.sum(jnp.where(hit, jnp.broadcast_to(pval, (nc, npart)), 0), axis=1, keepdims=True) + na * 4096
                a_at = nb + jnp.clip(lax.shift_right_arithmetic(found, 12), 0, na)
                b_at = jnp.clip(found & 4095, 0, nb - 1)
                table = jnp.where(lane == 2 * slot, a_at, table)
                table = jnp.where(lane == 2 * slot + 1, b_at, table)
            tab_v[...] = table
            pltpu.make_async_copy(tab_v, tab_s, loc_sem.at[5]).start()

    def stage(d, sides=(0, 1), lo=0, hi=nc, group=24, first=False):
        def product(side, c):
            ref, n = (twin if side else mine)[d], 4 * d + 2 * side
            p = jnp.dot(ref[tab_s[c, n]], ref[tab_s[c, n + 1]], preferred_element_type=jnp.float32)
            return p.astype(jnp.bfloat16).astype(jnp.float32)

        def body(step, carry):
            for sub in range(group):
                c = step * group + sub
                total = product(sides[0], c)
                for side in sides[1:]:
                    total = total + product(side, c)
                acc[c] = total if first else acc[c] + total
            return carry

        with jax.named_scope(f'stage{d}_{len(sides)}{sides[0]}_{lo}'):
            lax.fori_loop(lo // group, hi // group, body, 0)

    def ready(d):
        take_twin = twin[d].at[pl.ds(0, nb + na)]
        with jax.named_scope(f'ready{d}'):
            pltpu.make_async_copy(take_twin, take_twin, drecv.at[d]).wait()

    def y_taken(cols, k):
        u, v, size = lay(k, theirs)
        arrive(("y+", cols, k), size * len(cols))
        arrive(("y-", cols, k), size * len(cols))
        for d in cols:
            share(d, u, size)
            share(d, v, size)

    near = (LEFT, RIGHT)
    third = nc // 3

    for part in range(2):
        for link, d, (off, size) in (("x+", LEFT, parts[part]), ("x-", RIGHT, parts[1 - part])):
            arrive((link, "w", part), size)
            send("y+", ("y+w", near), d, d, q0 + off, size)
            send("y-", ("y-w", near), d, d, q0 + off, size)
            if part == 0:
                send(link, ("f", "w"), d, FAR, q0 + off, size)
            share(d, q0 + off, size)
    share(0, 0, nb + na)

    def spread(k):
        (up, up_size), (down, down_size) = parts if k == 0 else parts[::-1]
        for d in (near if k == 0 else (FAR,)):
            send("y+", ("g", k), d, d, qm + up, up_size)
            send("y-", ("g", k), d, d, qp + down, down_size)
            share(d, qm, quad)
            share(d, qp, quad)

    for k in range(nk):
        u, v, size = lay(k, own)
        arrive(("x+", "u", k), size)
        send("y+", ("y+", near, k), LEFT, LEFT, u, size)
        send("x+", ("f", k), LEFT, FAR, u, size)
        arrive(("x-", "v", k), size)
        send("y-", ("y-", near, k), RIGHT, RIGHT, v, size)
        send("x-", ("f", k), RIGHT, FAR, v, size)
        share(LEFT, u, size)
        share(RIGHT, v, size)
        if k == 0:
            lists_taken(RING - 1, 1)
            for d in range(1, RING):
                list_to(2 * d + 1, 2 * d, sib, 2)
        elif k == 1:
            arrive(("y+w", near), 2 * quad)
            arrive(("y-w", near), 2 * quad)
            spread(0)
        elif k == 2:
            stage(0, lo=third, hi=2 * third, first=True)
            y_taken(near, 0)
        elif k == 3:
            y_taken(near, 1)
        arrive(("x+", "v", k), size)
        send("y-", ("y-", near, k), LEFT, LEFT, v, size)
        arrive(("x-", "u", k), size)
        send("y+", ("y+", near, k), RIGHT, RIGHT, u, size)
        share(LEFT, v, size)
        share(RIGHT, u, size)
        if k == 0:
            build_table()
        elif k == 1:
            pltpu.make_async_copy(tab_v, tab_s, loc_sem.at[5]).wait()
            ready(0)
            stage(0, hi=third, first=True)
        elif k == 2:
            stage(0, lo=2 * third, first=True)
    for part in range(2):
        send("x+", ("a", part), 0, LEFT, nb + part * ah, ah)
        send("x-", ("a", part), 0, RIGHT, nb + (1 - part) * ah, ah)
    arrive(("g", 0), 2 * quad)
    for d in near:
        share(d, qf, quad)

    def far_block(k):
        u, v, size = lay(k, own)
        arrive(("f", k), 2 * size)
        send("y+", ("y+", (FAR,), k), FAR, FAR, u, size)
        send("y-", ("y-", (FAR,), k), FAR, FAR, v, size)
        share(FAR, u, size)
        share(FAR, v, size)

    arrive(("f", "w"), quad)
    send("y+", ("y+w", FAR), FAR, FAR, q0, quad)
    send("y-", ("y-w", FAR), FAR, FAR, q0, quad)
    share(FAR, q0, quad)
    y_taken(near, 2)
    far_block(0)
    far_block(1)
    y_taken(near, 3)
    far_block(2)
    arrive(("y+w", FAR), quad)
    arrive(("y-w", FAR), quad)
    spread(1)
    far_block(3)
    y_taken((FAR,), 0)

    arrive(("a", 0), 2 * ah)
    send("x+", ("f", "a"), LEFT, FAR, nb, ah)
    send("x-", ("f", "a"), RIGHT, FAR, nb + ah, ah)
    share(LEFT, nb, ah)
    share(RIGHT, nb + ah, ah)
    y_taken((FAR,), 1)
    y_taken((FAR,), 2)
    arrive(("a", 1), 2 * ah)
    share(LEFT, nb + ah, ah)
    share(RIGHT, nb, ah)
    stage(LEFT, (0,))
    stage(RIGHT, (0,))
    y_taken((FAR,), 3)
    arrive(("g", 1), quad)
    share(FAR, qf, quad)
    ready(LEFT)
    stage(LEFT, (1,))
    ready(RIGHT)
    stage(RIGHT, (1,), hi=2 * third)
    arrive(("f", "a"), 2 * ah)
    share(FAR, nb, na)
    stage(RIGHT, (1,), lo=2 * third)
    stage(FAR, (0,))
    ready(FAR)
    stage(FAR, (1,))

    assert load_of == waited and len(sems) == recv_sem.shape[0], len(sems)
    with jax.named_scope('sendwaits'):
        for slot, size in enumerate(link_of):
            take(size, link_sem.at[slot])
        own_meta = meta.at[pl.ds(0, 2 * RING - 1)]
        pltpu.make_async_copy(own_meta, own_meta, msem.at[0]).wait()
        for d in range(RING):
            take(nb + na, dsend.at[d])


def solution(mesh):
    row_spec = P(('batch', 'rows'), 'ksplit')
    col_spec = P(('batch', 'ksplit'))
    assert mesh.shape['rows'] == RING and mesh.shape['ksplit'] == 2 * RING

    def device_step(a_loc, b_loc, pair_loc, plist_loc, cidx_loc):
        a, b = a_loc[0, 0], b_loc[0]
        pairs = pair_loc[0, 0, :, 0, :].T
        plist = plist_loc[0, 0].T
        cidx = cidx_loc[0, 0].T
        na, nb, nc, size = a.shape[0], b.shape[0], cidx.shape[1], a.shape[-1]
        npart = plist.shape[1]
        nsem = 14 + 9 * len(HALF_CHUNKS)
        block = (size, size)
        args = [pltpu.with_memory_space_constraint(t, pltpu.HBM) for t in (a, b, pairs, plist, cidx)]
        out = pl.pallas_call(
            functools.partial(kernel, na, nb, nc),
            out_shape=jax.ShapeDtypeStruct((nc, *block), jnp.float32),
            in_specs=[pl.BlockSpec(memory_space=pltpu.HBM)] * 5,
            out_specs=pl.BlockSpec(memory_space=pltpu.VMEM),
            scratch_shapes=[
                *[pltpu.VMEM((nb + na + 1, *block), b.dtype) for _ in range(2 * RING)],
                pltpu.VMEM((2 * RING, 2, 2, npart), jnp.int32),
                pltpu.VMEM((2, nc), jnp.int32),
                pltpu.VMEM((nc, 128), jnp.int32),
                pltpu.SMEM((nc, 128), jnp.int32),
                pltpu.SemaphoreType.DMA((6,)),
                pltpu.SemaphoreType.DMA((4,)),
                pltpu.SemaphoreType.DMA((nsem,)),
                pltpu.SemaphoreType.DMA((RING,)),
                pltpu.SemaphoreType.DMA((RING,)),
                pltpu.SemaphoreType.DMA((3,)),
            ],
            compiler_params=pltpu.CompilerParams(
                collective_id=0, has_side_effects=True, vmem_limit_bytes=30 * 2**20),
        )(*args)
        return out[None, None]

    return jax.shard_map(device_step, mesh=mesh, in_specs=(row_spec, col_spec, row_spec, row_spec, row_spec), out_specs=row_spec, check_vma=False)
```

```python
import functools

import jax
import jax.numpy as jnp
from jax import lax
from jax.experimental import pallas as pl
from jax.experimental.pallas import tpu as pltpu
from jax.sharding import PartitionSpec as P


MESH = pl.DeviceIdType.MESH
RING = 4
HALF_CHUNKS = (3, 3, 3, 4)
LEFT, RIGHT, FAR = 3, 1, 2


def plan(nb):
    half = sum(HALF_CHUNKS)
    quad = (nb - 4 * half) // RING
    assert 4 * half + RING * quad == nb
    return half, quad


def kernel(na, nb, nc, a_hbm, b_hbm, pairs_hbm, plist_hbm, cidx_hbm, acc, *scratch):
    mine, twin = scratch[0:RING], scratch[RING:2 * RING]
    (meta, cidx, tab_v, tab_s, loc_sem, link_sem, recv_sem, dsend, drecv, msem) = scratch[2 * RING:]
    half, quad = plan(nb)
    nk, ah = len(HALF_CHUNKS), na // 2
    parts = ((0, quad // 2), (quad // 2, quad - quad // 2))
    offs = [(sum(HALF_CHUNKS[:k]), HALF_CHUNKS[k]) for k in range(nk)]
    ks = lax.axis_index("ksplit")
    y = lax.axis_index("rows")
    core = ks % 2
    x = ks // 2

    def chip(dx, flip=0):
        return {"ksplit": ((x + dx) % RING) * 2 + (1 - core if flip else core)}

    sib = chip(0, 1)
    links = {
        "x+": (0, chip(1)), "x-": (1, chip(3)),
        "y+": (2, {"rows": (y + 1) % RING}), "y-": (3, {"rows": (y + 3) % RING}),
    }

    loads = [
        pltpu.make_async_copy(b_hbm, mine[0].at[pl.ds(0, nb)], loc_sem.at[0]),
        pltpu.make_async_copy(a_hbm, mine[0].at[pl.ds(nb, na)], loc_sem.at[1]),
        pltpu.make_async_copy(pairs_hbm, meta.at[0, 0], loc_sem.at[2]),
        pltpu.make_async_copy(plist_hbm, meta.at[0, 1], loc_sem.at[3]),
        pltpu.make_async_copy(cidx_hbm, cidx, loc_sem.at[4]),
    ]
    for load in loads:
        load.start()

    barrier = pltpu.get_barrier_semaphore()
    devices = [dev for _, dev in links.values()] + [chip(2), sib]
    for dev in devices:
        pl.semaphore_signal(barrier, inc=1, device_id=dev, device_id_type=MESH)
    zero = jnp.zeros(mine[0].shape[1:], mine[0].dtype)
    for ref in (*mine, *twin):
        ref[nb + na] = zero
    with jax.named_scope('barrier'):
        pl.semaphore_wait(barrier, len(devices))

    sems = {}
    load_of = {}
    link_of = [0] * len(links)

    def index(key):
        return sems.setdefault(key, len(sems))

    def send(link, key, src, dst, start, size):
        slot, dev = links[link]
        n = index(key)
        load_of[n] = load_of.get(n, 0) + size
        link_of[slot] += size
        pltpu.make_async_remote_copy(
            src_ref=mine[src].at[pl.ds(start, size)], dst_ref=mine[dst].at[pl.ds(start, size)],
            send_sem=link_sem.at[slot], recv_sem=recv_sem.at[n],
            device_id=dev, device_id_type=MESH).start()

    def take(size, sem):
        view = mine[0].at[pl.ds(0, size)]
        pltpu.make_async_copy(view, view, sem).wait()

    waited = {}

    def arrive(key, size):
        n = index(key)
        waited[n] = waited.get(n, 0) + size
        with jax.named_scope('_'.join(str(t) for t in key).replace('+', 'p').replace('-', 'm').replace(' ', '')):
            take(size, recv_sem.at[n])

    def share(d, start, size):
        pltpu.make_async_remote_copy(
            src_ref=mine[d].at[pl.ds(start, size)], dst_ref=twin[d].at[pl.ds(start, size)],
            send_sem=dsend.at[d], recv_sem=drecv.at[d], device_id=sib, device_id_type=MESH).start()

    own = (y % 2) * (2 * half)
    theirs = (1 - y % 2) * (2 * half)

    def quad_at(dy):
        return 4 * half + ((y + dy) % RING) * quad

    def lay(k, base):
        off, size = offs[k]
        return base + off, base + half + off, size

    q0, qm, qp, qf = quad_at(0), quad_at(3), quad_at(1), quad_at(2)

    loads[0].wait()
    for part in range(2):
        for link, d, (off, size) in (("x+", LEFT, parts[part]), ("x-", RIGHT, parts[1 - part])):
            send(link, (link, "w", part), 0, d, q0 + off, size)
    loads[2].wait()
    loads[3].wait()

    def list_to(slot, src, dev, sem):
        pltpu.make_async_remote_copy(
            src_ref=meta.at[src], dst_ref=meta.at[slot], send_sem=msem.at[0], recv_sem=msem.at[sem],
            device_id=dev, device_id_type=MESH).start()

    def lists_taken(count, sem):
        view = meta.at[pl.ds(0, count)]
        pltpu.make_async_copy(view, view, msem.at[sem]).wait()

    for dx in range(1, RING):
        list_to(2 * (RING - dx), 0, chip(dx), 1)
    list_to(1, 0, sib, 2)
    for k in range(nk):
        u, v, size = lay(k, own)
        send("x+", ("x+", "u", k), 0, LEFT, u, size)
        send("x-", ("x-", "v", k), 0, RIGHT, v, size)
        send("x+", ("x+", "v", k), 0, LEFT, v, size)
        send("x-", ("x-", "u", k), 0, RIGHT, u, size)
    loads[1].wait()

    def build_table():
      with jax.named_scope('table'):
            loads[4].wait()
            lists_taken(RING, 2)
            npart = meta.shape[3]
            ckey = cidx[0:1, :] * 4096 + cidx[1:2, :]
            eye = lax.broadcasted_iota(jnp.int32, (nc, nc), 0) == lax.broadcasted_iota(jnp.int32, (nc, nc), 1)
            ccol = jnp.sum(jnp.where(eye, jnp.broadcast_to(ckey, (nc, nc)), 0), axis=1, keepdims=True)
            lane = lax.broadcasted_iota(jnp.int32, (nc, 128), 1)
            table = jnp.zeros((nc, 128), jnp.int32)
            for slot in range(2 * RING):
                pkey = meta[slot, 1, 0:1, :] * 4096 + meta[slot, 1, 1:2, :]
                pval = meta[slot, 0, 0:1, :] * 4096 + meta[slot, 0, 1:2, :] - na * 4096
                hit = jnp.broadcast_to(ccol, (nc, npart)) == jnp.broadcast_to(pkey, (nc, npart))
                found = jnp.sum(jnp.where(hit, jnp.broadcast_to(pval, (nc, npart)), 0), axis=1, keepdims=True) + na * 4096
                a_at = nb + jnp.clip(lax.shift_right_arithmetic(found, 12), 0, na)
                b_at = jnp.clip(found & 4095, 0, nb - 1)
                table = jnp.where(lane == 2 * slot, a_at, table)
                table = jnp.where(lane == 2 * slot + 1, b_at, table)
            tab_v[...] = table
            pltpu.make_async_copy(tab_v, tab_s, loc_sem.at[5]).start()

    def stage(d, sides=(0, 1), lo=0, hi=nc, group=24, first=False):
        def product(side, c):
            ref, n = (twin if side else mine)[d], 4 * d + 2 * side
            p = jnp.dot(ref[tab_s[c, n]], ref[tab_s[c, n + 1]], preferred_element_type=jnp.float32)
            return p.astype(jnp.bfloat16).astype(jnp.float32)

        def body(step, carry):
            for sub in range(group):
                c = step * group + sub
                total = product(sides[0], c)
                for side in sides[1:]:
                    total = total + product(side, c)
                acc[c] = total if first else acc[c] + total
            return carry

        with jax.named_scope(f'stage{d}_{len(sides)}{sides[0]}_{lo}'):
            lax.fori_loop(lo // group, hi // group, body, 0)

    def ready(d):
        take_twin = twin[d].at[pl.ds(0, nb + na)]
        with jax.named_scope(f'ready{d}'):
            pltpu.make_async_copy(take_twin, take_twin, drecv.at[d]).wait()

    def y_taken(cols, k):
        u, v, size = lay(k, theirs)
        arrive(("y", cols, k), 2 * size * len(cols))
        for d in cols:
            share(d, u, size)
            share(d, v, size)

    near = (LEFT, RIGHT)
    third = nc // 3

    for part in range(2):
        for link, d, (off, size) in (("x+", LEFT, parts[part]), ("x-", RIGHT, parts[1 - part])):
            arrive((link, "w", part), size)
            send("y+", ("yw", near), d, d, q0 + off, size)
            send("y-", ("yw", near), d, d, q0 + off, size)
            if part == 0:
                send(link, ("f", "w"), d, FAR, q0 + off, size)
            share(d, q0 + off, size)
    share(0, 0, nb + na)

    def spread(k):
        (up, up_size), (down, down_size) = parts if k == 0 else parts[::-1]
        for d in (near if k == 0 else (FAR,)):
            send("y+", ("g", k), d, d, qm + up, up_size)
            send("y-", ("g", k), d, d, qp + down, down_size)
            share(d, qm, quad)
            share(d, qp, quad)

    for k in range(nk):
        u, v, size = lay(k, own)
        arrive(("x+", "u", k), size)
        send("y+", ("y", near, k), LEFT, LEFT, u, size)
        send("x+", ("f", k), LEFT, FAR, u, size)
        arrive(("x-", "v", k), size)
        send("y-", ("y", near, k), RIGHT, RIGHT, v, size)
        send("x-", ("f", k), RIGHT, FAR, v, size)
        share(LEFT, u, size)
        share(RIGHT, v, size)
        if k == 0:
            lists_taken(RING - 1, 1)
            for d in range(1, RING):
                list_to(2 * d + 1, 2 * d, sib, 2)
        elif k == 1:
            arrive(("yw", near), 4 * quad)
            spread(0)
        elif k == 2:
            stage(0, lo=third, hi=2 * third, first=True)
            y_taken(near, 0)
        elif k == 3:
            y_taken(near, 1)
        arrive(("x+", "v", k), size)
        send("y-", ("y", near, k), LEFT, LEFT, v, size)
        arrive(("x-", "u", k), size)
        send("y+", ("y", near, k), RIGHT, RIGHT, u, size)
        share(LEFT, v, size)
        share(RIGHT, u, size)
        if k == 0:
            build_table()
        elif k == 1:
            pltpu.make_async_copy(tab_v, tab_s, loc_sem.at[5]).wait()
            ready(0)
            stage(0, hi=third, first=True)
        elif k == 2:
            stage(0, lo=2 * third, first=True)
    for part in range(2):
        send("x+", ("a", part), 0, LEFT, nb + part * ah, ah)
        send("x-", ("a", part), 0, RIGHT, nb + (1 - part) * ah, ah)
    arrive(("g", 0), 2 * quad)
    for d in near:
        share(d, qf, quad)

    def far_block(k):
        u, v, size = lay(k, own)
        arrive(("f", k), 2 * size)
        send("y+", ("y", (FAR,), k), FAR, FAR, u, size)
        send("y-", ("y", (FAR,), k), FAR, FAR, v, size)
        share(FAR, u, size)
        share(FAR, v, size)

    arrive(("f", "w"), quad)
    send("y+", ("yw", FAR), FAR, FAR, q0, quad)
    send("y-", ("yw", FAR), FAR, FAR, q0, quad)
    share(FAR, q0, quad)
    y_taken(near, 2)
    far_block(0)
    far_block(1)
    y_taken(near, 3)
    far_block(2)
    arrive(("yw", FAR), 2 * quad)
    spread(1)
    far_block(3)
    y_taken((FAR,), 0)

    arrive(("a", 0), 2 * ah)
    send("x+", ("f", "a"), LEFT, FAR, nb, ah)
    send("x-", ("f", "a"), RIGHT, FAR, nb + ah, ah)
    share(LEFT, nb, ah)
    share(RIGHT, nb + ah, ah)
    y_taken((FAR,), 1)
    arrive(("a", 1), 2 * ah)
    share(LEFT, nb + ah, ah)
    share(RIGHT, nb, ah)
    stage(LEFT, (0,))
    y_taken((FAR,), 2)
    ready(LEFT)
    stage(LEFT, (1,))
    ready(RIGHT)
    stage(RIGHT)
    arrive(("g", 1), quad)
    share(FAR, qf, quad)
    y_taken((FAR,), 3)
    arrive(("f", "a"), 2 * ah)
    share(FAR, nb, na)
    stage(FAR, (0,), group=nc // 2)
    ready(FAR)
    stage(FAR, (1,), group=nc // 2)

    assert load_of == waited and len(sems) == recv_sem.shape[0], len(sems)
    with jax.named_scope('sendwaits'):
        for slot, size in enumerate(link_of):
            take(size, link_sem.at[slot])
        own_meta = meta.at[pl.ds(0, 2 * RING - 1)]
        pltpu.make_async_copy(own_meta, own_meta, msem.at[0]).wait()
        for d in range(RING):
            take(nb + na, dsend.at[d])


def solution(mesh):
    row_spec = P(('batch', 'rows'), 'ksplit')
    col_spec = P(('batch', 'ksplit'))
    assert mesh.shape['rows'] == RING and mesh.shape['ksplit'] == 2 * RING

    def device_step(a_loc, b_loc, pair_loc, plist_loc, cidx_loc):
        a, b = a_loc[0, 0], b_loc[0]
        pairs = pair_loc[0, 0, :, 0, :].T
        plist = plist_loc[0, 0].T
        cidx = cidx_loc[0, 0].T
        na, nb, nc, size = a.shape[0], b.shape[0], cidx.shape[1], a.shape[-1]
        npart = plist.shape[1]
        nsem = 12 + 7 * len(HALF_CHUNKS)
        block = (size, size)
        args = [pltpu.with_memory_space_constraint(t, pltpu.HBM) for t in (a, b, pairs, plist, cidx)]
        out = pl.pallas_call(
            functools.partial(kernel, na, nb, nc),
            out_shape=jax.ShapeDtypeStruct((nc, *block), jnp.float32),
            in_specs=[pl.BlockSpec(memory_space=pltpu.HBM)] * 5,
            out_specs=pl.BlockSpec(memory_space=pltpu.VMEM),
            scratch_shapes=[
                *[pltpu.VMEM((nb + na + 1, *block), b.dtype) for _ in range(2 * RING)],
                pltpu.VMEM((2 * RING, 2, 2, npart), jnp.int32),
                pltpu.VMEM((2, nc), jnp.int32),
                pltpu.VMEM((nc, 128), jnp.int32),
                pltpu.SMEM((nc, 128), jnp.int32),
                pltpu.SemaphoreType.DMA((6,)),
                pltpu.SemaphoreType.DMA((4,)),
                pltpu.SemaphoreType.DMA((nsem,)),
                pltpu.SemaphoreType.DMA((RING,)),
                pltpu.SemaphoreType.DMA((RING,)),
                pltpu.SemaphoreType.DMA((3,)),
            ],
            compiler_params=pltpu.CompilerParams(
                collective_id=0, has_side_effects=True, vmem_limit_bytes=30 * 2**20),
        )(*args)
        return out[None, None]

    return jax.shard_map(device_step, mesh=mesh, in_specs=(row_spec, col_spec, row_spec, row_spec, row_spec), out_specs=row_spec, check_vma=False)
```

```python
import functools

import jax
import jax.numpy as jnp
from jax import lax
from jax.experimental import pallas as pl
from jax.experimental.pallas import tpu as pltpu
from jax.sharding import PartitionSpec as P


MESH = pl.DeviceIdType.MESH
RING = 4
HALF_CHUNKS = (3, 3, 3, 4)
LEFT, RIGHT, FAR = 3, 1, 2


def plan(nb):
    half = sum(HALF_CHUNKS)
    quad = (nb - 4 * half) // RING
    assert 4 * half + RING * quad == nb
    return half, quad


def kernel(na, nb, nc, a_hbm, b_hbm, pairs_hbm, plist_hbm, cidx_hbm, acc, *scratch):
    mine, twin = scratch[0:RING], scratch[RING:2 * RING]
    (meta, cidx, tab_v, tab_s, loc_sem, link_sem, recv_sem, dsend, drecv, msem) = scratch[2 * RING:]
    half, quad = plan(nb)
    nk, ah = len(HALF_CHUNKS), na // 2
    parts = ((0, quad // 2), (quad // 2, quad - quad // 2))
    offs = [(sum(HALF_CHUNKS[:k]), HALF_CHUNKS[k]) for k in range(nk)]
    ks = lax.axis_index("ksplit")
    y = lax.axis_index("rows")
    core = ks % 2
    x = ks // 2

    def chip(dx, flip=0):
        return {"ksplit": ((x + dx) % RING) * 2 + (1 - core if flip else core)}

    sib = chip(0, 1)
    links = {
        "x+": (0, chip(1)), "x-": (1, chip(3)),
        "y+": (2, {"rows": (y + 1) % RING}), "y-": (3, {"rows": (y + 3) % RING}),
    }

    loads = [
        pltpu.make_async_copy(b_hbm, mine[0].at[pl.ds(0, nb)], loc_sem.at[0]),
        pltpu.make_async_copy(a_hbm, mine[0].at[pl.ds(nb, na)], loc_sem.at[1]),
        pltpu.make_async_copy(pairs_hbm, meta.at[0, 0], loc_sem.at[2]),
        pltpu.make_async_copy(plist_hbm, meta.at[0, 1], loc_sem.at[3]),
        pltpu.make_async_copy(cidx_hbm, cidx, loc_sem.at[4]),
    ]
    for load in loads:
        load.start()

    barrier = pltpu.get_barrier_semaphore()
    devices = [dev for _, dev in links.values()] + [chip(2), sib]
    for dev in devices:
        pl.semaphore_signal(barrier, inc=1, device_id=dev, device_id_type=MESH)
    zero = jnp.zeros(mine[0].shape[1:], mine[0].dtype)
    for ref in (*mine, *twin):
        ref[nb + na] = zero
    with jax.named_scope('barrier'):
        pl.semaphore_wait(barrier, len(devices))

    sems = {}
    load_of = {}
    link_of = [0] * len(links)

    def index(key):
        return sems.setdefault(key, len(sems))

    def send(link, key, src, dst, start, size):
        slot, dev = links[link]
        n = index(key)
        load_of[n] = load_of.get(n, 0) + size
        link_of[slot] += size
        pltpu.make_async_remote_copy(
            src_ref=mine[src].at[pl.ds(start, size)], dst_ref=mine[dst].at[pl.ds(start, size)],
            send_sem=link_sem.at[slot], recv_sem=recv_sem.at[n],
            device_id=dev, device_id_type=MESH).start()

    def take(size, sem):
        view = mine[0].at[pl.ds(0, size)]
        pltpu.make_async_copy(view, view, sem).wait()

    waited = {}

    def arrive(key, size):
        n = index(key)
        waited[n] = waited.get(n, 0) + size
        with jax.named_scope('_'.join(str(t) for t in key).replace('+', 'p').replace('-', 'm').replace(' ', '')):
            take(size, recv_sem.at[n])

    def share(d, start, size):
        pltpu.make_async_remote_copy(
            src_ref=mine[d].at[pl.ds(start, size)], dst_ref=twin[d].at[pl.ds(start, size)],
            send_sem=dsend.at[d], recv_sem=drecv.at[d], device_id=sib, device_id_type=MESH).start()

    own = (y % 2) * (2 * half)
    theirs = (1 - y % 2) * (2 * half)

    def quad_at(dy):
        return 4 * half + ((y + dy) % RING) * quad

    def lay(k, base):
        off, size = offs[k]
        return base + off, base + half + off, size

    q0, qm, qp, qf = quad_at(0), quad_at(3), quad_at(1), quad_at(2)

    loads[0].wait()
    def pieces(first, second):
        (off, size), rest = parts[first], parts[second]
        return ((off, 1, "f"), (off + 1, size - 1, "f"), (*rest, ""))

    w_pieces = list(zip(pieces(0, 1), pieces(1, 0)))
    for n, pair in enumerate(w_pieces):
        for link, d, (off, size, _) in zip(("x+", "x-"), (LEFT, RIGHT), pair):
            send(link, (link, "w", n), 0, d, q0 + off, size)
    loads[2].wait()
    loads[3].wait()

    def list_to(slot, src, dev, sem):
        pltpu.make_async_remote_copy(
            src_ref=meta.at[src], dst_ref=meta.at[slot], send_sem=msem.at[0], recv_sem=msem.at[sem],
            device_id=dev, device_id_type=MESH).start()

    def lists_taken(count, sem):
        view = meta.at[pl.ds(0, count)]
        pltpu.make_async_copy(view, view, msem.at[sem]).wait()

    for dx in range(1, RING):
        list_to(2 * (RING - dx), 0, chip(dx), 1)
    list_to(1, 0, sib, 2)
    for k in range(nk):
        u, v, size = lay(k, own)
        send("x+", ("x+", "u", k), 0, LEFT, u, size)
        send("x-", ("x-", "v", k), 0, RIGHT, v, size)
        send("x+", ("x+", "v", k), 0, LEFT, v, size)
        send("x-", ("x-", "u", k), 0, RIGHT, u, size)
    loads[1].wait()

    def build_table():
      with jax.named_scope('table'):
            loads[4].wait()
            lists_taken(RING, 2)
            npart = meta.shape[3]
            ckey = cidx[0:1, :] * 4096 + cidx[1:2, :]
            eye = lax.broadcasted_iota(jnp.int32, (nc, nc), 0) == lax.broadcasted_iota(jnp.int32, (nc, nc), 1)
            ccol = jnp.sum(jnp.where(eye, jnp.broadcast_to(ckey, (nc, nc)), 0), axis=1, keepdims=True)
            lane = lax.broadcasted_iota(jnp.int32, (nc, 128), 1)
            table = jnp.zeros((nc, 128), jnp.int32)
            for slot in range(2 * RING):
                pkey = meta[slot, 1, 0:1, :] * 4096 + meta[slot, 1, 1:2, :]
                pval = meta[slot, 0, 0:1, :] * 4096 + meta[slot, 0, 1:2, :] - na * 4096
                hit = jnp.broadcast_to(ccol, (nc, npart)) == jnp.broadcast_to(pkey, (nc, npart))
                found = jnp.sum(jnp.where(hit, jnp.broadcast_to(pval, (nc, npart)), 0), axis=1, keepdims=True) + na * 4096
                a_at = nb + jnp.clip(lax.shift_right_arithmetic(found, 12), 0, na)
                b_at = jnp.clip(found & 4095, 0, nb - 1)
                table = jnp.where(lane == 2 * slot, a_at, table)
                table = jnp.where(lane == 2 * slot + 1, b_at, table)
            tab_v[...] = table
            pltpu.make_async_copy(tab_v, tab_s, loc_sem.at[5]).start()

    def stage(d, sides=(0, 1), lo=0, hi=nc, group=24, first=False):
        def product(side, c):
            ref, n = (twin if side else mine)[d], 4 * d + 2 * side
            p = jnp.dot(ref[tab_s[c, n]], ref[tab_s[c, n + 1]], preferred_element_type=jnp.float32)
            return p.astype(jnp.bfloat16).astype(jnp.float32)

        def body(step, carry):
            for sub in range(group):
                c = step * group + sub
                total = product(sides[0], c)
                for side in sides[1:]:
                    total = total + product(side, c)
                acc[c] = total if first else acc[c] + total
            return carry

        with jax.named_scope(f'stage{d}_{len(sides)}{sides[0]}_{lo}'):
            lax.fori_loop(lo // group, hi // group, body, 0)

    def ready(d):
        take_twin = twin[d].at[pl.ds(0, nb + na)]
        with jax.named_scope(f'ready{d}'):
            pltpu.make_async_copy(take_twin, take_twin, drecv.at[d]).wait()

    def y_taken(cols, k):
        u, v, size = lay(k, theirs)
        arrive(("y", cols, k), 2 * size * len(cols))
        for d in cols:
            share(d, u, size)
            share(d, v, size)

    near = (LEFT, RIGHT)
    third = nc // 3

    for n, pair in enumerate(w_pieces):
        for link, d, (off, size, goes_on) in zip(("x+", "x-"), (LEFT, RIGHT), pair):
            arrive((link, "w", n), size)
            send("y+", ("yw", near), d, d, q0 + off, size)
            send("y-", ("yw", near), d, d, q0 + off, size)
            if goes_on:
                send(link, ("f", "w"), d, FAR, q0 + off, size)
            share(d, q0 + off, size)
    share(0, 0, nb + na)

    def spread(k):
        (up, up_size), (down, down_size) = parts if k == 0 else parts[::-1]
        for d in (near if k == 0 else (FAR,)):
            send("y+", ("g", k), d, d, qm + up, up_size)
            send("y-", ("g", k), d, d, qp + down, down_size)
            share(d, qm, quad)
            share(d, qp, quad)

    for k in range(nk):
        u, v, size = lay(k, own)
        if k == nk - 1:
            for part in range(2):
                send("x+", ("a", part), 0, LEFT, nb + part * ah, ah)
                send("x-", ("a", part), 0, RIGHT, nb + (1 - part) * ah, ah)
        arrive(("x+", "u", k), size)
        send("y+", ("y", near, k), LEFT, LEFT, u, size)
        send("x+", ("f", k), LEFT, FAR, u, size)
        arrive(("x-", "v", k), size)
        send("y-", ("y", near, k), RIGHT, RIGHT, v, size)
        send("x-", ("f", k), RIGHT, FAR, v, size)
        share(LEFT, u, size)
        share(RIGHT, v, size)
        if k == 0:
            lists_taken(RING - 1, 1)
            for d in range(1, RING):
                list_to(2 * d + 1, 2 * d, sib, 2)
        elif k == 1:
            arrive(("yw", near), 4 * quad)
            spread(0)
        elif k == 2:
            stage(0, lo=third, hi=2 * third, first=True)
            y_taken(near, 0)
        elif k == 3:
            y_taken(near, 1)
        arrive(("x+", "v", k), size)
        send("y-", ("y", near, k), LEFT, LEFT, v, size)
        arrive(("x-", "u", k), size)
        send("y+", ("y", near, k), RIGHT, RIGHT, u, size)
        share(LEFT, v, size)
        share(RIGHT, u, size)
        if k == 0:
            build_table()
        elif k == 1:
            pltpu.make_async_copy(tab_v, tab_s, loc_sem.at[5]).wait()
            ready(0)
            stage(0, hi=third, first=True)
        elif k == 2:
            stage(0, lo=2 * third, first=True)
    arrive(("g", 0), 2 * quad)
    for d in near:
        share(d, qf, quad)

    def far_block(k):
        u, v, size = lay(k, own)
        arrive(("f", k), 2 * size)
        send("y+", ("y", (FAR,), k), FAR, FAR, u, size)
        send("y-", ("y", (FAR,), k), FAR, FAR, v, size)
        share(FAR, u, size)
        share(FAR, v, size)

    arrive(("f", "w"), quad)
    send("y+", ("yw", FAR), FAR, FAR, q0, quad)
    send("y-", ("yw", FAR), FAR, FAR, q0, quad)
    share(FAR, q0, quad)
    y_taken(near, 2)
    far_block(0)
    far_block(1)
    y_taken(near, 3)
    far_block(2)
    arrive(("yw", FAR), 2 * quad)
    spread(1)
    y_taken((FAR,), 0)

    arrive(("a", 0), 2 * ah)
    send("x+", ("f", "a"), LEFT, FAR, nb, ah)
    send("x-", ("f", "a"), RIGHT, FAR, nb + ah, ah)
    share(LEFT, nb, ah)
    share(RIGHT, nb + ah, ah)
    arrive(("a", 1), 2 * ah)
    share(LEFT, nb + ah, ah)
    share(RIGHT, nb, ah)
    stage(LEFT, (0,))
    ready(LEFT)
    stage(LEFT, (1,))
    y_taken((FAR,), 1)
    far_block(3)
    ready(RIGHT)
    stage(RIGHT)
    y_taken((FAR,), 2)
    arrive(("g", 1), quad)
    share(FAR, qf, quad)
    y_taken((FAR,), 3)
    arrive(("f", "a"), 2 * ah)
    share(FAR, nb, na)
    stage(FAR, (0,), group=nc // 2)
    ready(FAR)
    stage(FAR, (1,), group=nc // 2)

    assert load_of == waited and len(sems) == recv_sem.shape[0], len(sems)
    with jax.named_scope('sendwaits'):
        for slot, size in enumerate(link_of):
            take(size, link_sem.at[slot])
        own_meta = meta.at[pl.ds(0, 2 * RING - 1)]
        pltpu.make_async_copy(own_meta, own_meta, msem.at[0]).wait()
        for d in range(RING):
            take(nb + na, dsend.at[d])


def solution(mesh):
    row_spec = P(('batch', 'rows'), 'ksplit')
    col_spec = P(('batch', 'ksplit'))
    assert mesh.shape['rows'] == RING and mesh.shape['ksplit'] == 2 * RING

    def device_step(a_loc, b_loc, pair_loc, plist_loc, cidx_loc):
        a, b = a_loc[0, 0], b_loc[0]
        pairs = pair_loc[0, 0, :, 0, :].T
        plist = plist_loc[0, 0].T
        cidx = cidx_loc[0, 0].T
        na, nb, nc, size = a.shape[0], b.shape[0], cidx.shape[1], a.shape[-1]
        npart = plist.shape[1]
        nsem = 14 + 7 * len(HALF_CHUNKS)
        block = (size, size)
        args = [pltpu.with_memory_space_constraint(t, pltpu.HBM) for t in (a, b, pairs, plist, cidx)]
        out = pl.pallas_call(
            functools.partial(kernel, na, nb, nc),
            out_shape=jax.ShapeDtypeStruct((nc, *block), jnp.float32),
            in_specs=[pl.BlockSpec(memory_space=pltpu.HBM)] * 5,
            out_specs=pl.BlockSpec(memory_space=pltpu.VMEM),
            scratch_shapes=[
                *[pltpu.VMEM((nb + na + 1, *block), b.dtype) for _ in range(2 * RING)],
                pltpu.VMEM((2 * RING, 2, 2, npart), jnp.int32),
                pltpu.VMEM((2, nc), jnp.int32),
                pltpu.VMEM((nc, 128), jnp.int32),
                pltpu.SMEM((nc, 128), jnp.int32),
                pltpu.SemaphoreType.DMA((6,)),
                pltpu.SemaphoreType.DMA((4,)),
                pltpu.SemaphoreType.DMA((nsem,)),
                pltpu.SemaphoreType.DMA((RING,)),
                pltpu.SemaphoreType.DMA((RING,)),
                pltpu.SemaphoreType.DMA((3,)),
            ],
            compiler_params=pltpu.CompilerParams(
                collective_id=0, has_side_effects=True, vmem_limit_bytes=30 * 2**20),
        )(*args)
        return out[None, None]

    return jax.shard_map(device_step, mesh=mesh, in_specs=(row_spec, col_spec, row_spec, row_spec, row_spec), out_specs=row_spec, check_vma=False)
```

```python
import functools

import jax
import jax.numpy as jnp
from jax import lax
from jax.experimental import pallas as pl
from jax.experimental.pallas import tpu as pltpu
from jax.sharding import PartitionSpec as P


MESH = pl.DeviceIdType.MESH
RING = 4
HALF_CHUNKS = (3, 3, 3, 2, 2)
LEFT, RIGHT, FAR = 3, 1, 2


def plan(nb):
    half = sum(HALF_CHUNKS)
    quad = (nb - 4 * half) // RING
    assert 4 * half + RING * quad == nb
    return half, quad


def kernel(na, nb, nc, a_hbm, b_hbm, pairs_hbm, plist_hbm, cidx_hbm, acc, *scratch):
    mine, twin = scratch[0:RING], scratch[RING:2 * RING]
    (meta, cidx, tab_v, tab_s, loc_sem, link_sem, recv_sem, dsend, drecv, msem) = scratch[2 * RING:]
    half, quad = plan(nb)
    nk, ah = len(HALF_CHUNKS), na // 2
    parts = ((0, quad // 2), (quad // 2, quad - quad // 2))
    offs = [(sum(HALF_CHUNKS[:k]), HALF_CHUNKS[k]) for k in range(nk)]
    ks = lax.axis_index("ksplit")
    y = lax.axis_index("rows")
    core = ks % 2
    x = ks // 2

    def chip(dx, flip=0):
        return {"ksplit": ((x + dx) % RING) * 2 + (1 - core if flip else core)}

    sib = chip(0, 1)
    links = {
        "x+": (0, chip(1)), "x-": (1, chip(3)),
        "y+": (2, {"rows": (y + 1) % RING}), "y-": (3, {"rows": (y + 3) % RING}),
    }

    loads = [
        pltpu.make_async_copy(b_hbm, mine[0].at[pl.ds(0, nb)], loc_sem.at[0]),
        pltpu.make_async_copy(a_hbm, mine[0].at[pl.ds(nb, na)], loc_sem.at[1]),
        pltpu.make_async_copy(pairs_hbm, meta.at[0, 0], loc_sem.at[2]),
        pltpu.make_async_copy(plist_hbm, meta.at[0, 1], loc_sem.at[3]),
        pltpu.make_async_copy(cidx_hbm, cidx, loc_sem.at[4]),
    ]
    for load in loads:
        load.start()

    barrier = pltpu.get_barrier_semaphore()
    devices = [dev for _, dev in links.values()] + [chip(2), sib]
    for dev in devices:
        pl.semaphore_signal(barrier, inc=1, device_id=dev, device_id_type=MESH)
    zero = jnp.zeros(mine[0].shape[1:], mine[0].dtype)
    for ref in (*mine, *twin):
        ref[nb + na] = zero
    with jax.named_scope('barrier'):
        pl.semaphore_wait(barrier, len(devices))

    sems = {}
    load_of = {}
    link_of = [0] * len(links)

    def index(key):
        return sems.setdefault(key, len(sems))

    def send(link, key, src, dst, start, size):
        slot, dev = links[link]
        n = index(key)
        load_of[n] = load_of.get(n, 0) + size
        link_of[slot] += size
        pltpu.make_async_remote_copy(
            src_ref=mine[src].at[pl.ds(start, size)], dst_ref=mine[dst].at[pl.ds(start, size)],
            send_sem=link_sem.at[slot], recv_sem=recv_sem.at[n],
            device_id=dev, device_id_type=MESH).start()

    def take(size, sem):
        view = mine[0].at[pl.ds(0, size)]
        pltpu.make_async_copy(view, view, sem).wait()

    waited = {}

    def arrive(key, size):
        n = index(key)
        waited[n] = waited.get(n, 0) + size
        with jax.named_scope('_'.join(str(t) for t in key).replace('+', 'p').replace('-', 'm').replace(' ', '')):
            take(size, recv_sem.at[n])

    def share(d, start, size):
        pltpu.make_async_remote_copy(
            src_ref=mine[d].at[pl.ds(start, size)], dst_ref=twin[d].at[pl.ds(start, size)],
            send_sem=dsend.at[d], recv_sem=drecv.at[d], device_id=sib, device_id_type=MESH).start()

    own = (y % 2) * (2 * half)
    theirs = (1 - y % 2) * (2 * half)

    def quad_at(dy):
        return 4 * half + ((y + dy) % RING) * quad

    def lay(k, base):
        off, size = offs[k]
        return base + off, base + half + off, size

    q0, qm, qp, qf = quad_at(0), quad_at(3), quad_at(1), quad_at(2)

    loads[0].wait()
    def pieces(first, second):
        (off, size), rest = parts[first], parts[second]
        return ((off, 1, "f"), (off + 1, size - 1, "f"), (*rest, ""))

    w_pieces = list(zip(pieces(0, 1), pieces(1, 0)))
    for n, pair in enumerate(w_pieces):
        for link, d, (off, size, _) in zip(("x+", "x-"), (LEFT, RIGHT), pair):
            send(link, (link, "w", n), 0, d, q0 + off, size)
    loads[2].wait()
    loads[3].wait()

    def list_to(slot, src, dev, sem):
        pltpu.make_async_remote_copy(
            src_ref=meta.at[src], dst_ref=meta.at[slot], send_sem=msem.at[0], recv_sem=msem.at[sem],
            device_id=dev, device_id_type=MESH).start()

    def lists_taken(count, sem):
        view = meta.at[pl.ds(0, count)]
        pltpu.make_async_copy(view, view, msem.at[sem]).wait()

    for dx in range(1, RING):
        list_to(2 * (RING - dx), 0, chip(dx), 1)
    list_to(1, 0, sib, 2)
    for k in range(nk):
        u, v, size = lay(k, own)
        send("x+", ("x+", "u", k), 0, LEFT, u, size)
        send("x-", ("x-", "v", k), 0, RIGHT, v, size)
        send("x+", ("x+", "v", k), 0, LEFT, v, size)
        send("x-", ("x-", "u", k), 0, RIGHT, u, size)
    loads[1].wait()

    def build_table():
      with jax.named_scope('table'):
            loads[4].wait()
            lists_taken(RING, 2)
            npart = meta.shape[3]
            ckey = cidx[0:1, :] * 4096 + cidx[1:2, :]
            eye = lax.broadcasted_iota(jnp.int32, (nc, nc), 0) == lax.broadcasted_iota(jnp.int32, (nc, nc), 1)
            ccol = jnp.sum(jnp.where(eye, jnp.broadcast_to(ckey, (nc, nc)), 0), axis=1, keepdims=True)
            lane = lax.broadcasted_iota(jnp.int32, (nc, 128), 1)
            table = jnp.zeros((nc, 128), jnp.int32)
            for slot in range(2 * RING):
                pkey = meta[slot, 1, 0:1, :] * 4096 + meta[slot, 1, 1:2, :]
                pval = meta[slot, 0, 0:1, :] * 4096 + meta[slot, 0, 1:2, :] - na * 4096
                hit = jnp.broadcast_to(ccol, (nc, npart)) == jnp.broadcast_to(pkey, (nc, npart))
                found = jnp.sum(jnp.where(hit, jnp.broadcast_to(pval, (nc, npart)), 0), axis=1, keepdims=True) + na * 4096
                a_at = nb + jnp.clip(lax.shift_right_arithmetic(found, 12), 0, na)
                b_at = jnp.clip(found & 4095, 0, nb - 1)
                table = jnp.where(lane == 2 * slot, a_at, table)
                table = jnp.where(lane == 2 * slot + 1, b_at, table)
            tab_v[...] = table
            pltpu.make_async_copy(tab_v, tab_s, loc_sem.at[5]).start()

    def stage(d, sides=(0, 1), lo=0, hi=nc, group=24, first=False):
        def product(side, c):
            ref, n = (twin if side else mine)[d], 4 * d + 2 * side
            p = jnp.dot(ref[tab_s[c, n]], ref[tab_s[c, n + 1]], preferred_element_type=jnp.float32)
            return p.astype(jnp.bfloat16).astype(jnp.float32)

        def body(step, carry):
            for sub in range(group):
                c = step * group + sub
                total = product(sides[0], c)
                for side in sides[1:]:
                    total = total + product(side, c)
                acc[c] = total if first else acc[c] + total
            return carry

        with jax.named_scope(f'stage{d}_{len(sides)}{sides[0]}_{lo}'):
            lax.fori_loop(lo // group, hi // group, body, 0)

    def ready(d):
        take_twin = twin[d].at[pl.ds(0, nb + na)]
        with jax.named_scope(f'ready{d}'):
            pltpu.make_async_copy(take_twin, take_twin, drecv.at[d]).wait()

    def y_taken(cols, k):
        u, v, size = lay(k, theirs)
        arrive(("y", cols, k), 2 * size * len(cols))
        for d in cols:
            share(d, u, size)
            share(d, v, size)

    near = (LEFT, RIGHT)
    third = nc // 3

    for n, pair in enumerate(w_pieces):
        for link, d, (off, size, goes_on) in zip(("x+", "x-"), (LEFT, RIGHT), pair):
            arrive((link, "w", n), size)
            send("y+", ("yw", near), d, d, q0 + off, size)
            send("y-", ("yw", near), d, d, q0 + off, size)
            if goes_on:
                send(link, ("f", "w"), d, FAR, q0 + off, size)
            share(d, q0 + off, size)
    share(0, 0, nb + na)

    def spread(k):
        (up, up_size), (down, down_size) = parts if k == 0 else parts[::-1]
        for d in (near if k == 0 else (FAR,)):
            send("y+", ("g", k), d, d, qm + up, up_size)
            send("y-", ("g", k), d, d, qp + down, down_size)
            share(d, qm, quad)
            share(d, qp, quad)

    for k in range(nk):
        u, v, size = lay(k, own)
        if k == nk - 1:
            for part in range(2):
                send("x+", ("a", part), 0, LEFT, nb + part * ah, ah)
                send("x-", ("a", part), 0, RIGHT, nb + (1 - part) * ah, ah)
        arrive(("x+", "u", k), size)
        send("y+", ("y", near, k), LEFT, LEFT, u, size)
        send("x+", ("f", k), LEFT, FAR, u, size)
        arrive(("x-", "v", k), size)
        send("y-", ("y", near, k), RIGHT, RIGHT, v, size)
        send("x-", ("f", k), RIGHT, FAR, v, size)
        share(LEFT, u, size)
        share(RIGHT, v, size)
        if k == 0:
            lists_taken(RING - 1, 1)
            for d in range(1, RING):
                list_to(2 * d + 1, 2 * d, sib, 2)
        elif k == 1:
            arrive(("yw", near), 4 * quad)
            spread(0)
        elif k == 2:
            stage(0, lo=third, hi=2 * third, first=True)
            y_taken(near, 0)
        elif k == 3:
            y_taken(near, 1)
        arrive(("x+", "v", k), size)
        send("y-", ("y", near, k), LEFT, LEFT, v, size)
        arrive(("x-", "u", k), size)
        send("y+", ("y", near, k), RIGHT, RIGHT, u, size)
        share(LEFT, v, size)
        share(RIGHT, u, size)
        if k == 0:
            build_table()
        elif k == 1:
            pltpu.make_async_copy(tab_v, tab_s, loc_sem.at[5]).wait()
            ready(0)
            stage(0, hi=third, first=True)
        elif k == 2:
            stage(0, lo=2 * third, first=True)
    arrive(("g", 0), 2 * quad)
    for d in near:
        share(d, qf, quad)

    def far_block(k):
        u, v, size = lay(k, own)
        arrive(("f", k), 2 * size)
        send("y+", ("y", (FAR,), k), FAR, FAR, u, size)
        send("y-", ("y", (FAR,), k), FAR, FAR, v, size)
        share(FAR, u, size)
        share(FAR, v, size)

    arrive(("f", "w"), quad)
    send("y+", ("yw", FAR), FAR, FAR, q0, quad)
    send("y-", ("yw", FAR), FAR, FAR, q0, quad)
    share(FAR, q0, quad)
    y_taken(near, 2)
    far_block(0)
    far_block(1)
    y_taken(near, 3)
    far_block(2)
    y_taken(near, 4)
    far_block(3)
    arrive(("yw", FAR), 2 * quad)
    spread(1)
    y_taken((FAR,), 0)

    arrive(("a", 0), 2 * ah)
    send("x+", ("f", "a"), LEFT, FAR, nb, ah)
    send("x-", ("f", "a"), RIGHT, FAR, nb + ah, ah)
    share(LEFT, nb, ah)
    share(RIGHT, nb + ah, ah)
    arrive(("a", 1), 2 * ah)
    share(LEFT, nb + ah, ah)
    share(RIGHT, nb, ah)
    stage(LEFT, (0,))
    far_block(4)
    stage(RIGHT, (0,))
    y_taken((FAR,), 1)
    ready(LEFT)
    stage(LEFT, (1,))
    y_taken((FAR,), 2)
    ready(RIGHT)
    stage(RIGHT, (1,))
    arrive(("g", 1), quad)
    share(FAR, qf, quad)
    y_taken((FAR,), 3)
    arrive(("f", "a"), 2 * ah)
    share(FAR, nb, na)
    y_taken((FAR,), 4)
    stage(FAR, (0,), group=nc // 2)
    ready(FAR)
    stage(FAR, (1,), group=nc // 2)

    assert load_of == waited and len(sems) == recv_sem.shape[0], len(sems)
    with jax.named_scope('sendwaits'):
        for slot, size in enumerate(link_of):
            take(size, link_sem.at[slot])
        own_meta = meta.at[pl.ds(0, 2 * RING - 1)]
        pltpu.make_async_copy(own_meta, own_meta, msem.at[0]).wait()
        for d in range(RING):
            take(nb + na, dsend.at[d])


def solution(mesh):
    row_spec = P(('batch', 'rows'), 'ksplit')
    col_spec = P(('batch', 'ksplit'))
    assert mesh.shape['rows'] == RING and mesh.shape['ksplit'] == 2 * RING

    def device_step(a_loc, b_loc, pair_loc, plist_loc, cidx_loc):
        a, b = a_loc[0, 0], b_loc[0]
        pairs = pair_loc[0, 0, :, 0, :].T
        plist = plist_loc[0, 0].T
        cidx = cidx_loc[0, 0].T
        na, nb, nc, size = a.shape[0], b.shape[0], cidx.shape[1], a.shape[-1]
        npart = plist.shape[1]
        nsem = 14 + 7 * len(HALF_CHUNKS)
        block = (size, size)
        args = [pltpu.with_memory_space_constraint(t, pltpu.HBM) for t in (a, b, pairs, plist, cidx)]
        out = pl.pallas_call(
            functools.partial(kernel, na, nb, nc),
            out_shape=jax.ShapeDtypeStruct((nc, *block), jnp.float32),
            in_specs=[pl.BlockSpec(memory_space=pltpu.HBM)] * 5,
            out_specs=pl.BlockSpec(memory_space=pltpu.VMEM),
            scratch_shapes=[
                *[pltpu.VMEM((nb + na + 1, *block), b.dtype) for _ in range(2 * RING)],
                pltpu.VMEM((2 * RING, 2, 2, npart), jnp.int32),
                pltpu.VMEM((2, nc), jnp.int32),
                pltpu.VMEM((nc, 128), jnp.int32),
                pltpu.SMEM((nc, 128), jnp.int32),
                pltpu.SemaphoreType.DMA((6,)),
                pltpu.SemaphoreType.DMA((4,)),
                pltpu.SemaphoreType.DMA((nsem,)),
                pltpu.SemaphoreType.DMA((RING,)),
                pltpu.SemaphoreType.DMA((RING,)),
                pltpu.SemaphoreType.DMA((3,)),
            ],
            compiler_params=pltpu.CompilerParams(
                collective_id=0, has_side_effects=True, vmem_limit_bytes=30 * 2**20),
        )(*args)
        return out[None, None]

    return jax.shard_map(device_step, mesh=mesh, in_specs=(row_spec, col_spec, row_spec, row_spec, row_spec), out_specs=row_spec, check_vma=False)
```

```python
import functools

import jax
import jax.numpy as jnp
from jax import lax
from jax.experimental import pallas as pl
from jax.experimental.pallas import tpu as pltpu
from jax.sharding import PartitionSpec as P


MESH = pl.DeviceIdType.MESH
RING = 4
HALF_CHUNKS = (3, 3, 3, 2, 2)
LEFT, RIGHT, FAR = 3, 1, 2


def plan(nb):
    half = sum(HALF_CHUNKS)
    quad = (nb - 4 * half) // RING
    assert 4 * half + RING * quad == nb
    return half, quad


def kernel(na, nb, nc, a_hbm, b_hbm, pairs_hbm, plist_hbm, cidx_hbm, acc, far_twin, far_tab, *scratch):
    mine, twin = scratch[0:RING], list(scratch[RING:2 * RING - 1])
    twin.insert(FAR, far_twin)
    (meta, cidx, tab_v, tab_s, loc_sem, link_sem, recv_sem, dsend, drecv, msem) = scratch[2 * RING - 1:]
    half, quad = plan(nb)
    nk, ah = len(HALF_CHUNKS), na // 2
    parts = ((0, quad // 2), (quad // 2, quad - quad // 2))
    offs = [(sum(HALF_CHUNKS[:k]), HALF_CHUNKS[k]) for k in range(nk)]
    ks = lax.axis_index("ksplit")
    y = lax.axis_index("rows")
    core = ks % 2
    x = ks // 2

    def chip(dx, flip=0):
        return {"ksplit": ((x + dx) % RING) * 2 + (1 - core if flip else core)}

    sib = chip(0, 1)
    links = {
        "x+": (0, chip(1)), "x-": (1, chip(3)),
        "y+": (2, {"rows": (y + 1) % RING}), "y-": (3, {"rows": (y + 3) % RING}),
    }

    loads = [
        pltpu.make_async_copy(b_hbm, mine[0].at[pl.ds(0, nb)], loc_sem.at[0]),
        pltpu.make_async_copy(a_hbm, mine[0].at[pl.ds(nb, na)], loc_sem.at[1]),
        pltpu.make_async_copy(pairs_hbm, meta.at[0, 0], loc_sem.at[2]),
        pltpu.make_async_copy(plist_hbm, meta.at[0, 1], loc_sem.at[2]),
        pltpu.make_async_copy(cidx_hbm, cidx, loc_sem.at[3]),
    ]
    for load in loads:
        load.start()

    barrier = pltpu.get_barrier_semaphore()
    devices = [dev for _, dev in links.values()] + [chip(2), sib]
    for dev in devices:
        pl.semaphore_signal(barrier, inc=1, device_id=dev, device_id_type=MESH)
    zero = jnp.zeros(mine[0].shape[1:], mine[0].dtype)
    for ref in (*mine, *twin):
        ref[nb + na] = zero
    with jax.named_scope('barrier'):
        pl.semaphore_wait(barrier, len(devices))

    sems = {}
    load_of = {}
    link_of = [0] * len(links)

    def index(key):
        return sems.setdefault(key, len(sems))

    def send(link, key, src, dst, start, size):
        slot, dev = links[link]
        n = index(key)
        load_of[n] = load_of.get(n, 0) + size
        link_of[slot] += size
        pltpu.make_async_remote_copy(
            src_ref=mine[src].at[pl.ds(start, size)], dst_ref=mine[dst].at[pl.ds(start, size)],
            send_sem=link_sem.at[slot], recv_sem=recv_sem.at[n],
            device_id=dev, device_id_type=MESH).start()

    def take(size, sem):
        view = mine[0].at[pl.ds(0, size)]
        pltpu.make_async_copy(view, view, sem).wait()

    waited = {}

    def arrive(key, size):
        n = index(key)
        waited[n] = waited.get(n, 0) + size
        with jax.named_scope('_'.join(str(t) for t in key).replace('+', 'p').replace('-', 'm').replace(' ', '')):
            take(size, recv_sem.at[n])

    def share(d, start, size):
        pltpu.make_async_remote_copy(
            src_ref=mine[d].at[pl.ds(start, size)], dst_ref=twin[d].at[pl.ds(start, size)],
            send_sem=dsend.at[d], recv_sem=drecv.at[d], device_id=sib, device_id_type=MESH).start()

    own = (y % 2) * (2 * half)
    theirs = (1 - y % 2) * (2 * half)

    def quad_at(dy):
        return 4 * half + ((y + dy) % RING) * quad

    def lay(k, base):
        off, size = offs[k]
        return base + off, base + half + off, size

    q0, qm, qp, qf = quad_at(0), quad_at(3), quad_at(1), quad_at(2)

    loads[0].wait()
    def pieces(first, second):
        (off, size), rest = parts[first], parts[second]
        return ((off, 1, "f"), (off + 1, size - 1, "f"), (*rest, ""))

    w_pieces = list(zip(pieces(0, 1), pieces(1, 0)))
    for n, pair in enumerate(w_pieces):
        for link, d, (off, size, _) in zip(("x+", "x-"), (LEFT, RIGHT), pair):
            send(link, ("xw", n), 0, d, q0 + off, size)
    pltpu.make_async_copy(meta.at[0], meta.at[0], loc_sem.at[2]).wait()

    def list_to(slot, src, dev, sem):
        pltpu.make_async_remote_copy(
            src_ref=meta.at[src], dst_ref=meta.at[slot], send_sem=msem.at[0], recv_sem=msem.at[sem],
            device_id=dev, device_id_type=MESH).start()

    def lists_taken(count, sem):
        view = meta.at[pl.ds(0, count)]
        pltpu.make_async_copy(view, view, msem.at[sem]).wait()

    for dx in range(1, RING):
        list_to(2 * (RING - dx), 0, chip(dx), 1)
    list_to(1, 0, sib, 2)
    for k in range(nk):
        u, v, size = lay(k, own)
        send("x+", ("x", k, 0), 0, LEFT, u, size)
        send("x-", ("x", k, 0), 0, RIGHT, v, size)
        send("x+", ("x", k, 1), 0, LEFT, v, size)
        send("x-", ("x", k, 1), 0, RIGHT, u, size)
    loads[1].wait()

    def build_table():
      with jax.named_scope('table'):
            loads[4].wait()
            lists_taken(RING, 2)
            npart = meta.shape[3]
            ckey = cidx[0:1, :] * 4096 + cidx[1:2, :]
            eye = lax.broadcasted_iota(jnp.int32, (nc, nc), 0) == lax.broadcasted_iota(jnp.int32, (nc, nc), 1)
            ccol = jnp.sum(jnp.where(eye, jnp.broadcast_to(ckey, (nc, nc)), 0), axis=1, keepdims=True)
            lane = lax.broadcasted_iota(jnp.int32, (nc, 128), 1)
            table = jnp.zeros((nc, 128), jnp.int32)
            for slot in range(2 * RING):
                pkey = meta[slot, 1, 0:1, :] * 4096 + meta[slot, 1, 1:2, :]
                pval = meta[slot, 0, 0:1, :] * 4096 + meta[slot, 0, 1:2, :] - na * 4096
                hit = jnp.broadcast_to(ccol, (nc, npart)) == jnp.broadcast_to(pkey, (nc, npart))
                found = jnp.sum(jnp.where(hit, jnp.broadcast_to(pval, (nc, npart)), 0), axis=1, keepdims=True) + na * 4096
                a_at = nb + jnp.clip(lax.shift_right_arithmetic(found, 12), 0, na)
                b_at = jnp.clip(found & 4095, 0, nb - 1)
                table = jnp.where(lane == 2 * slot, a_at, table)
                table = jnp.where(lane == 2 * slot + 1, b_at, table)
                if slot == 2 * FAR + 1:
                    for n, column in enumerate((a_at, b_at)):
                        row = jnp.sum(jnp.where(eye, jnp.broadcast_to(column, (nc, nc)), 0), axis=0, keepdims=True)
                        far_tab[n:n + 1, 0:nc] = row
            tab_v[...] = table
            pltpu.make_async_copy(tab_v, tab_s, loc_sem.at[3]).start()

    def stage(d, sides=(0, 1), lo=0, hi=nc, group=24, first=False):
        def product(side, c):
            ref, n = (twin if side else mine)[d], 4 * d + 2 * side
            p = jnp.dot(ref[tab_s[c, n]], ref[tab_s[c, n + 1]], preferred_element_type=jnp.float32)
            return p.astype(jnp.bfloat16).astype(jnp.float32)

        def body(step, carry):
            for sub in range(group):
                c = step * group + sub
                total = product(sides[0], c)
                for side in sides[1:]:
                    total = total + product(side, c)
                acc[c] = total if first else acc[c] + total
            return carry

        with jax.named_scope(f'stage{d}_{len(sides)}{sides[0]}_{lo}'):
            lax.fori_loop(lo // group, hi // group, body, 0)

    def ready(d):
        take_twin = twin[d].at[pl.ds(0, nb + na)]
        with jax.named_scope(f'ready{d}'):
            pltpu.make_async_copy(take_twin, take_twin, drecv.at[d]).wait()

    def y_taken(cols, k):
        u, v, size = lay(k, theirs)
        arrive(("y", cols, k), 2 * size * len(cols))
        for d in cols:
            share(d, u, size)
            share(d, v, size)

    near = (LEFT, RIGHT)
    third = nc // 3

    for n, pair in enumerate(w_pieces):
        arrive(("xw", n), sum(size for _, size, _ in pair))
        for link, d, (off, size, goes_on) in zip(("x+", "x-"), (LEFT, RIGHT), pair):
            send("y+", ("yw", near), d, d, q0 + off, size)
            send("y-", ("yw", near), d, d, q0 + off, size)
            if goes_on:
                send(link, ("f", "w"), d, FAR, q0 + off, size)
            share(d, q0 + off, size)
    share(0, 0, nb + na)

    def spread(k):
        (up, up_size), (down, down_size) = parts if k == 0 else parts[::-1]
        for d in (near if k == 0 else (FAR,)):
            send("y+", ("g", k), d, d, qm + up, up_size)
            send("y-", ("g", k), d, d, qp + down, down_size)
            share(d, qm, quad)
            share(d, qp, quad)

    for k in range(nk):
        u, v, size = lay(k, own)
        if k == nk - 1:
            for part in range(2):
                send("x+", ("a", part), 0, LEFT, nb + part * ah, ah)
                send("x-", ("a", part), 0, RIGHT, nb + (1 - part) * ah, ah)
        arrive(("x", k, 0), 2 * size)
        send("y+", ("y", near, k), LEFT, LEFT, u, size)
        send("x+", ("f", k), LEFT, FAR, u, size)
        send("y-", ("y", near, k), RIGHT, RIGHT, v, size)
        send("x-", ("f", k), RIGHT, FAR, v, size)
        share(LEFT, u, size)
        share(RIGHT, v, size)
        if k == 0:
            lists_taken(RING - 1, 1)
            for d in range(1, RING):
                list_to(2 * d + 1, 2 * d, sib, 2)
        elif k == 1:
            arrive(("yw", near), 4 * quad)
            spread(0)
        elif k == 2:
            stage(0, lo=third, hi=2 * third, first=True)
            y_taken(near, 0)
        elif k == 3:
            y_taken(near, 1)
        arrive(("x", k, 1), 2 * size)
        send("y-", ("y", near, k), LEFT, LEFT, v, size)
        send("y+", ("y", near, k), RIGHT, RIGHT, u, size)
        share(LEFT, v, size)
        share(RIGHT, u, size)
        if k == 0:
            build_table()
        elif k == 1:
            pltpu.make_async_copy(tab_v, tab_s, loc_sem.at[3]).wait()
            ready(0)
            stage(0, hi=third, first=True)
        elif k == 2:
            stage(0, lo=2 * third, first=True)
    arrive(("g", 0), 2 * quad)
    for d in near:
        share(d, qf, quad)

    def far_block(k):
        u, v, size = lay(k, own)
        arrive(("f", k), 2 * size)
        send("y+", ("y", (FAR,), k), FAR, FAR, u, size)
        send("y-", ("y", (FAR,), k), FAR, FAR, v, size)
        share(FAR, u, size)
        share(FAR, v, size)

    arrive(("f", "w"), quad)
    send("y+", ("yw", FAR), FAR, FAR, q0, quad)
    send("y-", ("yw", FAR), FAR, FAR, q0, quad)
    share(FAR, q0, quad)
    y_taken(near, 2)
    far_block(0)
    far_block(1)
    y_taken(near, 3)
    far_block(2)
    y_taken(near, 4)
    far_block(3)
    arrive(("yw", FAR), 2 * quad)
    spread(1)
    y_taken((FAR,), 0)

    arrive(("a", 0), 2 * ah)
    send("x+", ("f", "a"), LEFT, FAR, nb, ah)
    send("x-", ("f", "a"), RIGHT, FAR, nb + ah, ah)
    share(LEFT, nb, ah)
    share(RIGHT, nb + ah, ah)
    arrive(("a", 1), 2 * ah)
    share(LEFT, nb + ah, ah)
    share(RIGHT, nb, ah)
    stage(LEFT, (0,))
    far_block(4)
    stage(RIGHT, (0,))
    y_taken((FAR,), 1)
    ready(LEFT)
    stage(LEFT, (1,))
    y_taken((FAR,), 2)
    ready(RIGHT)
    stage(RIGHT, (1,))
    arrive(("g", 1), quad)
    share(FAR, qf, quad)
    y_taken((FAR,), 3)
    arrive(("f", "a"), 2 * ah)
    share(FAR, nb, na)
    y_taken((FAR,), 4)
    stage(FAR, (0,), group=nc // 2)
    ready(FAR)

    assert load_of == waited and len(sems) == recv_sem.shape[0], len(sems)
    with jax.named_scope('sendwaits'):
        for slot, size in enumerate(link_of):
            take(size, link_sem.at[slot])
        own_meta = meta.at[pl.ds(0, 2 * RING - 1)]
        pltpu.make_async_copy(own_meta, own_meta, msem.at[0]).wait()
        for d in range(RING):
            take(nb + na, dsend.at[d])


def finish(cuts, acc, far, tab, out_hbm, buf, tab_s, tab_sem, out_sem):
    table = pltpu.make_async_copy(tab, tab_s, tab_sem)
    table.start()
    table.wait()
    outs, lo = [], 0
    for n, hi in enumerate(cuts):
        for c in range(lo, hi):
            p = jnp.dot(far[tab_s[0, c]], far[tab_s[1, c]], preferred_element_type=jnp.float32)
            buf[c] = acc[c] + p.astype(jnp.bfloat16).astype(jnp.float32)
        view = pl.ds(lo, hi - lo)
        outs.append(pltpu.make_async_copy(buf.at[view], out_hbm.at[view], out_sem.at[n]))
        outs[-1].start()
        lo = hi
    for copy in outs:
        copy.wait()


def solution(mesh):
    row_spec = P(('batch', 'rows'), 'ksplit')
    col_spec = P(('batch', 'ksplit'))
    assert mesh.shape['rows'] == RING and mesh.shape['ksplit'] == 2 * RING

    def device_step(a_loc, b_loc, pair_loc, plist_loc, cidx_loc):
        a, b = a_loc[0, 0], b_loc[0]
        pairs = pair_loc[0, 0, :, 0, :].T
        plist = plist_loc[0, 0].T
        cidx = cidx_loc[0, 0].T
        na, nb, nc, size = a.shape[0], b.shape[0], cidx.shape[1], a.shape[-1]
        npart = plist.shape[1]
        nsem = 11 + 5 * len(HALF_CHUNKS)
        block = (size, size)
        args = [pltpu.with_memory_space_constraint(t, pltpu.HBM) for t in (a, b, pairs, plist, cidx)]
        acc, far, tab = pl.pallas_call(
            functools.partial(kernel, na, nb, nc),
            out_shape=(
                jax.ShapeDtypeStruct((nc, *block), jnp.float32),
                jax.ShapeDtypeStruct((nb + na + 1, *block), b.dtype),
                jax.ShapeDtypeStruct((2, 128), jnp.int32),
            ),
            in_specs=[pl.BlockSpec(memory_space=pltpu.HBM)] * 5,
            out_specs=(pl.BlockSpec(memory_space=pltpu.VMEM),) * 3,
            scratch_shapes=[
                *[pltpu.VMEM((nb + na + 1, *block), b.dtype) for _ in range(2 * RING - 1)],
                pltpu.VMEM((2 * RING, 2, 2, npart), jnp.int32),
                pltpu.VMEM((2, nc), jnp.int32),
                pltpu.VMEM((nc, 128), jnp.int32),
                pltpu.SMEM((nc, 128), jnp.int32),
                pltpu.SemaphoreType.DMA((4,)),
                pltpu.SemaphoreType.DMA((4,)),
                pltpu.SemaphoreType.DMA((nsem,)),
                pltpu.SemaphoreType.DMA((RING,)),
                pltpu.SemaphoreType.DMA((RING,)),
                pltpu.SemaphoreType.DMA((3,)),
            ],
            compiler_params=pltpu.CompilerParams(
                collective_id=0, has_side_effects=True, vmem_limit_bytes=30 * 2**20),
        )(*args)
        cuts = tuple(nc * n // 6 for n in (2, 4, 5, 6))
        vmem = pl.BlockSpec(memory_space=pltpu.VMEM)
        out = pl.pallas_call(
            functools.partial(finish, cuts),
            out_shape=jax.ShapeDtypeStruct((nc, *block), jnp.float32),
            in_specs=[vmem] * 3,
            out_specs=pl.BlockSpec(memory_space=pltpu.HBM),
            scratch_shapes=[
                pltpu.VMEM((nc, *block), jnp.float32),
                pltpu.SMEM((2, 128), jnp.int32),
                pltpu.SemaphoreType.DMA,
                pltpu.SemaphoreType.DMA((len(cuts),)),
            ],
            compiler_params=pltpu.CompilerParams(vmem_limit_bytes=8 * 2**20),
        )(acc, far, tab)
        return out[None, None]

    return jax.shard_map(device_step, mesh=mesh, in_specs=(row_spec, col_spec, row_spec, row_spec, row_spec), out_specs=row_spec, check_vma=False)
```

```python
import functools

import jax
import jax.numpy as jnp
from jax import lax
from jax.experimental import pallas as pl
from jax.experimental.pallas import tpu as pltpu
from jax.sharding import PartitionSpec as P


MESH = pl.DeviceIdType.MESH
RING = 4
HALF_CHUNKS = (3, 3, 3, 2, 2)
LEFT, RIGHT, FAR = 3, 1, 2


def plan(nb):
    half = sum(HALF_CHUNKS)
    quad = (nb - 4 * half) // RING
    assert 4 * half + RING * quad == nb
    return half, quad


def kernel(na, nb, nc, head, a_hbm, b_hbm, pairs_hbm, plist_hbm, cidx_hbm, acc, far_twin, far_tab, *scratch):
    mine, twin = scratch[0:RING], list(scratch[RING:2 * RING - 1])
    twin.insert(FAR, far_twin)
    (meta, cidx, tab_v, tab_s, loc_sem, link_sem, recv_sem, dsend, drecv, msem) = scratch[2 * RING - 1:]
    half, quad = plan(nb)
    nk, ah = len(HALF_CHUNKS), na // 2
    parts = ((0, quad // 2), (quad // 2, quad - quad // 2))
    offs = [(sum(HALF_CHUNKS[:k]), HALF_CHUNKS[k]) for k in range(nk)]
    ks = lax.axis_index("ksplit")
    y = lax.axis_index("rows")
    core = ks % 2
    x = ks // 2

    def chip(dx, flip=0):
        return {"ksplit": ((x + dx) % RING) * 2 + (1 - core if flip else core)}

    sib = chip(0, 1)
    links = {
        "x+": (0, chip(1)), "x-": (1, chip(3)),
        "y+": (2, {"rows": (y + 1) % RING}), "y-": (3, {"rows": (y + 3) % RING}),
    }

    loads = [
        pltpu.make_async_copy(b_hbm, mine[0].at[pl.ds(0, nb)], loc_sem.at[0]),
        pltpu.make_async_copy(a_hbm, mine[0].at[pl.ds(nb, na)], loc_sem.at[1]),
        pltpu.make_async_copy(pairs_hbm, meta.at[0, 0], loc_sem.at[2]),
        pltpu.make_async_copy(plist_hbm, meta.at[0, 1], loc_sem.at[2]),
        pltpu.make_async_copy(cidx_hbm, cidx, loc_sem.at[3]),
    ]
    for load in loads:
        load.start()

    barrier = pltpu.get_barrier_semaphore()
    devices = [dev for _, dev in links.values()] + [chip(2), sib]
    for dev in devices:
        pl.semaphore_signal(barrier, inc=1, device_id=dev, device_id_type=MESH)
    zero = jnp.zeros(mine[0].shape[1:], mine[0].dtype)
    for ref in (*mine, *twin):
        ref[nb + na] = zero
    with jax.named_scope('barrier'):
        pl.semaphore_wait(barrier, len(devices))

    sems = {}
    load_of = {}
    link_of = [0] * len(links)

    def index(key):
        return sems.setdefault(key, len(sems))

    def send(link, key, src, dst, start, size):
        slot, dev = links[link]
        n = index(key)
        load_of[n] = load_of.get(n, 0) + size
        link_of[slot] += size
        pltpu.make_async_remote_copy(
            src_ref=mine[src].at[pl.ds(start, size)], dst_ref=mine[dst].at[pl.ds(start, size)],
            send_sem=link_sem.at[slot], recv_sem=recv_sem.at[n],
            device_id=dev, device_id_type=MESH).start()

    def take(size, sem):
        view = mine[0].at[pl.ds(0, size)]
        pltpu.make_async_copy(view, view, sem).wait()

    waited = {}

    def arrive(key, size):
        n = index(key)
        waited[n] = waited.get(n, 0) + size
        with jax.named_scope('_'.join(str(t) for t in key).replace('+', 'p').replace('-', 'm').replace(' ', '')):
            take(size, recv_sem.at[n])

    def share(d, start, size):
        pltpu.make_async_remote_copy(
            src_ref=mine[d].at[pl.ds(start, size)], dst_ref=twin[d].at[pl.ds(start, size)],
            send_sem=dsend.at[d], recv_sem=drecv.at[d], device_id=sib, device_id_type=MESH).start()

    own = (y % 2) * (2 * half)
    theirs = (1 - y % 2) * (2 * half)

    def quad_at(dy):
        return 4 * half + ((y + dy) % RING) * quad

    def lay(k, base):
        off, size = offs[k]
        return base + off, base + half + off, size

    q0, qm, qp, qf = quad_at(0), quad_at(3), quad_at(1), quad_at(2)

    loads[0].wait()
    def pieces(first, second):
        (off, size), rest = parts[first], parts[second]
        return ((off, 1, "f"), (off + 1, size - 1, "f"), (*rest, ""))

    w_pieces = list(zip(pieces(0, 1), pieces(1, 0)))
    for n, pair in enumerate(w_pieces):
        for link, d, (off, size, _) in zip(("x+", "x-"), (LEFT, RIGHT), pair):
            send(link, ("xw", n), 0, d, q0 + off, size)
    pltpu.make_async_copy(meta.at[0], meta.at[0], loc_sem.at[2]).wait()

    def list_to(slot, src, dev, sem):
        pltpu.make_async_remote_copy(
            src_ref=meta.at[src], dst_ref=meta.at[slot], send_sem=msem.at[0], recv_sem=msem.at[sem],
            device_id=dev, device_id_type=MESH).start()

    def lists_taken(count, sem):
        view = meta.at[pl.ds(0, count)]
        pltpu.make_async_copy(view, view, msem.at[sem]).wait()

    for dx in range(1, RING):
        list_to(2 * (RING - dx), 0, chip(dx), 1)
    list_to(1, 0, sib, 2)
    for k in range(nk):
        u, v, size = lay(k, own)
        send("x+", ("x", k, 0), 0, LEFT, u, size)
        send("x-", ("x", k, 0), 0, RIGHT, v, size)
        send("x+", ("x", k, 1), 0, LEFT, v, size)
        send("x-", ("x", k, 1), 0, RIGHT, u, size)
    loads[1].wait()

    def build_table():
      with jax.named_scope('table'):
            loads[4].wait()
            lists_taken(RING, 2)
            npart = meta.shape[3]
            ckey = cidx[0:1, :] * 4096 + cidx[1:2, :]
            eye = lax.broadcasted_iota(jnp.int32, (nc, nc), 0) == lax.broadcasted_iota(jnp.int32, (nc, nc), 1)
            ccol = jnp.sum(jnp.where(eye, jnp.broadcast_to(ckey, (nc, nc)), 0), axis=1, keepdims=True)
            lane = lax.broadcasted_iota(jnp.int32, (nc, 128), 1)
            table = jnp.zeros((nc, 128), jnp.int32)
            for slot in range(2 * RING):
                pkey = meta[slot, 1, 0:1, :] * 4096 + meta[slot, 1, 1:2, :]
                pval = meta[slot, 0, 0:1, :] * 4096 + meta[slot, 0, 1:2, :] - na * 4096
                hit = jnp.broadcast_to(ccol, (nc, npart)) == jnp.broadcast_to(pkey, (nc, npart))
                found = jnp.sum(jnp.where(hit, jnp.broadcast_to(pval, (nc, npart)), 0), axis=1, keepdims=True) + na * 4096
                a_at = nb + jnp.clip(lax.shift_right_arithmetic(found, 12), 0, na)
                b_at = jnp.clip(found & 4095, 0, nb - 1)
                table = jnp.where(lane == 2 * slot, a_at, table)
                table = jnp.where(lane == 2 * slot + 1, b_at, table)
                if slot == 2 * FAR + 1:
                    for n, column in enumerate((a_at, b_at)):
                        row = jnp.sum(jnp.where(eye, jnp.broadcast_to(column, (nc, nc)), 0), axis=0, keepdims=True)
                        far_tab[n:n + 1, 0:nc] = row
            tab_v[...] = table
            pltpu.make_async_copy(tab_v, tab_s, loc_sem.at[3]).start()

    def stage(d, sides=(0, 1), lo=0, hi=nc, group=24, first=False):
        def product(side, c):
            ref, n = (twin if side else mine)[d], 4 * d + 2 * side
            p = jnp.dot(ref[tab_s[c, n]], ref[tab_s[c, n + 1]], preferred_element_type=jnp.float32)
            return p.astype(jnp.bfloat16).astype(jnp.float32)

        def body(step, carry):
            for sub in range(group):
                c = step * group + sub
                total = product(sides[0], c)
                for side in sides[1:]:
                    total = total + product(side, c)
                acc[c] = total if first else acc[c] + total
            return carry

        with jax.named_scope(f'stage{d}_{len(sides)}{sides[0]}_{lo}'):
            lax.fori_loop(lo // group, hi // group, body, 0)

    def ready(d):
        take_twin = twin[d].at[pl.ds(0, nb + na)]
        with jax.named_scope(f'ready{d}'):
            pltpu.make_async_copy(take_twin, take_twin, drecv.at[d]).wait()

    def y_taken(cols, k):
        u, v, size = lay(k, theirs)
        arrive(("y", cols, k), 2 * size * len(cols))
        for d in cols:
            share(d, u, size)
            share(d, v, size)

    near = (LEFT, RIGHT)
    third = nc // 3

    for n, pair in enumerate(w_pieces):
        arrive(("xw", n), sum(size for _, size, _ in pair))
        for link, d, (off, size, goes_on) in zip(("x+", "x-"), (LEFT, RIGHT), pair):
            send("y+", ("yw", near), d, d, q0 + off, size)
            send("y-", ("yw", near), d, d, q0 + off, size)
            if goes_on:
                send(link, ("f", "w"), d, FAR, q0 + off, size)
            share(d, q0 + off, size)
    share(0, 0, nb + na)

    def spread(k):
        (up, up_size), (down, down_size) = parts if k == 0 else parts[::-1]
        for d in (near if k == 0 else (FAR,)):
            send("y+", ("g", k), d, d, qm + up, up_size)
            send("y-", ("g", k), d, d, qp + down, down_size)
            share(d, qm, quad)
            share(d, qp, quad)

    for k in range(nk):
        u, v, size = lay(k, own)
        if k == nk - 1:
            for part in range(2):
                send("x+", ("a", part), 0, LEFT, nb + part * ah, ah)
                send("x-", ("a", part), 0, RIGHT, nb + (1 - part) * ah, ah)
        arrive(("x", k, 0), 2 * size)
        send("y+", ("y", near, k), LEFT, LEFT, u, size)
        send("x+", ("f", k), LEFT, FAR, u, size)
        send("y-", ("y", near, k), RIGHT, RIGHT, v, size)
        send("x-", ("f", k), RIGHT, FAR, v, size)
        share(LEFT, u, size)
        share(RIGHT, v, size)
        if k == 0:
            lists_taken(RING - 1, 1)
            for d in range(1, RING):
                list_to(2 * d + 1, 2 * d, sib, 2)
        elif k == 1:
            arrive(("yw", near), 4 * quad)
            spread(0)
        elif k == 2:
            stage(0, lo=third, hi=2 * third, first=True)
            y_taken(near, 0)
        elif k == 3:
            y_taken(near, 1)
        arrive(("x", k, 1), 2 * size)
        send("y-", ("y", near, k), LEFT, LEFT, v, size)
        send("y+", ("y", near, k), RIGHT, RIGHT, u, size)
        share(LEFT, v, size)
        share(RIGHT, u, size)
        if k == 0:
            build_table()
        elif k == 1:
            pltpu.make_async_copy(tab_v, tab_s, loc_sem.at[3]).wait()
            ready(0)
            stage(0, hi=third, first=True)
        elif k == 2:
            stage(0, lo=2 * third, first=True)
    arrive(("g", 0), 2 * quad)
    for d in near:
        share(d, qf, quad)

    def far_block(k):
        u, v, size = lay(k, own)
        arrive(("f", k), 2 * size)
        send("y+", ("y", (FAR,), k), FAR, FAR, u, size)
        send("y-", ("y", (FAR,), k), FAR, FAR, v, size)
        share(FAR, u, size)
        share(FAR, v, size)

    arrive(("f", "w"), quad)
    send("y+", ("yw", FAR), FAR, FAR, q0, quad)
    send("y-", ("yw", FAR), FAR, FAR, q0, quad)
    share(FAR, q0, quad)
    y_taken(near, 2)
    far_block(0)
    far_block(1)
    y_taken(near, 3)
    far_block(2)
    y_taken(near, 4)
    far_block(3)
    arrive(("yw", FAR), 2 * quad)
    spread(1)
    y_taken((FAR,), 0)

    arrive(("a", 0), 2 * ah)
    send("x+", ("f", "a"), LEFT, FAR, nb, ah)
    send("x-", ("f", "a"), RIGHT, FAR, nb + ah, ah)
    share(LEFT, nb, ah)
    share(RIGHT, nb + ah, ah)
    arrive(("a", 1), 2 * ah)
    share(LEFT, nb + ah, ah)
    share(RIGHT, nb, ah)
    stage(LEFT, (0,))
    far_block(4)
    y_taken((FAR,), 1)
    ready(LEFT)
    stage(LEFT, (1,))
    y_taken((FAR,), 2)
    arrive(("g", 1), quad)
    share(FAR, qf, quad)
    ready(RIGHT)
    stage(RIGHT)
    y_taken((FAR,), 3)
    arrive(("f", "a"), 2 * ah)
    share(FAR, nb, na)
    y_taken((FAR,), 4)
    stage(FAR, (0,), group=nc // 2)
    ready(FAR)
    stage(FAR, (1,), hi=head)

    assert load_of == waited and len(sems) == recv_sem.shape[0], len(sems)
    with jax.named_scope('sendwaits'):
        for slot, size in enumerate(link_of):
            take(size, link_sem.at[slot])
        own_meta = meta.at[pl.ds(0, 2 * RING - 1)]
        pltpu.make_async_copy(own_meta, own_meta, msem.at[0]).wait()
        for d in range(RING):
            take(nb + na, dsend.at[d])


def finish(head, cuts, acc, far, tab, out_hbm, buf, tab_s, tab_sem, out_sem):
    table = pltpu.make_async_copy(tab, tab_s, tab_sem)
    table.start()
    first = pl.ds(0, head)
    outs, lo = [pltpu.make_async_copy(acc.at[first], out_hbm.at[first], out_sem.at[len(cuts)])], head
    outs[0].start()
    table.wait()
    for n, hi in enumerate(cuts):
        for c in range(lo, hi):
            p = jnp.dot(far[tab_s[0, c]], far[tab_s[1, c]], preferred_element_type=jnp.float32)
            buf[c] = acc[c] + p.astype(jnp.bfloat16).astype(jnp.float32)
        view = pl.ds(lo, hi - lo)
        outs.append(pltpu.make_async_copy(buf.at[view], out_hbm.at[view], out_sem.at[n]))
        outs[-1].start()
        lo = hi
    for copy in outs:
        copy.wait()


def solution(mesh):
    row_spec = P(('batch', 'rows'), 'ksplit')
    col_spec = P(('batch', 'ksplit'))
    assert mesh.shape['rows'] == RING and mesh.shape['ksplit'] == 2 * RING

    def device_step(a_loc, b_loc, pair_loc, plist_loc, cidx_loc):
        a, b = a_loc[0, 0], b_loc[0]
        pairs = pair_loc[0, 0, :, 0, :].T
        plist = plist_loc[0, 0].T
        cidx = cidx_loc[0, 0].T
        na, nb, nc, size = a.shape[0], b.shape[0], cidx.shape[1], a.shape[-1]
        npart = plist.shape[1]
        nsem = 11 + 5 * len(HALF_CHUNKS)
        block = (size, size)
        args = [pltpu.with_memory_space_constraint(t, pltpu.HBM) for t in (a, b, pairs, plist, cidx)]
        head = nc // 3
        acc, far, tab = pl.pallas_call(
            functools.partial(kernel, na, nb, nc, head),
            out_shape=(
                jax.ShapeDtypeStruct((nc, *block), jnp.float32),
                jax.ShapeDtypeStruct((nb + na + 1, *block), b.dtype),
                jax.ShapeDtypeStruct((2, 128), jnp.int32),
            ),
            in_specs=[pl.BlockSpec(memory_space=pltpu.HBM)] * 5,
            out_specs=(pl.BlockSpec(memory_space=pltpu.VMEM),) * 3,
            scratch_shapes=[
                *[pltpu.VMEM((nb + na + 1, *block), b.dtype) for _ in range(2 * RING - 1)],
                pltpu.VMEM((2 * RING, 2, 2, npart), jnp.int32),
                pltpu.VMEM((2, nc), jnp.int32),
                pltpu.VMEM((nc, 128), jnp.int32),
                pltpu.SMEM((nc, 128), jnp.int32),
                pltpu.SemaphoreType.DMA((4,)),
                pltpu.SemaphoreType.DMA((4,)),
                pltpu.SemaphoreType.DMA((nsem,)),
                pltpu.SemaphoreType.DMA((RING,)),
                pltpu.SemaphoreType.DMA((RING,)),
                pltpu.SemaphoreType.DMA((3,)),
            ],
            compiler_params=pltpu.CompilerParams(
                collective_id=0, has_side_effects=True, vmem_limit_bytes=30 * 2**20),
        )(*args)
        cuts = tuple(head + (nc - head) * n // 6 for n in (2, 4, 5, 6))
        vmem = pl.BlockSpec(memory_space=pltpu.VMEM)
        out = pl.pallas_call(
            functools.partial(finish, head, cuts),
            out_shape=jax.ShapeDtypeStruct((nc, *block), jnp.float32),
            in_specs=[vmem] * 3,
            out_specs=pl.BlockSpec(memory_space=pltpu.HBM),
            scratch_shapes=[
                pltpu.VMEM((nc, *block), jnp.float32),
                pltpu.SMEM((2, 128), jnp.int32),
                pltpu.SemaphoreType.DMA,
                pltpu.SemaphoreType.DMA((len(cuts) + 1,)),
            ],
            compiler_params=pltpu.CompilerParams(vmem_limit_bytes=8 * 2**20),
        )(acc, far, tab)
        return out[None, None]

    return jax.shard_map(device_step, mesh=mesh, in_specs=(row_spec, col_spec, row_spec, row_spec, row_spec), out_specs=row_spec, check_vma=False)
```

```python
import functools

import jax
import jax.numpy as jnp
from jax import lax
from jax.experimental import pallas as pl
from jax.experimental.pallas import tpu as pltpu
from jax.sharding import PartitionSpec as P


MESH = pl.DeviceIdType.MESH
RING = 4
HALF_CHUNKS = (3, 3, 3, 2, 2)
LEFT, RIGHT, FAR = 3, 1, 2


def plan(nb):
    half = sum(HALF_CHUNKS)
    quad = (nb - 4 * half) // RING
    assert 4 * half + RING * quad == nb
    return half, quad


def kernel(na, nb, nc, head, a_hbm, b_hbm, pairs_hbm, plist_hbm, cidx_hbm, acc, far_twin, far_tab, *scratch):
    mine, twin = scratch[0:RING], list(scratch[RING:2 * RING - 1])
    twin.insert(FAR, far_twin)
    (meta, cidx, tab_v, tab_s, loc_sem, link_sem, recv_sem, dsend, drecv, msem) = scratch[2 * RING - 1:]
    half, quad = plan(nb)
    nk, ah = len(HALF_CHUNKS), na // 2
    parts = ((0, quad // 2), (quad // 2, quad - quad // 2))
    offs = [(sum(HALF_CHUNKS[:k]), HALF_CHUNKS[k]) for k in range(nk)]
    ks = lax.axis_index("ksplit")
    y = lax.axis_index("rows")
    core = ks % 2
    x = ks // 2

    def chip(dx, flip=0):
        return {"ksplit": ((x + dx) % RING) * 2 + (1 - core if flip else core)}

    sib = chip(0, 1)
    links = {
        "x+": (0, chip(1)), "x-": (1, chip(3)),
        "y+": (2, {"rows": (y + 1) % RING}), "y-": (3, {"rows": (y + 3) % RING}),
    }

    loads = [
        pltpu.make_async_copy(b_hbm, mine[0].at[pl.ds(0, nb)], loc_sem.at[0]),
        pltpu.make_async_copy(a_hbm, mine[0].at[pl.ds(nb, na)], loc_sem.at[1]),
        pltpu.make_async_copy(pairs_hbm, meta.at[0, 0], loc_sem.at[2]),
        pltpu.make_async_copy(plist_hbm, meta.at[0, 1], loc_sem.at[2]),
        pltpu.make_async_copy(cidx_hbm, cidx, loc_sem.at[3]),
    ]
    for load in loads:
        load.start()

    barrier = pltpu.get_barrier_semaphore()
    devices = [dev for _, dev in links.values()] + [chip(2), sib]
    for dev in devices:
        pl.semaphore_signal(barrier, inc=1, device_id=dev, device_id_type=MESH)
    zero = jnp.zeros(mine[0].shape[1:], mine[0].dtype)
    for ref in (*mine, *twin):
        ref[nb + na] = zero
    with jax.named_scope('barrier'):
        pl.semaphore_wait(barrier, len(devices))

    sems = {}
    load_of = {}
    link_of = [0] * len(links)

    def index(key):
        return sems.setdefault(key, len(sems))

    def send(link, key, src, dst, start, size):
        slot, dev = links[link]
        n = index(key)
        load_of[n] = load_of.get(n, 0) + size
        link_of[slot] += size
        pltpu.make_async_remote_copy(
            src_ref=mine[src].at[pl.ds(start, size)], dst_ref=mine[dst].at[pl.ds(start, size)],
            send_sem=link_sem.at[slot], recv_sem=recv_sem.at[n],
            device_id=dev, device_id_type=MESH).start()

    def take(size, sem):
        view = mine[0].at[pl.ds(0, size)]
        pltpu.make_async_copy(view, view, sem).wait()

    waited = {}

    def arrive(key, size):
        n = index(key)
        waited[n] = waited.get(n, 0) + size
        with jax.named_scope('_'.join(str(t) for t in key).replace('+', 'p').replace('-', 'm').replace(' ', '')):
            take(size, recv_sem.at[n])

    def share(d, start, size):
        pltpu.make_async_remote_copy(
            src_ref=mine[d].at[pl.ds(start, size)], dst_ref=twin[d].at[pl.ds(start, size)],
            send_sem=dsend.at[d], recv_sem=drecv.at[d], device_id=sib, device_id_type=MESH).start()

    own = (y % 2) * (2 * half)
    theirs = (1 - y % 2) * (2 * half)

    def quad_at(dy):
        return 4 * half + ((y + dy) % RING) * quad

    def lay(k, base):
        off, size = offs[k]
        return base + off, base + half + off, size

    q0, qm, qp, qf = quad_at(0), quad_at(3), quad_at(1), quad_at(2)

    loads[0].wait()
    def pieces(first, second):
        (off, size), rest = parts[first], parts[second]
        return ((off, 1, "f"), (off + 1, size - 1, "f"), (*rest, ""))

    w_pieces = list(zip(pieces(0, 1), pieces(1, 0)))
    for n, pair in enumerate(w_pieces):
        for link, d, (off, size, _) in zip(("x+", "x-"), (LEFT, RIGHT), pair):
            send(link, ("xw", n), 0, d, q0 + off, size)
    pltpu.make_async_copy(meta.at[0], meta.at[0], loc_sem.at[2]).wait()

    def list_to(slot, src, dev, sem):
        pltpu.make_async_remote_copy(
            src_ref=meta.at[src], dst_ref=meta.at[slot], send_sem=msem.at[0], recv_sem=msem.at[sem],
            device_id=dev, device_id_type=MESH).start()

    def lists_taken(count, sem):
        view = meta.at[pl.ds(0, count)]
        pltpu.make_async_copy(view, view, msem.at[sem]).wait()

    for dx in range(1, RING):
        list_to(2 * (RING - dx), 0, chip(dx), 1)
    list_to(1, 0, sib, 2)
    for k in range(nk):
        u, v, size = lay(k, own)
        send("x+", ("x", k, 0), 0, LEFT, u, size)
        send("x-", ("x", k, 0), 0, RIGHT, v, size)
        send("x+", ("x", k, 1), 0, LEFT, v, size)
        send("x-", ("x", k, 1), 0, RIGHT, u, size)
    loads[1].wait()

    def build_table():
      with jax.named_scope('table'):
            loads[4].wait()
            lists_taken(RING, 2)
            npart = meta.shape[3]
            ckey = cidx[0:1, :] * 4096 + cidx[1:2, :]
            eye = lax.broadcasted_iota(jnp.int32, (nc, nc), 0) == lax.broadcasted_iota(jnp.int32, (nc, nc), 1)
            ccol = jnp.sum(jnp.where(eye, jnp.broadcast_to(ckey, (nc, nc)), 0), axis=1, keepdims=True)
            lane = lax.broadcasted_iota(jnp.int32, (nc, 128), 1)
            table = jnp.zeros((nc, 128), jnp.int32)
            for slot in range(2 * RING):
                pkey = meta[slot, 1, 0:1, :] * 4096 + meta[slot, 1, 1:2, :]
                pval = meta[slot, 0, 0:1, :] * 4096 + meta[slot, 0, 1:2, :] - na * 4096
                hit = jnp.broadcast_to(ccol, (nc, npart)) == jnp.broadcast_to(pkey, (nc, npart))
                found = jnp.sum(jnp.where(hit, jnp.broadcast_to(pval, (nc, npart)), 0), axis=1, keepdims=True) + na * 4096
                a_at = nb + jnp.clip(lax.shift_right_arithmetic(found, 12), 0, na)
                b_at = jnp.clip(found & 4095, 0, nb - 1)
                table = jnp.where(lane == 2 * slot, a_at, table)
                table = jnp.where(lane == 2 * slot + 1, b_at, table)
                if slot == 2 * FAR + 1:
                    for n, column in enumerate((a_at, b_at)):
                        row = jnp.sum(jnp.where(eye, jnp.broadcast_to(column, (nc, nc)), 0), axis=0, keepdims=True)
                        far_tab[n:n + 1, 0:nc] = row
            tab_v[...] = table
            pltpu.make_async_copy(tab_v, tab_s, loc_sem.at[3]).start()

    def stage(d, sides=(0, 1), lo=0, hi=nc, group=24, first=False):
        def product(side, c):
            ref, n = (twin if side else mine)[d], 4 * d + 2 * side
            p = jnp.dot(ref[tab_s[c, n]], ref[tab_s[c, n + 1]], preferred_element_type=jnp.float32)
            return p.astype(jnp.bfloat16).astype(jnp.float32)

        def body(step, carry):
            for sub in range(group):
                c = step * group + sub
                total = product(sides[0], c)
                for side in sides[1:]:
                    total = total + product(side, c)
                acc[c] = total if first else acc[c] + total
            return carry

        with jax.named_scope(f'stage{d}_{len(sides)}{sides[0]}_{lo}'):
            lax.fori_loop(lo // group, hi // group, body, 0)

    def ready(d):
        take_twin = twin[d].at[pl.ds(0, nb + na)]
        with jax.named_scope(f'ready{d}'):
            pltpu.make_async_copy(take_twin, take_twin, drecv.at[d]).wait()

    def y_taken(cols, k):
        u, v, size = lay(k, theirs)
        arrive(("y", cols, k), 2 * size * len(cols))
        for d in cols:
            share(d, u, size)
            share(d, v, size)

    near = (LEFT, RIGHT)
    third = nc // 3

    for n, pair in enumerate(w_pieces):
        arrive(("xw", n), sum(size for _, size, _ in pair))
        for link, d, (off, size, goes_on) in zip(("x+", "x-"), (LEFT, RIGHT), pair):
            send("y+", ("yw", near), d, d, q0 + off, size)
            send("y-", ("yw", near), d, d, q0 + off, size)
            if goes_on:
                send(link, ("f", "w"), d, FAR, q0 + off, size)
            share(d, q0 + off, size)
    share(0, 0, nb + na)

    def spread(k):
        (up, up_size), (down, down_size) = parts if k == 0 else parts[::-1]
        for d in (near if k == 0 else (FAR,)):
            send("y+", ("g", k), d, d, qm + up, up_size)
            send("y-", ("g", k), d, d, qp + down, down_size)
            share(d, qm, quad)
            share(d, qp, quad)

    for k in range(nk):
        u, v, size = lay(k, own)
        if k == nk - 1:
            for part in range(2):
                send("x+", ("a", part), 0, LEFT, nb + part * ah, ah)
                send("x-", ("a", part), 0, RIGHT, nb + (1 - part) * ah, ah)
        arrive(("x", k, 0), 2 * size)
        send("y+", ("y", near, k), LEFT, LEFT, u, size)
        send("x+", ("f", k), LEFT, FAR, u, size)
        send("y-", ("y", near, k), RIGHT, RIGHT, v, size)
        send("x-", ("f", k), RIGHT, FAR, v, size)
        share(LEFT, u, size)
        share(RIGHT, v, size)
        if k == 0:
            lists_taken(RING - 1, 1)
            for d in range(1, RING):
                list_to(2 * d + 1, 2 * d, sib, 2)
        elif k == 1:
            arrive(("yw", near), 4 * quad)
            spread(0)
        elif k == 2:
            stage(0, lo=third, hi=2 * third, first=True)
            y_taken(near, 0)
        elif k == 3:
            y_taken(near, 1)
        arrive(("x", k, 1), 2 * size)
        send("y-", ("y", near, k), LEFT, LEFT, v, size)
        send("y+", ("y", near, k), RIGHT, RIGHT, u, size)
        share(LEFT, v, size)
        share(RIGHT, u, size)
        if k == 0:
            build_table()
        elif k == 1:
            pltpu.make_async_copy(tab_v, tab_s, loc_sem.at[3]).wait()
            ready(0)
            stage(0, hi=third, first=True)
        elif k == 2:
            stage(0, lo=2 * third, first=True)
    arrive(("g", 0), 2 * quad)
    for d in near:
        share(d, qf, quad)

    def far_block(k):
        u, v, size = lay(k, own)
        arrive(("f", k), 2 * size)
        send("y+", ("y", (FAR,), k), FAR, FAR, u, size)
        send("y-", ("y", (FAR,), k), FAR, FAR, v, size)
        share(FAR, u, size)
        share(FAR, v, size)

    arrive(("f", "w"), quad)
    send("y+", ("yw", FAR), FAR, FAR, q0, quad)
    send("y-", ("yw", FAR), FAR, FAR, q0, quad)
    share(FAR, q0, quad)
    y_taken(near, 2)
    far_block(0)
    far_block(1)
    y_taken(near, 3)
    far_block(2)
    y_taken(near, 4)
    far_block(3)
    arrive(("yw", FAR), 2 * quad)
    spread(1)
    y_taken((FAR,), 0)

    arrive(("a", 0), 2 * ah)
    send("x+", ("f", "a"), LEFT, FAR, nb, ah)
    send("x-", ("f", "a"), RIGHT, FAR, nb + ah, ah)
    share(LEFT, nb, ah)
    share(RIGHT, nb + ah, ah)
    arrive(("a", 1), 2 * ah)
    share(LEFT, nb + ah, ah)
    share(RIGHT, nb, ah)
    stage(LEFT, (0,))
    far_block(4)
    y_taken((FAR,), 1)
    ready(LEFT)
    stage(LEFT, (1,))
    y_taken((FAR,), 2)
    ready(RIGHT)
    stage(RIGHT)
    arrive(("g", 1), quad)
    share(FAR, qf, quad)
    y_taken((FAR,), 3)
    arrive(("f", "a"), 2 * ah)
    share(FAR, nb, na)
    y_taken((FAR,), 4)
    stage(FAR, (0,), group=nc // 2)
    ready(FAR)
    stage(FAR, (1,), hi=head)

    assert load_of == waited and len(sems) == recv_sem.shape[0], len(sems)
    with jax.named_scope('sendwaits'):
        for slot, size in enumerate(link_of):
            take(size, link_sem.at[slot])
        own_meta = meta.at[pl.ds(0, 2 * RING - 1)]
        pltpu.make_async_copy(own_meta, own_meta, msem.at[0]).wait()
        for d in range(RING):
            take(nb + na, dsend.at[d])


def finish(head, cuts, acc, far, tab, out_hbm, buf, tab_s, tab_sem, out_sem):
    table = pltpu.make_async_copy(tab, tab_s, tab_sem)
    table.start()
    first = pl.ds(0, head)
    outs, lo = [pltpu.make_async_copy(acc.at[first], out_hbm.at[first], out_sem.at[len(cuts)])], head
    outs[0].start()
    table.wait()
    for n, hi in enumerate(cuts):
        for c in range(lo, hi):
            p = jnp.dot(far[tab_s[0, c]], far[tab_s[1, c]], preferred_element_type=jnp.float32)
            buf[c] = acc[c] + p.astype(jnp.bfloat16).astype(jnp.float32)
        view = pl.ds(lo, hi - lo)
        outs.append(pltpu.make_async_copy(buf.at[view], out_hbm.at[view], out_sem.at[n]))
        outs[-1].start()
        lo = hi
    for copy in outs:
        copy.wait()


def solution(mesh):
    row_spec = P(('batch', 'rows'), 'ksplit')
    col_spec = P(('batch', 'ksplit'))
    assert mesh.shape['rows'] == RING and mesh.shape['ksplit'] == 2 * RING

    def device_step(a_loc, b_loc, pair_loc, plist_loc, cidx_loc):
        a, b = a_loc[0, 0], b_loc[0]
        pairs = pair_loc[0, 0, :, 0, :].T
        plist = plist_loc[0, 0].T
        cidx = cidx_loc[0, 0].T
        na, nb, nc, size = a.shape[0], b.shape[0], cidx.shape[1], a.shape[-1]
        npart = plist.shape[1]
        nsem = 11 + 5 * len(HALF_CHUNKS)
        block = (size, size)
        args = [pltpu.with_memory_space_constraint(t, pltpu.HBM) for t in (a, b, pairs, plist, cidx)]
        head = nc // 3
        acc, far, tab = pl.pallas_call(
            functools.partial(kernel, na, nb, nc, head),
            out_shape=(
                jax.ShapeDtypeStruct((nc, *block), jnp.float32),
                jax.ShapeDtypeStruct((nb + na + 1, *block), b.dtype),
                jax.ShapeDtypeStruct((2, 128), jnp.int32),
            ),
            in_specs=[pl.BlockSpec(memory_space=pltpu.HBM)] * 5,
            out_specs=(pl.BlockSpec(memory_space=pltpu.VMEM),) * 3,
            scratch_shapes=[
                *[pltpu.VMEM((nb + na + 1, *block), b.dtype) for _ in range(2 * RING - 1)],
                pltpu.VMEM((2 * RING, 2, 2, npart), jnp.int32),
                pltpu.VMEM((2, nc), jnp.int32),
                pltpu.VMEM((nc, 128), jnp.int32),
                pltpu.SMEM((nc, 128), jnp.int32),
                pltpu.SemaphoreType.DMA((4,)),
                pltpu.SemaphoreType.DMA((4,)),
                pltpu.SemaphoreType.DMA((nsem,)),
                pltpu.SemaphoreType.DMA((RING,)),
                pltpu.SemaphoreType.DMA((RING,)),
                pltpu.SemaphoreType.DMA((3,)),
            ],
            compiler_params=pltpu.CompilerParams(
                collective_id=0, has_side_effects=True, vmem_limit_bytes=30 * 2**20),
        )(*args)
        cuts = tuple(head + (nc - head) * n // 6 for n in (2, 4, 5, 6))
        vmem = pl.BlockSpec(memory_space=pltpu.VMEM)
        out = pl.pallas_call(
            functools.partial(finish, head, cuts),
            out_shape=jax.ShapeDtypeStruct((nc, *block), jnp.float32),
            in_specs=[vmem] * 3,
            out_specs=pl.BlockSpec(memory_space=pltpu.HBM),
            scratch_shapes=[
                pltpu.VMEM((nc, *block), jnp.float32),
                pltpu.SMEM((2, 128), jnp.int32),
                pltpu.SemaphoreType.DMA,
                pltpu.SemaphoreType.DMA((len(cuts) + 1,)),
            ],
            compiler_params=pltpu.CompilerParams(vmem_limit_bytes=8 * 2**20),
        )(acc, far, tab)
        return out[None, None]

    return jax.shard_map(device_step, mesh=mesh, in_specs=(row_spec, col_spec, row_spec, row_spec, row_spec), out_specs=row_spec, check_vma=False)
```

```python
import functools

import jax
import jax.numpy as jnp
from jax import lax
from jax.experimental import pallas as pl
from jax.experimental.pallas import tpu as pltpu
from jax.sharding import PartitionSpec as P

MESH = pl.DeviceIdType.MESH
RING = 4
HALF_CHUNKS = (3, 3, 3, 2, 2)
LEFT, RIGHT, FAR = 3, 1, 2


def plan(nb):
    half = sum(HALF_CHUNKS)
    quad = (nb - 4 * half) // RING
    assert 4 * half + RING * quad == nb
    return half, quad


def kernel(na, nb, nc, head, a_hbm, b_hbm, pairs_hbm, plist_hbm, cidx_hbm, acc, far_twin, far_tab, *scratch):
    mine, twin = scratch[0:RING], list(scratch[RING:2 * RING - 1])
    twin.insert(FAR, far_twin)
    (meta, cidx, tab_v, tab_s, loc_sem, link_sem, recv_sem, dsend, drecv, msem) = scratch[2 * RING - 1:]
    half, quad = plan(nb)
    nk, ah = len(HALF_CHUNKS), na // 2
    parts = ((0, quad // 2), (quad // 2, quad - quad // 2))
    offs = [(sum(HALF_CHUNKS[:k]), HALF_CHUNKS[k]) for k in range(nk)]
    ks = lax.axis_index("ksplit")
    y = lax.axis_index("rows")
    core = ks % 2
    x = ks // 2

    def chip(dx, flip=0):
        return {"ksplit": ((x + dx) % RING) * 2 + (1 - core if flip else core)}

    sib = chip(0, 1)
    links = {
        "x+": (0, chip(1)), "x-": (1, chip(3)),
        "y+": (2, {"rows": (y + 1) % RING}), "y-": (3, {"rows": (y + 3) % RING}),
    }

    loads = [
        pltpu.make_async_copy(b_hbm, mine[0].at[pl.ds(0, nb)], loc_sem.at[0]),
        pltpu.make_async_copy(a_hbm, mine[0].at[pl.ds(nb, na)], loc_sem.at[1]),
        pltpu.make_async_copy(pairs_hbm, meta.at[0, 0], loc_sem.at[2]),
        pltpu.make_async_copy(plist_hbm, meta.at[0, 1], loc_sem.at[2]),
        pltpu.make_async_copy(cidx_hbm, cidx, loc_sem.at[3]),
    ]
    for load in loads:
        load.start()

    barrier = pltpu.get_barrier_semaphore()
    devices = [dev for _, dev in links.values()] + [chip(2), sib]
    for dev in devices:
        pl.semaphore_signal(barrier, inc=1, device_id=dev, device_id_type=MESH)
    zero = jnp.zeros(mine[0].shape[1:], mine[0].dtype)
    for ref in (*mine, *twin):
        ref[nb + na] = zero
    with jax.named_scope('barrier'):
        pl.semaphore_wait(barrier, len(devices))

    sems = {}
    load_of = {}
    link_of = [0] * len(links)

    def index(key):
        return sems.setdefault(key, len(sems))

    def send(link, key, src, dst, start, size):
        slot, dev = links[link]
        n = index(key)
        load_of[n] = load_of.get(n, 0) + size
        link_of[slot] += size
        pltpu.make_async_remote_copy(
            src_ref=mine[src].at[pl.ds(start, size)], dst_ref=mine[dst].at[pl.ds(start, size)],
            send_sem=link_sem.at[slot], recv_sem=recv_sem.at[n],
            device_id=dev, device_id_type=MESH).start()

    def take(size, sem):
        view = mine[0].at[pl.ds(0, size)]
        pltpu.make_async_copy(view, view, sem).wait()

    waited = {}

    def arrive(key, size):
        n = index(key)
        waited[n] = waited.get(n, 0) + size
        with jax.named_scope('_'.join(str(t) for t in key).replace('+', 'p').replace('-', 'm').replace(' ', '')):
            take(size, recv_sem.at[n])

    def share(d, start, size):
        pltpu.make_async_remote_copy(
            src_ref=mine[d].at[pl.ds(start, size)], dst_ref=twin[d].at[pl.ds(start, size)],
            send_sem=dsend.at[d], recv_sem=drecv.at[d], device_id=sib, device_id_type=MESH).start()

    own = (y % 2) * (2 * half)
    theirs = (1 - y % 2) * (2 * half)

    def quad_at(dy):
        return 4 * half + ((y + dy) % RING) * quad

    def lay(k, base):
        off, size = offs[k]
        return base + off, base + half + off, size

    q0, qm, qp, qf = quad_at(0), quad_at(3), quad_at(1), quad_at(2)

    loads[0].wait()
    def pieces(first, second):
        (off, size), rest = parts[first], parts[second]
        return ((off, 1, "f"), (off + 1, size - 1, "f"), (*rest, ""))

    w_pieces = list(zip(pieces(0, 1), pieces(1, 0)))
    for n, pair in enumerate(w_pieces):
        for link, d, (off, size, _) in zip(("x+", "x-"), (LEFT, RIGHT), pair):
            send(link, ("xw", n), 0, d, q0 + off, size)
    pltpu.make_async_copy(meta.at[0], meta.at[0], loc_sem.at[2]).wait()

    def list_to(slot, src, dev, sem):
        pltpu.make_async_remote_copy(
            src_ref=meta.at[src], dst_ref=meta.at[slot], send_sem=msem.at[0], recv_sem=msem.at[sem],
            device_id=dev, device_id_type=MESH).start()

    def lists_taken(count, sem):
        view = meta.at[pl.ds(0, count)]
        pltpu.make_async_copy(view, view, msem.at[sem]).wait()

    for dx in range(1, RING):
        list_to(2 * (RING - dx), 0, chip(dx), 1)
    list_to(1, 0, sib, 2)
    for k in range(nk):
        u, v, size = lay(k, own)
        send("x+", ("x", k, 0), 0, LEFT, u, size)
        send("x-", ("x", k, 0), 0, RIGHT, v, size)
        send("x+", ("x", k, 1), 0, LEFT, v, size)
        send("x-", ("x", k, 1), 0, RIGHT, u, size)
    loads[1].wait()

    def build_table():
      with jax.named_scope('table'):
            loads[4].wait()
            lists_taken(RING, 2)
            npart = meta.shape[3]
            ckey = cidx[0:1, :] * 4096 + cidx[1:2, :]
            eye = lax.broadcasted_iota(jnp.int32, (nc, nc), 0) == lax.broadcasted_iota(jnp.int32, (nc, nc), 1)
            ccol = jnp.sum(jnp.where(eye, jnp.broadcast_to(ckey, (nc, nc)), 0), axis=1, keepdims=True)
            lane = lax.broadcasted_iota(jnp.int32, (nc, 128), 1)
            table = jnp.zeros((nc, 128), jnp.int32)
            for slot in range(2 * RING):
                pkey = meta[slot, 1, 0:1, :] * 4096 + meta[slot, 1, 1:2, :]
                pval = meta[slot, 0, 0:1, :] * 4096 + meta[slot, 0, 1:2, :] - na * 4096
                hit = jnp.broadcast_to(ccol, (nc, npart)) == jnp.broadcast_to(pkey, (nc, npart))
                found = jnp.sum(jnp.where(hit, jnp.broadcast_to(pval, (nc, npart)), 0), axis=1, keepdims=True) + na * 4096
                a_at = nb + jnp.clip(lax.shift_right_arithmetic(found, 12), 0, na)
                b_at = jnp.clip(found & 4095, 0, nb - 1)
                table = jnp.where(lane == 2 * slot, a_at, table)
                table = jnp.where(lane == 2 * slot + 1, b_at, table)
                if slot == 2 * FAR + 1:
                    for n, column in enumerate((a_at, b_at)):
                        row = jnp.sum(jnp.where(eye, jnp.broadcast_to(column, (nc, nc)), 0), axis=0, keepdims=True)
                        far_tab[n:n + 1, 0:nc] = row
            tab_v[...] = table
            pltpu.make_async_copy(tab_v, tab_s, loc_sem.at[3]).start()

    def stage(d, sides=(0, 1), lo=0, hi=nc, group=24, first=False):
        def product(side, c):
            ref, n = (twin if side else mine)[d], 4 * d + 2 * side
            p = jnp.dot(ref[tab_s[c, n]], ref[tab_s[c, n + 1]], preferred_element_type=jnp.float32)
            return p.astype(jnp.bfloat16).astype(jnp.float32)

        def body(step, carry):
            for sub in range(group):
                c = step * group + sub
                total = product(sides[0], c)
                for side in sides[1:]:
                    total = total + product(side, c)
                acc[c] = total if first else acc[c] + total
            return carry

        with jax.named_scope(f'stage{d}_{len(sides)}{sides[0]}_{lo}'):
            lax.fori_loop(lo // group, hi // group, body, 0)

    def ready(d):
        take_twin = twin[d].at[pl.ds(0, nb + na)]
        with jax.named_scope(f'ready{d}'):
            pltpu.make_async_copy(take_twin, take_twin, drecv.at[d]).wait()

    def y_taken(cols, k):
        u, v, size = lay(k, theirs)
        arrive(("y", cols, k), 2 * size * len(cols))
        for d in cols:
            share(d, u, size)
            share(d, v, size)

    near = (LEFT, RIGHT)
    third = nc // 3

    for n, pair in enumerate(w_pieces):
        arrive(("xw", n), sum(size for _, size, _ in pair))
        for link, d, (off, size, goes_on) in zip(("x+", "x-"), (LEFT, RIGHT), pair):
            send("y+", ("yw", near), d, d, q0 + off, size)
            send("y-", ("yw", near), d, d, q0 + off, size)
            if goes_on:
                send(link, ("f", "w"), d, FAR, q0 + off, size)
            share(d, q0 + off, size)
    share(0, 0, nb + na)

    def spread(k):
        (up, up_size), (down, down_size) = parts if k == 0 else parts[::-1]
        for d in (near if k == 0 else (FAR,)):
            send("y+", ("g", k), d, d, qm + up, up_size)
            send("y-", ("g", k), d, d, qp + down, down_size)
            share(d, qm, quad)
            share(d, qp, quad)

    for k in range(nk):
        u, v, size = lay(k, own)
        if k == nk - 1:
            for part in range(2):
                send("x+", ("a", part), 0, LEFT, nb + part * ah, ah)
                send("x-", ("a", part), 0, RIGHT, nb + (1 - part) * ah, ah)
        arrive(("x", k, 0), 2 * size)
        send("y+", ("y", near, k), LEFT, LEFT, u, size)
        send("x+", ("f", k), LEFT, FAR, u, size)
        send("y-", ("y", near, k), RIGHT, RIGHT, v, size)
        send("x-", ("f", k), RIGHT, FAR, v, size)
        share(LEFT, u, size)
        share(RIGHT, v, size)
        if k == 0:
            lists_taken(RING - 1, 1)
            for d in range(1, RING):
                list_to(2 * d + 1, 2 * d, sib, 2)
        elif k == 1:
            arrive(("yw", near), 4 * quad)
            spread(0)
        elif k == 2:
            stage(0, lo=third, hi=2 * third, first=True)
            y_taken(near, 0)
        elif k == 3:
            y_taken(near, 1)
        arrive(("x", k, 1), 2 * size)
        send("y-", ("y", near, k), LEFT, LEFT, v, size)
        send("y+", ("y", near, k), RIGHT, RIGHT, u, size)
        share(LEFT, v, size)
        share(RIGHT, u, size)
        if k == 0:
            build_table()
        elif k == 1:
            pltpu.make_async_copy(tab_v, tab_s, loc_sem.at[3]).wait()
            ready(0)
            stage(0, hi=third, first=True)
        elif k == 2:
            stage(0, lo=2 * third, first=True)
    arrive(("g", 0), 2 * quad)
    for d in near:
        share(d, qf, quad)

    def far_block(k):
        u, v, size = lay(k, own)
        arrive(("f", k), 2 * size)
        send("y+", ("y", (FAR,), k), FAR, FAR, u, size)
        send("y-", ("y", (FAR,), k), FAR, FAR, v, size)
        share(FAR, u, size)
        share(FAR, v, size)

    arrive(("f", "w"), quad)
    send("y+", ("yw", FAR), FAR, FAR, q0, quad)
    send("y-", ("yw", FAR), FAR, FAR, q0, quad)
    share(FAR, q0, quad)
    y_taken(near, 2)
    far_block(0)
    far_block(1)
    y_taken(near, 3)
    far_block(2)
    y_taken(near, 4)
    far_block(3)
    arrive(("yw", FAR), 2 * quad)
    spread(1)
    y_taken((FAR,), 0)

    arrive(("a", 0), 2 * ah)
    send("x+", ("f", "a"), LEFT, FAR, nb, ah)
    send("x-", ("f", "a"), RIGHT, FAR, nb + ah, ah)
    share(LEFT, nb, ah)
    share(RIGHT, nb + ah, ah)
    arrive(("a", 1), 2 * ah)
    share(LEFT, nb + ah, ah)
    share(RIGHT, nb, ah)
    stage(LEFT, (0,))
    far_block(4)
    y_taken((FAR,), 1)
    ready(LEFT)
    stage(LEFT, (1,))
    y_taken((FAR,), 2)
    ready(RIGHT)
    stage(RIGHT)
    arrive(("g", 1), quad)
    share(FAR, qf, quad)
    y_taken((FAR,), 3)
    arrive(("f", "a"), 2 * ah)
    share(FAR, nb, na)
    y_taken((FAR,), 4)
    stage(FAR, (0,), group=nc // 2)
    ready(FAR)
    stage(FAR, (1,), hi=head)

    assert load_of == waited and len(sems) == recv_sem.shape[0], len(sems)
    with jax.named_scope('sendwaits'):
        for slot, size in enumerate(link_of):
            take(size, link_sem.at[slot])
        own_meta = meta.at[pl.ds(0, 2 * RING - 1)]
        pltpu.make_async_copy(own_meta, own_meta, msem.at[0]).wait()
        for d in range(RING):
            take(nb + na, dsend.at[d])


def finish(head, cuts, acc, far, tab, out_hbm, buf, tab_s, tab_sem, out_sem):
    table = pltpu.make_async_copy(tab, tab_s, tab_sem)
    table.start()
    outs = []

    def write(src, lo, hi):
        view, n = pl.ds(lo, hi - lo), len(outs)
        outs.append(pltpu.make_async_copy(src.at[view], out_hbm.at[view], out_sem.at[n]))
        outs[-1].start(priority=n % 2)

    step = cuts[0] - head
    for lo in range(0, head, step):
        write(acc, lo, lo + step)
    table.wait()
    lo = head
    for hi in cuts:
        for c in range(lo, hi):
            p = jnp.dot(far[tab_s[0, c]], far[tab_s[1, c]], preferred_element_type=jnp.float32)
            buf[c] = acc[c] + p.astype(jnp.bfloat16).astype(jnp.float32)
        write(buf, lo, hi)
        lo = hi
    for copy in outs:
        copy.wait()


def solution(mesh):
    row_spec = P(('batch', 'rows'), 'ksplit')
    col_spec = P(('batch', 'ksplit'))
    assert mesh.shape['rows'] == RING and mesh.shape['ksplit'] == 2 * RING

    def device_step(a_loc, b_loc, pair_loc, plist_loc, cidx_loc):
        a, b = a_loc[0, 0], b_loc[0]
        pairs = pair_loc[0, 0, :, 0, :].T
        plist = plist_loc[0, 0].T
        cidx = cidx_loc[0, 0].T
        na, nb, nc, size = a.shape[0], b.shape[0], cidx.shape[1], a.shape[-1]
        npart = plist.shape[1]
        nsem = 11 + 5 * len(HALF_CHUNKS)
        block = (size, size)
        args = [pltpu.with_memory_space_constraint(t, pltpu.HBM) for t in (a, b, pairs, plist, cidx)]
        head = nc // 3
        acc, far, tab = pl.pallas_call(
            functools.partial(kernel, na, nb, nc, head),
            out_shape=(
                jax.ShapeDtypeStruct((nc, *block), jnp.float32),
                jax.ShapeDtypeStruct((nb + na + 1, *block), b.dtype),
                jax.ShapeDtypeStruct((2, 128), jnp.int32),
            ),
            in_specs=[pl.BlockSpec(memory_space=pltpu.HBM)] * 5,
            out_specs=(pl.BlockSpec(memory_space=pltpu.VMEM),) * 3,
            scratch_shapes=[
                *[pltpu.VMEM((nb + na + 1, *block), b.dtype) for _ in range(2 * RING - 1)],
                pltpu.VMEM((2 * RING, 2, 2, npart), jnp.int32),
                pltpu.VMEM((2, nc), jnp.int32),
                pltpu.VMEM((nc, 128), jnp.int32),
                pltpu.SMEM((nc, 128), jnp.int32),
                pltpu.SemaphoreType.DMA((4,)),
                pltpu.SemaphoreType.DMA((4,)),
                pltpu.SemaphoreType.DMA((nsem,)),
                pltpu.SemaphoreType.DMA((RING,)),
                pltpu.SemaphoreType.DMA((RING,)),
                pltpu.SemaphoreType.DMA((3,)),
            ],
            compiler_params=pltpu.CompilerParams(
                collective_id=0, has_side_effects=True, vmem_limit_bytes=30 * 2**20),
        )(*args)
        cuts = tuple(head + (nc - head) * n // 6 for n in range(1, 7))
        vmem = pl.BlockSpec(memory_space=pltpu.VMEM)
        out = pl.pallas_call(
            functools.partial(finish, head, cuts),
            out_shape=jax.ShapeDtypeStruct((nc, *block), jnp.float32),
            in_specs=[vmem] * 3,
            out_specs=pl.BlockSpec(memory_space=pltpu.HBM),
            scratch_shapes=[
                pltpu.VMEM((nc, *block), jnp.float32),
                pltpu.SMEM((2, 128), jnp.int32),
                pltpu.SemaphoreType.DMA,
                pltpu.SemaphoreType.DMA((len(cuts) + 3,)),
            ],
            compiler_params=pltpu.CompilerParams(vmem_limit_bytes=8 * 2**20),
        )(acc, far, tab)
        return out[None, None]

    return jax.shard_map(device_step, mesh=mesh, in_specs=(row_spec, col_spec, row_spec, row_spec, row_spec), out_specs=row_spec, check_vma=False)
```
